32 devices in a mesh: chain: 32 (over z, y, x, core).
Axes of the slice: x: 2, y: 2, z: 4, core: 2. Of those that a mesh axis runs over, the one named last changes fastest.
Arguments:
- right_side: float32 [8, 4096], P(None, 'chain'), may hold values from -6 to 6
- diag_block: float32 [8, 8, 4096], P(None, None, 'chain'), may hold values from -2 to 2
- below_block: float32 [8, 8, 4096], P(None, None, 'chain'), may hold values from -2 to 2
- above_block: float32 [8, 8, 4096], P(None, None, 'chain'), may hold values from -2 to 2
- lower_level: float32 [12, 8, 8, 4096], P(None, None, None, 'chain'), may hold values from -0.5 to 0.5
- upper_level: float32 [12, 8, 8, 4096], P(None, None, None, 'chain'), may hold values from -0.5 to 0.5
- final_block: float32 [8, 8, 4096], P(None, None, 'chain'), may hold values from -1 to 1
Outputs:
- basis: float32 [4, 8, 4096], P(None, None, 'chain')
- hess: float32 [4, 3], replicated
The draws below stay inside these ranges and needn't reach their ends.
All inputs are finite; a program needn't handle non-finite values.
Results may differ from the reference program's by a relative error of at most 0.0001.
Values sent between devices are 32-bit elements; how exact they have to be, the bound alone decides.
No kernel may reach another device: no remote copies, remote signals or barrier semaphores. Data moves between devices by JAX's collectives and lax.ppermute only.
A program may use at most 64 MiB of HBM per device.

```python
import jax
import jax.numpy as jnp
from jax import lax

BLK = 8
ITERS = 3
NB = 4096
LEVELS = 12


def level_of(stream_key, extent, shards, least, high):
    gain = 1.0
    for position, blocks in shards:
        steps = jax.random.uniform(jax.random.fold_in(jax.random.fold_in(stream_key, 6), position), (blocks,), jnp.float32, least / len(shards), high / len(shards))
        gain = gain * jnp.repeat(jnp.exp(steps), extent[position] // blocks).reshape((-1,) + (1,) * (len(extent) - 1 - position))
    return gain


def noise(rng, extent, scale, reach, shards=(), kind=jnp.bfloat16):
    level = level_of(rng, extent, shards, -0.22, 0.18) if shards else 1.0
    entries = jax.random.normal(rng, extent, jnp.float32) * scale * level
    return jnp.minimum(jnp.maximum(entries, -reach), reach).astype(kind)


def setup_inputs(seed: int = 0) -> dict:
    streams_of = jax.random.split(jax.random.key(seed), 8)
    return {
        "right_side": noise(streams_of[0], (BLK, NB), 1.0, 6.0, ((1, 32),), jnp.float32),
        "diag_block": noise(streams_of[1], (BLK, BLK, NB), BLK ** -0.5, 2.0, ((2, 32),), jnp.float32),
        "below_block": noise(streams_of[2], (BLK, BLK, NB), BLK ** -0.5, 2.0, ((2, 32),), jnp.float32),
        "above_block": noise(streams_of[3], (BLK, BLK, NB), BLK ** -0.5, 2.0, ((2, 32),), jnp.float32),
        "lower_level": noise(streams_of[4], (LEVELS, BLK, BLK, NB), (16 * BLK) ** -0.5, 0.5, ((3, 32),), jnp.float32),
        "upper_level": noise(streams_of[5], (LEVELS, BLK, BLK, NB), (16 * BLK) ** -0.5, 0.5, ((3, 32),), jnp.float32),
        "final_block": noise(streams_of[6], (BLK, BLK, NB), (4 * BLK) ** -0.5, 1.0, ((2, 32),), jnp.float32),
    }


EPS = 1e-06

def blockmul(blocks, field):
    return jnp.einsum('abi,bi->ai', blocks, field, precision=lax.Precision.HIGHEST)

def lower_shift(field, stride):
    total = field.shape[1]
    if stride >= total:
        return jnp.zeros_like(field)
    return jnp.pad(field, ((0, 0), (stride, 0)))[:, :total]

def upper_shift(field, stride):
    total = field.shape[1]
    if stride >= total:
        return jnp.zeros_like(field)
    return jnp.pad(field, ((0, 0), (0, stride)))[:, stride:]

def operate(field, diag_block, below_block, above_block):
    result = 2.0 * field + blockmul(diag_block, field)
    result = result + blockmul(below_block, lower_shift(field, 1))
    return result + blockmul(above_block, upper_shift(field, 1))

def precondition(field, lower_level, upper_level, final_block):
    for level in range(lower_level.shape[0]):
        stride = 2 ** level
        field = field + blockmul(lower_level[level], lower_shift(field, stride)) + blockmul(upper_level[level], upper_shift(field, stride))
    return field + blockmul(final_block, field)

def reference(right_side, diag_block, below_block, above_block, lower_level, upper_level, final_block):
    count = right_side.shape[0] * right_side.shape[1]
    start = right_side / jnp.sqrt(jnp.sum(right_side * right_side) / count + EPS)
    basis = [start]
    hess = jnp.zeros((ITERS + 1, ITERS), jnp.float32)
    for column in range(ITERS):
        vector = operate(precondition(basis[column], lower_level, upper_level, final_block), diag_block, below_block, above_block)
        stacked = jnp.stack(basis)
        dots = jnp.einsum('kai,ai->k', stacked, vector, precision=lax.Precision.HIGHEST) / count
        vector = vector - jnp.einsum('k,kai->ai', dots, stacked, precision=lax.Precision.HIGHEST)
        length = jnp.sqrt(jnp.sum(vector * vector) / count + EPS)
        basis.append(vector / length)
        hess = hess.at[:column + 1, column].set(dots).at[column + 1, column].set(length)
    return (jnp.stack(basis), hess)
```

```python
import functools

import jax
import jax.numpy as jnp
from jax import lax
from jax.experimental import pallas as pl
from jax.experimental.pallas import tpu as pltpu
from jax.sharding import PartitionSpec as P

ITERS = 3


EPS = 1e-06
AXIS = "chain"
SUB = 8


def padded_2(x, sides, width):
    for axis, dim in sides:
        peers, length = (lax.axis_size(axis), x.shape[dim])
        up = [(i, (i + 1) % peers) for i in range(peers - 1)]
        down = [(j, i) for i, j in up]
        last = lax.slice_in_dim(x, length - width, length, axis=dim)
        initial = lax.slice_in_dim(x, 0, width, axis=dim)
        before = lax.ppermute(last, axis, up)
        after = lax.ppermute(initial, axis, down)
        x = jnp.concatenate([before, x, after], axis=dim)
    return x


def from_behind(x, axis, by):
    peers = lax.axis_size(axis)
    pairs = [(i, i + by) for i in range(peers) if 0 <= i + by < peers]
    return lax.ppermute(x, axis, pairs)


def blockmul(blocks, field):
    return jnp.einsum("abi,bi->ai", blocks, field, precision=lax.Precision.HIGHEST)


def general(
    right_side, diag_block, below_block, above_block, lower_level, upper_level, final_block
):
    rows_here = right_side.shape[1]
    devices = lax.axis_size("chain")
    whole = rows_here * devices
    count = right_side.shape[0] * whole
    depth = lower_level.shape[0]
    near = [level for level in range(depth) if 2**level < rows_here]
    far = [level for level in range(depth) if 2**level >= rows_here and 2**level < whole]
    reach = sum((2**level for level in near))
    stacked_coef = jnp.concatenate([lower_level[: len(near)], upper_level[: len(near)]], 0)
    wide_coef = padded_2(stacked_coef, (("chain", 3),), reach)
    start_sum = lax.psum(jnp.sum(right_side * right_side), "chain")
    basis = [right_side / jnp.sqrt(start_sum / count + EPS)]
    hess = jnp.zeros((ITERS + 1, ITERS), jnp.float32)
    for column in range(ITERS):
        precondition_field = basis[column]
        current = padded_2(precondition_field, (("chain", 1),), reach)
        offset = 0
        for position in range(len(near)):
            stride = 2 ** near[position]
            length = current.shape[1]
            first_col = offset + stride
            last_col = offset + length - stride
            low_coef = wide_coef[position][:, :, first_col:last_col]
            high_coef = wide_coef[len(near) + position][:, :, first_col:last_col]
            current = (
                current[:, stride : length - stride]
                + blockmul(low_coef, current[:, : length - 2 * stride])
                + blockmul(high_coef, current[:, 2 * stride :])
            )
            offset = first_col
        precondition_field = current
        for precondition_level in far:
            hops = 2**precondition_level // rows_here
            below_rows = from_behind(precondition_field, "chain", hops)
            above_rows = from_behind(precondition_field, "chain", -hops)
            precondition_field = (
                precondition_field
                + blockmul(lower_level[precondition_level], below_rows)
                + blockmul(upper_level[precondition_level], above_rows)
            )
        field = precondition_field + blockmul(final_block, precondition_field)
        padded = padded_2(field, (("chain", 1),), 1)
        result = 2.0 * field + blockmul(diag_block, field)
        result = result + blockmul(below_block, padded[:, :rows_here])
        vector = result + blockmul(above_block, padded[:, 2:])
        stacked = jnp.stack(basis)
        local_dots = jnp.einsum("kai,ai->k", stacked, vector, precision=lax.Precision.HIGHEST)
        dots = lax.psum(local_dots, "chain") / count
        vector = vector - jnp.einsum("k,kai->ai", dots, stacked, precision=lax.Precision.HIGHEST)
        squares = lax.psum(jnp.sum(vector * vector), "chain") / count
        length = jnp.sqrt(squares + EPS)
        basis.append(vector / length)
        hess = hess.at[: column + 1, column].set(dots).at[column + 1, column].set(length)
    return (jnp.stack(basis), hess)


class Plan:
    def __init__(self, devices, rows, depth):
        self.devices, self.rows, self.depth = devices, rows, depth
        self.piece = rows // devices
        self.near = [k for k in range(depth) if 2**k < rows]
        self.far = [k for k in range(depth) if rows <= 2**k < rows * devices]
        self.sent = len(self.near) - 1
        self.count = SUB * rows * devices
        n = len(self.far)
        self.own_mats = 2 * n + 4
        self.halo_mats = 2 * n + 1
        self.own_tiles = self.own_mats * SUB
        self.halo_tiles = self.halo_mats * SUB
        self.halo_packed = self.halo_tiles // 2
        self.coef_tiles = self.own_tiles + self.halo_packed
        self.per_group = rows // SUB
        tiles = self.coef_tiles + 4
        groups = -(-tiles // self.per_group)
        step = max(1, SUB // self.piece)
        self.groups = -(-groups // step) * step
        self.chunk = self.groups * self.piece
        self.width = rows // self.piece


def fits(devices, rows, block, lanes=128):
    piece = rows // devices
    return block == SUB and rows == lanes and piece >= 1 and piece * devices == rows and rows // piece >= 4 * SUB


def lane(shape=(SUB, 128)):
    return lax.broadcasted_iota(jnp.int32, shape, 1)


def sub(shape=(SUB, 128)):
    return lax.broadcasted_iota(jnp.int32, shape, 0)


def spread(v, b):
    return jnp.broadcast_to(v[b : b + 1, :], v.shape)


def total(x):
    return jnp.sum(jnp.sum(x, axis=0, keepdims=True), axis=1, keepdims=True)


def send(plan, tiles, z_ref, out_ref):
    r = plan.rows
    stacked = jnp.concatenate(tiles + [jnp.zeros((r - SUB * len(tiles), r), jnp.float32)], 0)
    z_ref[...] = stacked.T
    out = z_ref[pl.ds(0, plan.devices, stride=plan.piece), :]
    for i in range(1, plan.piece):
        part = z_ref[pl.ds(i, plan.devices, stride=plan.piece), :]
        out = out + pltpu.roll(part, i * plan.width, 1)
    out_ref[...] = out


def receive(plan, in_ref, z_ref):
    got = in_ref[...]
    for i in range(plan.piece):
        part = got if i == 0 else pltpu.roll(got, plan.rows - i * plan.width, 1)
        z_ref[pl.ds(i, plan.devices, stride=plan.piece), :] = part
    t = z_ref[...].T
    return [t[SUB * k : SUB * k + SUB] for k in range(4)]


def halo_of(plan, y):
    pos = lane() % plan.piece
    before, after = pltpu.roll(y, 1, 1), pltpu.roll(y, plan.rows - 1, 1)
    return jnp.where(pos == 0, before, jnp.where(pos == plan.piece - 1, after, 0.0))


def wrapped(plan, x):
    q, r = plan.piece, plan.rows
    me = lax.axis_index(AXIS)
    at = lane()
    pos = at % q
    later = jnp.where(at == 0, 0.0, pltpu.roll(x, q, 1))
    sooner = jnp.where(at == r - 1, 0.0, pltpu.roll(x, r - q, 1))
    first = jnp.where(me == 0, later, x)
    last = jnp.where(me == plan.devices - 1, sooner, x)
    return jnp.where(pos == 0, first, jnp.where(pos == q - 1, last, 0.0))


def near_levels(plan, v, lo_ref, up_ref, prev_ref, next_ref):
    r = plan.rows
    at = lane()
    for k in plan.near:
        s = 2**k
        turned = [pltpu.roll(x, s, 1) for x in v]
        back = [pltpu.roll(x, r - s, 1) for x in v]
        lower = [turned[0]] + [jnp.where(at < s, turned[t - 1], turned[t]) for t in (1, 2)]
        upper = [jnp.where(at >= r - s, back[t + 1], back[t]) for t in (0, 1)] + [back[2]]
        fresh = list(v)
        for t in (0, 1, 2) if k < plan.sent else (1,):
            low_sum = high_sum = None
            for b in range(SUB):
                if t == 1:
                    lc = lo_ref[pl.ds(64 * k + b, SUB, stride=SUB), :]
                    uc = up_ref[pl.ds(64 * k + b, SUB, stride=SUB), :]
                else:
                    ref = prev_ref if t == 0 else next_ref
                    lc = ref[pl.ds(64 * k + b, SUB, stride=SUB), :]
                    uc = ref[pl.ds(64 * (plan.sent + k) + b, SUB, stride=SUB), :]
                low = lc * spread(lower[t], b)
                high = uc * spread(upper[t], b)
                low_sum = low if low_sum is None else low_sum + low
                high_sum = high if high_sum is None else high_sum + high
            fresh[t] = v[t] + low_sum + high_sum
        v = fresh
    return v[1]


def square_tile(u):
    return jnp.where(sub() == 0, jnp.broadcast_to(total(u * u), u.shape), 0.0)


def pack_kernel(plan, lo_ref, up_ref, rhs_ref, out_ref):
    n = 64 * plan.sent
    out_ref[pl.ds(0, n), :] = lo_ref[pl.ds(0, n), :]
    out_ref[pl.ds(n, n), :] = up_ref[pl.ds(0, n), :]
    out_ref[pl.ds(2 * n, SUB), :] = rhs_ref[...]


def first_kernel(
    plan, lo_ref, up_ref, fin_ref, dia_ref, bel_ref, abo_ref, rhs_ref, prev_ref, next_ref, out_ref, z_ref
):
    n = 64 * 2 * plan.sent
    rhs = rhs_ref[...]
    y = near_levels(
        plan,
        [prev_ref[pl.ds(n, SUB), :], rhs, next_ref[pl.ds(n, SUB), :]],
        lo_ref,
        up_ref,
        prev_ref,
        next_ref,
    )
    mats = [(lo_ref, 64 * k) for k in plan.far] + [(up_ref, 64 * k) for k in plan.far]
    mats += [(fin_ref, 0), (dia_ref, 0), (bel_ref, 0), (abo_ref, 0)]

    def raw(index):
        ref, base = mats[index // SUB]
        return ref[pl.ds(base + index % SUB, SUB, stride=SUB), :]

    def tile(index):
        if index < plan.own_tiles:
            return raw(index)
        if index < plan.coef_tiles:
            j = 2 * (index - plan.own_tiles)
            a, b = halo_of(plan, raw(j)), halo_of(plan, raw(j + 1))
            pos = lane() % plan.piece
            moved = jnp.where(pos == 1, pltpu.roll(b, 1, 1), pltpu.roll(b, plan.rows - 1, 1))
            return jnp.where((pos == 0) | (pos == plan.piece - 1), a, moved)
        extra = index - plan.coef_tiles
        if extra == 0:
            return y
        if extra == 1:
            return halo_of(plan, y)
        if extra == 2:
            return square_tile(rhs)
        if extra == 3:
            return rhs
        return jnp.zeros((SUB, plan.rows), jnp.float32)

    g_tiles = plan.per_group
    for g in range(plan.groups):
        block = jnp.concatenate([tile(g * g_tiles + t) for t in range(g_tiles)], 0)
        z_ref[g] = block.T
        for i in range(plan.piece):
            out_ref[pl.ds(g * plan.piece + i, plan.devices, stride=plan.chunk), :] = z_ref[
                g, pl.ds(i, plan.devices, stride=plan.piece), :
            ]


def far_stage(plan, own, halo, coef_ref):
    q, r, n = plan.piece, plan.rows, len(plan.far)
    base = plan.own_tiles

    def apply(mat, x, start):
        out = coef_ref[start + mat * SUB] * spread(x, 0)
        for b in range(1, SUB):
            out = out + coef_ref[start + mat * SUB + b] * spread(x, b)
        return out

    for k in range(n):
        by = q * 2**k
        fresh = []
        for x, start in ((own, 0), (halo, base)):
            low = apply(k, pltpu.roll(x, by, 1), start)
            high = apply(n + k, pltpu.roll(x, r - by, 1), start)
            fresh.append(x + low + high)
        own, halo = fresh
    own = own + apply(2 * n, own, 0)
    halo = wrapped(plan, halo + apply(2 * n, halo, base))
    pos = lane() % q
    before = jnp.where(pos == 0, halo, pltpu.roll(own, 1, 1))
    after = jnp.where(pos == q - 1, halo, pltpu.roll(own, r - 1, 1))
    w = 2.0 * own + apply(2 * n + 1, own, 0)
    return w + apply(2 * n + 2, before, 0) + apply(2 * n + 3, after, 0)


def norm_of(plan, squares):
    pos = lane() % plan.piece
    one = jnp.where((pos == 0) & (sub() == 0), squares, 0.0)
    return jnp.sqrt(jnp.broadcast_to(total(one), one.shape) / plan.count + EPS)


def finish_far(plan, y, halo, s, vs, coef_ref, z_ref, out_ref):
    w = far_stage(plan, y / s, halo / s, coef_ref)
    q, r = plan.piece, plan.rows
    at = lane()
    before = jnp.where(at < q, 0.0, pltpu.roll(w, q, 1))
    after = jnp.where(at >= r - q, 0.0, pltpu.roll(w, r - q, 1))
    dots = jnp.zeros_like(w)
    for i, v in enumerate(vs):
        dots = jnp.where(sub() == i, jnp.broadcast_to(total(v * w), w.shape), dots)
    send(plan, [before, w, after, dots], z_ref, out_ref)
    return w


def start_far_kernel(plan, in_ref, out_ref, coef_ref, w_ref, v_ref, s_ref, z_ref, zs_ref):
    q, r = plan.piece, plan.rows
    at = lane()
    pos = at % q
    n = len(plan.far)
    g_tiles = plan.per_group
    extra = []
    for g in range(plan.groups):
        for i in range(q):
            z_ref[g, pl.ds(i, plan.devices, stride=q), :] = in_ref[
                pl.ds(g * q + i, plan.devices, stride=plan.chunk), :
            ]
        t = z_ref[g].T
        for j in range(g_tiles):
            index = g * g_tiles + j
            tile = t[SUB * j : SUB * j + SUB]

            def limited(x, mat):
                if mat < n:
                    return jnp.where(at < q * 2**mat, 0.0, x)
                if mat < 2 * n:
                    return jnp.where(at >= r - q * 2 ** (mat - n), 0.0, x)
                return x

            if index < plan.own_tiles:
                coef_ref[index] = limited(tile, index // SUB)
            elif index < plan.coef_tiles:
                k = 2 * (index - plan.own_tiles)
                other = jnp.where(pos == 0, pltpu.roll(tile, r - 1, 1), pltpu.roll(tile, 1, 1))
                coef_ref[plan.own_tiles + k] = limited(tile, k // SUB)
                coef_ref[plan.own_tiles + k + 1] = limited(other, (k + 1) // SUB)
            elif index < plan.coef_tiles + 4:
                extra.append(tile)
    y, halo, squares, rhs = extra
    s = norm_of(plan, squares)
    v = rhs / s
    v_ref[...] = v
    s_ref[...] = s
    w_ref[...] = finish_far(plan, y, halo, s, [v], coef_ref, zs_ref, out_ref)


def near_kernel(plan, j, in_ref, lo_ref, up_ref, rhs_ref, prev_ref, next_ref, *rest):
    us, ss = rest[: j - 1], rest[j - 1 : 2 * j - 1]
    out_ref, u_ref, h_ref, zr_ref, zs_ref = rest[2 * j - 1 :]
    n = 64 * 2 * plan.sent
    prev, own, nxt, dots = receive(plan, in_ref, zr_ref)
    pos = lane() % plan.piece
    h = jnp.sum(jnp.where(pos == 0, dots, 0.0), axis=1, keepdims=True) / plan.count
    h = jnp.broadcast_to(h, dots.shape)
    h_ref[...] = h
    w = [prev, own, nxt]
    fields = [[prev_ref[pl.ds(n, SUB), :], rhs_ref[...], next_ref[pl.ds(n, SUB), :]]]
    fields += [[u[t] for t in range(3)] for u in us]
    for t in range(3):
        acc = None
        for i in range(j):
            term = spread(h, i) * (fields[i][t] / ss[i][...])
            acc = term if acc is None else acc + term
        w[t] = w[t] - acc
        u_ref[t] = w[t]
    y = near_levels(plan, w, lo_ref, up_ref, prev_ref, next_ref)
    send(plan, [y, halo_of(plan, y), square_tile(w[1])], zs_ref, out_ref)


def far_kernel(plan, j, in_ref, coef_ref, h_ref, w_in_ref, *rest):
    vs = [v[...] for v in rest[:j]]
    out_ref, w_ref, v_ref, s_ref, zr_ref, zs_ref = rest[j:]
    y, halo, squares, _ = receive(plan, in_ref, zr_ref)
    s = norm_of(plan, squares)
    h = h_ref[...]
    acc = None
    for i in range(j):
        term = spread(h, i) * vs[i]
        acc = term if acc is None else acc + term
    v = (w_in_ref[...] - acc) / s
    v_ref[...] = v
    s_ref[...] = s
    w_ref[...] = finish_far(plan, y, halo, s, vs + [v], coef_ref, zs_ref, out_ref)


def last_kernel(plan, in_ref, rhs_ref, *rest):
    us, ss = rest[: ITERS - 1], rest[ITERS - 1 : 2 * ITERS - 1]
    u_ref, h_ref, out_ref, zr_ref = rest[2 * ITERS - 1 :]
    _, own, _, dots = receive(plan, in_ref, zr_ref)
    pos = lane() % plan.piece
    h = jnp.sum(jnp.where(pos == 0, dots, 0.0), axis=1, keepdims=True) / plan.count
    h = jnp.broadcast_to(h, dots.shape)
    h_ref[...] = h
    fields = [rhs_ref[...]] + [u[1] for u in us]
    acc = None
    for i in range(ITERS):
        term = spread(h, i) * (fields[i] / ss[i][...])
        acc = term if acc is None else acc + term
    u = own - acc
    u_ref[...] = u
    out_ref[...] = jnp.broadcast_to(total(u * u), out_ref.shape)


def output_kernel(plan, in_ref, rhs_ref, *rest):
    us = [u[1] for u in rest[: ITERS - 1]] + [rest[ITERS - 1][...]]
    ss = [s[...] for s in rest[ITERS : 2 * ITERS]]
    hs = [h[...] for h in rest[2 * ITERS : 3 * ITERS]]
    basis_ref, hess_ref = rest[3 * ITERS :]
    squares = jnp.sum(in_ref[...], axis=0, keepdims=True)
    ss.append(jnp.broadcast_to(jnp.sqrt(squares / plan.count + EPS), ss[0].shape))
    fields = [rhs_ref[...]] + us
    for j in range(ITERS + 1):
        basis_ref[j] = fields[j] / ss[j]
    hess = jnp.zeros_like(ss[0])
    for j in range(ITERS):
        col = jnp.where(sub() <= j, hs[j], jnp.where(sub() == j + 1, ss[j + 1], 0.0))
        hess = jnp.where(lane() == j, col, hess)
    hess_ref[...] = hess[: ITERS + 1, :ITERS]


def transposed(
    plan, right_side, diag_block, below_block, above_block, lower_level, upper_level, final_block
):
    r, d = plan.rows, plan.devices
    flat = lambda x: x.reshape(-1, r)
    lo, up, fin = flat(lower_level), flat(upper_level), flat(final_block)
    dia, bel, abo = flat(diag_block), flat(below_block), flat(above_block)
    shape = lambda *s: jax.ShapeDtypeStruct(s, jnp.float32)
    tile = shape(SUB, r)
    scratch = lambda *s: pltpu.VMEM(s, jnp.float32)

    def call(kernel, outs, scratches, *args):
        return pl.pallas_call(
            kernel,
            out_shape=outs,
            in_specs=[pl.BlockSpec(memory_space=pltpu.VMEM)] * len(args),
            out_specs=jax.tree.map(lambda _: pl.BlockSpec(memory_space=pltpu.VMEM), outs),
            scratch_shapes=scratches,
            compiler_params=pltpu.CompilerParams(vmem_limit_bytes=24 * 2**20),
            cost_estimate=pl.CostEstimate(flops=4_000_000, bytes_accessed=2_000_000, transcendentals=0),
        )(*args)

    def exchange(x):
        y = lax.all_to_all(x.reshape(d, -1, r), AXIS, 0, 0)
        return y.reshape(-1, r)

    part = functools.partial
    edge = call(part(pack_kernel, plan), shape(64 * 2 * plan.sent + SUB, r), [], lo, up, right_side)
    prev = lax.ppermute(edge, AXIS, [(i, i + 1) for i in range(d - 1)])
    nxt = lax.ppermute(edge, AXIS, [(i + 1, i) for i in range(d - 1)])
    big = call(
        part(first_kernel, plan),
        shape(d * plan.chunk, r),
        [scratch(plan.groups, r, r)],
        lo, up, fin, dia, bel, abo, right_side, prev, nxt,
    )
    got = exchange(big)
    small = shape(d, r)
    out, coef, w, v, s = call(
        part(start_far_kernel, plan),
        (small, shape(plan.own_tiles + plan.halo_tiles, SUB, r), tile, tile, tile),
        [scratch(plan.groups, r, r), scratch(r, r)],
        got,
    )
    us, ss, vs, hs = [], [s], [v], []
    for j in range(1, ITERS):
        out, u, h = call(
            part(near_kernel, plan, j),
            (small, shape(3, SUB, r), tile),
            [scratch(r, r), scratch(r, r)],
            exchange(out), lo, up, right_side, prev, nxt, *us, *ss,
        )
        us.append(u)
        hs.append(h)
        out, w, v, s = call(
            part(far_kernel, plan, j),
            (small, tile, tile, tile),
            [scratch(r, r), scratch(r, r)],
            exchange(out), coef, h, w, *vs,
        )
        vs.append(v)
        ss.append(s)
    u, h, out = call(
        part(last_kernel, plan), (tile, tile, small), [scratch(r, r)], exchange(out), right_side, *us, *ss
    )
    hs.append(h)
    return call(
        part(output_kernel, plan),
        (shape(ITERS + 1, SUB, r), shape(ITERS + 1, ITERS)),
        [],
        exchange(out), right_side, *us, u, *ss, *hs,
    )


def on_device(*args):
    right_side, lower_level = args[0], args[4]
    devices, rows = lax.axis_size(AXIS), right_side.shape[1]
    if not fits(devices, rows, right_side.shape[0]):
        return general(*args)
    return tuple(transposed(Plan(devices, rows, lower_level.shape[0]), *args))


def solution(mesh):
    return jax.shard_map(
        on_device,
        mesh=mesh,
        in_specs=(
            P(None, "chain"),
            P(None, None, "chain"),
            P(None, None, "chain"),
            P(None, None, "chain"),
            P(None, None, None, "chain"),
            P(None, None, None, "chain"),
            P(None, None, "chain"),
        ),
        out_specs=(P(None, None, "chain"), P()),
        check_vma=False,
    )
```

```python
import functools

import jax
import jax.numpy as jnp
from jax import lax
from jax.experimental import pallas as pl
from jax.experimental.pallas import tpu as pltpu
from jax.sharding import PartitionSpec as P

ITERS = 3


EPS = 1e-06
AXIS = "chain"
SUB = 8


def padded_2(x, sides, width):
    for axis, dim in sides:
        peers, length = (lax.axis_size(axis), x.shape[dim])
        up = [(i, (i + 1) % peers) for i in range(peers - 1)]
        down = [(j, i) for i, j in up]
        last = lax.slice_in_dim(x, length - width, length, axis=dim)
        initial = lax.slice_in_dim(x, 0, width, axis=dim)
        before = lax.ppermute(last, axis, up)
        after = lax.ppermute(initial, axis, down)
        x = jnp.concatenate([before, x, after], axis=dim)
    return x


def from_behind(x, axis, by):
    peers = lax.axis_size(axis)
    pairs = [(i, i + by) for i in range(peers) if 0 <= i + by < peers]
    return lax.ppermute(x, axis, pairs)


def blockmul(blocks, field):
    return jnp.einsum("abi,bi->ai", blocks, field, precision=lax.Precision.HIGHEST)


def general(
    right_side, diag_block, below_block, above_block, lower_level, upper_level, final_block
):
    rows_here = right_side.shape[1]
    devices = lax.axis_size("chain")
    whole = rows_here * devices
    count = right_side.shape[0] * whole
    depth = lower_level.shape[0]
    near = [level for level in range(depth) if 2**level < rows_here]
    far = [level for level in range(depth) if 2**level >= rows_here and 2**level < whole]
    reach = sum((2**level for level in near))
    stacked_coef = jnp.concatenate([lower_level[: len(near)], upper_level[: len(near)]], 0)
    wide_coef = padded_2(stacked_coef, (("chain", 3),), reach)
    start_sum = lax.psum(jnp.sum(right_side * right_side), "chain")
    basis = [right_side / jnp.sqrt(start_sum / count + EPS)]
    hess = jnp.zeros((ITERS + 1, ITERS), jnp.float32)
    for column in range(ITERS):
        precondition_field = basis[column]
        current = padded_2(precondition_field, (("chain", 1),), reach)
        offset = 0
        for position in range(len(near)):
            stride = 2 ** near[position]
            length = current.shape[1]
            first_col = offset + stride
            last_col = offset + length - stride
            low_coef = wide_coef[position][:, :, first_col:last_col]
            high_coef = wide_coef[len(near) + position][:, :, first_col:last_col]
            current = (
                current[:, stride : length - stride]
                + blockmul(low_coef, current[:, : length - 2 * stride])
                + blockmul(high_coef, current[:, 2 * stride :])
            )
            offset = first_col
        precondition_field = current
        for precondition_level in far:
            hops = 2**precondition_level // rows_here
            below_rows = from_behind(precondition_field, "chain", hops)
            above_rows = from_behind(precondition_field, "chain", -hops)
            precondition_field = (
                precondition_field
                + blockmul(lower_level[precondition_level], below_rows)
                + blockmul(upper_level[precondition_level], above_rows)
            )
        field = precondition_field + blockmul(final_block, precondition_field)
        padded = padded_2(field, (("chain", 1),), 1)
        result = 2.0 * field + blockmul(diag_block, field)
        result = result + blockmul(below_block, padded[:, :rows_here])
        vector = result + blockmul(above_block, padded[:, 2:])
        stacked = jnp.stack(basis)
        local_dots = jnp.einsum("kai,ai->k", stacked, vector, precision=lax.Precision.HIGHEST)
        dots = lax.psum(local_dots, "chain") / count
        vector = vector - jnp.einsum("k,kai->ai", dots, stacked, precision=lax.Precision.HIGHEST)
        squares = lax.psum(jnp.sum(vector * vector), "chain") / count
        length = jnp.sqrt(squares + EPS)
        basis.append(vector / length)
        hess = hess.at[: column + 1, column].set(dots).at[column + 1, column].set(length)
    return (jnp.stack(basis), hess)


class Plan:
    def __init__(self, devices, rows, depth):
        self.devices, self.rows, self.depth = devices, rows, depth
        self.piece = rows // devices
        self.near = [k for k in range(depth) if 2**k < rows]
        self.far = [k for k in range(depth) if rows <= 2**k < rows * devices]
        self.sent = len(self.near) - 1
        self.count = SUB * rows * devices
        n = len(self.far)
        self.own_mats = 2 * n + 4
        self.halo_mats = 2 * n + 1
        self.own_tiles = self.own_mats * SUB
        self.halo_tiles = self.halo_mats * SUB
        self.halo_packed = self.halo_tiles // 2
        self.coef_tiles = self.own_tiles + self.halo_packed
        self.per_group = rows // SUB
        tiles = self.coef_tiles + 4
        groups = -(-tiles // self.per_group)
        step = max(1, SUB // self.piece)
        self.groups = -(-groups // step) * step
        self.whole_groups = self.coef_tiles // self.per_group
        self.chunk = self.groups * self.piece
        self.width = rows // self.piece


def fits(devices, rows, block, lanes=128):
    piece = rows // devices
    return block == SUB and rows == lanes and piece >= 1 and piece * devices == rows and rows // piece >= 4 * SUB


def lane(shape=(SUB, 128)):
    return lax.broadcasted_iota(jnp.int32, shape, 1)


def sub(shape=(SUB, 128)):
    return lax.broadcasted_iota(jnp.int32, shape, 0)


def spread(v, b):
    return jnp.broadcast_to(v[b : b + 1, :], v.shape)


def total(x):
    return jnp.sum(jnp.sum(x, axis=0, keepdims=True), axis=1, keepdims=True)


def send(plan, tiles, z_ref, out_ref):
    r = plan.rows
    stacked = jnp.concatenate(tiles + [jnp.zeros((r - SUB * len(tiles), r), jnp.float32)], 0)
    z_ref[...] = stacked.T
    out = z_ref[pl.ds(0, plan.devices, stride=plan.piece), :]
    for i in range(1, plan.piece):
        part = z_ref[pl.ds(i, plan.devices, stride=plan.piece), :]
        out = out + pltpu.roll(part, i * plan.width, 1)
    out_ref[...] = out


def receive(plan, in_ref, z_ref):
    got = in_ref[...]
    for i in range(plan.piece):
        part = got if i == 0 else pltpu.roll(got, plan.rows - i * plan.width, 1)
        z_ref[pl.ds(i, plan.devices, stride=plan.piece), :] = part
    t = z_ref[...].T
    return [t[SUB * k : SUB * k + SUB] for k in range(4)]


def halo_of(plan, y):
    pos = lane() % plan.piece
    before, after = pltpu.roll(y, 1, 1), pltpu.roll(y, plan.rows - 1, 1)
    return jnp.where(pos == 0, before, jnp.where(pos == plan.piece - 1, after, 0.0))


def wrapped(plan, x):
    q, r = plan.piece, plan.rows
    me = lax.axis_index(AXIS)
    at = lane()
    pos = at % q
    later = jnp.where(at == 0, 0.0, pltpu.roll(x, q, 1))
    sooner = jnp.where(at == r - 1, 0.0, pltpu.roll(x, r - q, 1))
    first = jnp.where(me == 0, later, x)
    last = jnp.where(me == plan.devices - 1, sooner, x)
    return jnp.where(pos == 0, first, jnp.where(pos == q - 1, last, 0.0))


def near_levels(plan, v, coef):
    r = plan.rows
    at = lane()
    for k in plan.near:
        s = 2**k
        turned = [pltpu.roll(x, s, 1) for x in v]
        back = [pltpu.roll(x, r - s, 1) for x in v]
        lower = [turned[0]] + [jnp.where(at < s, turned[t - 1], turned[t]) for t in (1, 2)]
        upper = [jnp.where(at >= r - s, back[t + 1], back[t]) for t in (0, 1)] + [back[2]]
        fresh = list(v)
        for t in (0, 1, 2) if k < plan.sent else (1,):
            low_sum = high_sum = None
            for b in range(SUB):
                low = coef(t, 0, k, b) * spread(lower[t], b)
                high = coef(t, 1, k, b) * spread(upper[t], b)
                low_sum = low if low_sum is None else low_sum + low
                high_sum = high if high_sum is None else high_sum + high
            fresh[t] = v[t] + low_sum + high_sum
        v = fresh
    return v[1]


def square_tile(u):
    return jnp.where(sub() == 0, jnp.broadcast_to(total(u * u), u.shape), 0.0)


def edge_kernel(plan, lo_ref, up_ref, rhs_ref, out_ref, sems):
    n = 64 * plan.sent
    copies = [
        pltpu.make_async_copy(lo_ref.at[pl.ds(0, n)], out_ref.at[pl.ds(0, n)], sems.at[0]),
        pltpu.make_async_copy(up_ref.at[pl.ds(0, n)], out_ref.at[pl.ds(n, n)], sems.at[1]),
        pltpu.make_async_copy(rhs_ref, out_ref.at[pl.ds(2 * n, SUB)], sems.at[2]),
    ]
    for c in copies:
        c.start()
    for c in copies:
        c.wait()


def pack_tile(plan, raw, index):
    if index < plan.own_tiles:
        return raw(index)
    j = 2 * (index - plan.own_tiles)
    a, b = halo_of(plan, raw(j)), halo_of(plan, raw(j + 1))
    pos = lane() % plan.piece
    moved = jnp.where(pos == 1, pltpu.roll(b, 1, 1), pltpu.roll(b, plan.rows - 1, 1))
    return jnp.where((pos == 0) | (pos == plan.piece - 1), a, moved)


def pack_group(plan, g, tiles, z_ref, out_ref):
    z_ref[g % z_ref.shape[0]] = jnp.concatenate(tiles, 0).T
    for i in range(plan.piece):
        out_ref[pl.ds(g * plan.piece + i, plan.devices, stride=plan.chunk), :] = z_ref[
            g % z_ref.shape[0], pl.ds(i, plan.devices, stride=plan.piece), :
        ]


def pack_kernel(plan, lo_ref, up_ref, fin_ref, dia_ref, bel_ref, abo_ref, out_ref, rest_ref, z_ref):
    mats = [(lo_ref, 64 * k) for k in plan.far] + [(up_ref, 64 * k) for k in plan.far]
    mats += [(fin_ref, 0), (dia_ref, 0), (bel_ref, 0), (abo_ref, 0)]

    def raw(index):
        ref, base = mats[index // SUB]
        return ref[pl.ds(base + index % SUB, SUB, stride=SUB), :]

    t = plan.per_group
    for g in range(plan.whole_groups):
        pack_group(plan, g, [pack_tile(plan, raw, g * t + i) for i in range(t)], z_ref, out_ref)
    for i in range(plan.whole_groups * t, plan.coef_tiles):
        rest_ref[i - plan.whole_groups * t] = pack_tile(plan, raw, i)


def first_kernel(
    plan, lo_ref, up_ref, rhs_ref, pair_ref, other_ref, rest_in_ref, chunk_ref, out_ref, coef_ref, field_ref, z_ref
):
    n = 64 * 2 * plan.sent
    odd = lax.rem(lax.axis_index(AXIS), 2) == 1
    rhs = rhs_ref[...]

    def halo(t, start, stride):
        a, b = pair_ref[pl.ds(start, SUB, stride=stride), :], other_ref[pl.ds(start, SUB, stride=stride), :]
        return jnp.where(odd, a, b) if t == 0 else jnp.where(odd, b, a)

    def coef(t, side, k, b):
        if t == 1:
            ref = up_ref if side else lo_ref
            x = ref[pl.ds(64 * k + b, SUB, stride=SUB), :]
        else:
            x = halo(t, 64 * (plan.sent * side + k) + b, SUB)
        coef_ref[t, side, k, b] = x
        return x

    fields = [halo(0, n, 1), rhs, halo(2, n, 1)]
    for t in range(3):
        field_ref[t] = fields[t]
    y = near_levels(plan, fields, coef)
    t = plan.per_group
    first = plan.whole_groups * t
    tiles = [rest_in_ref[i] for i in range(plan.coef_tiles - first)]
    tiles += [y, halo_of(plan, y), square_tile(rhs), rhs]
    tiles += [jnp.zeros_like(rhs)] * (plan.groups * t - first - len(tiles))
    for g in range(plan.whole_groups, plan.groups):
        at = g * t - first
        pack_group(plan, g, tiles[at : at + t], z_ref, out_ref)


def far_stage(plan, own, halo, coef_ref):
    q, r, n = plan.piece, plan.rows, len(plan.far)
    base = plan.own_tiles

    def apply(mat, x, start):
        out = coef_ref[start + mat * SUB] * spread(x, 0)
        for b in range(1, SUB):
            out = out + coef_ref[start + mat * SUB + b] * spread(x, b)
        return out

    for k in range(n):
        by = q * 2**k
        fresh = []
        for x, start in ((own, 0), (halo, base)):
            low = apply(k, pltpu.roll(x, by, 1), start)
            high = apply(n + k, pltpu.roll(x, r - by, 1), start)
            fresh.append(x + low + high)
        own, halo = fresh
    own = own + apply(2 * n, own, 0)
    halo = wrapped(plan, halo + apply(2 * n, halo, base))
    pos = lane() % q
    before = jnp.where(pos == 0, halo, pltpu.roll(own, 1, 1))
    after = jnp.where(pos == q - 1, halo, pltpu.roll(own, r - 1, 1))
    w = 2.0 * own + apply(2 * n + 1, own, 0)
    return w + apply(2 * n + 2, before, 0) + apply(2 * n + 3, after, 0)


def norm_of(plan, squares):
    pos = lane() % plan.piece
    one = jnp.where((pos == 0) & (sub() == 0), squares, 0.0)
    return jnp.sqrt(jnp.broadcast_to(total(one), one.shape) / plan.count + EPS)


def finish_far(plan, y, halo, s, vs, coef_ref, z_ref, out_ref):
    w = far_stage(plan, y / s, halo / s, coef_ref)
    q, r = plan.piece, plan.rows
    at = lane()
    before = jnp.where(at < q, 0.0, pltpu.roll(w, q, 1))
    after = jnp.where(at >= r - q, 0.0, pltpu.roll(w, r - q, 1))
    dots = jnp.zeros_like(w)
    for i, v in enumerate(vs):
        dots = jnp.where(sub() == i, jnp.broadcast_to(total(v * w), w.shape), dots)
    send(plan, [before, w, after, dots], z_ref, out_ref)
    return w


def two_sum(a, b):
    s = a + b
    t = s - a
    return s, (a - (s - t)) + (b - t)


def halves(a):
    c = 4097.0 * a
    hi = c - (c - a)
    return hi, a - hi


def two_prod(a, b):
    p = a * b
    ah, al = halves(a)
    bh, bl = halves(b)
    return p, ((ah * bh - p) + ah * bl + al * bh) + al * bl


def pair_add(x, y):
    s, e = two_sum(x[0], y[0])
    e = e + (x[1] + y[1])
    hi = s + e
    return hi, e - (hi - s)


def pair_mul(x, y):
    p, e = two_prod(x[0], y[0])
    e = e + (x[0] * y[1] + x[1] * y[0])
    hi = p + e
    return hi, e - (hi - p)


def folded(x, shifts, axis):
    for s in shifts:
        x = pair_add(x, tuple(pltpu.roll(a, s, axis) for a in x))
    return x


def products():
    out = [(i, None) for i in range(ITERS)] + [(None, None)]
    return out + [(i, j) for i in range(ITERS) for j in range(i, ITERS)]


def last_far_kernel(plan, in_ref, coef_ref, h_ref, w_in_ref, *rest):
    j = ITERS - 1
    vs = [v[...] for v in rest[:j]]
    out_ref, s_ref, zr_ref, zs_ref = rest[j:]
    y, halo, s, v = enter_far(plan, in_ref, h_ref, w_in_ref, vs, zr_ref)
    s_ref[...] = s
    vs = vs + [v]
    w = far_stage(plan, y / s, halo / s, coef_ref)
    sums = []
    for a, b in products():
        pair = two_prod(w if a is None else vs[a], w if b is None else vs[b])
        sums.append(folded(pair, (4, 2, 1), 0))
    at = sub()
    packed = []
    for start in range(0, len(sums), SUB):
        tile = [jnp.zeros_like(w), jnp.zeros_like(w)]
        for i, pair in enumerate(sums[start : start + SUB]):
            tile = [jnp.where(at == i, x, old) for x, old in zip(pair, tile)]
        packed.append(folded(tile, [2**i for i in range(plan.rows.bit_length() - 1)], 1))
    (hi, lo), (hi2, lo2) = packed
    last = jnp.where(at < SUB // 2, hi2, pltpu.roll(lo2, SUB // 2, 0))
    send(plan, [w, hi, lo, last], zs_ref, out_ref)


def start_far_kernel(plan, in_ref, out_ref, coef_ref, w_ref, v_ref, s_ref, z_ref, zs_ref):
    q, r = plan.piece, plan.rows
    at = lane()
    pos = at % q
    n = len(plan.far)
    g_tiles = plan.per_group
    extra = []
    for g in range(plan.groups):
        for i in range(q):
            z_ref[g, pl.ds(i, plan.devices, stride=q), :] = in_ref[
                pl.ds(g * q + i, plan.devices, stride=plan.chunk), :
            ]
        t = z_ref[g].T
        for j in range(g_tiles):
            index = g * g_tiles + j
            tile = t[SUB * j : SUB * j + SUB]

            def limited(x, mat):
                if mat < n:
                    return jnp.where(at < q * 2**mat, 0.0, x)
                if mat < 2 * n:
                    return jnp.where(at >= r - q * 2 ** (mat - n), 0.0, x)
                return x

            if index < plan.own_tiles:
                coef_ref[index] = limited(tile, index // SUB)
            elif index < plan.coef_tiles:
                k = 2 * (index - plan.own_tiles)
                other = jnp.where(pos == 0, pltpu.roll(tile, r - 1, 1), pltpu.roll(tile, 1, 1))
                coef_ref[plan.own_tiles + k] = limited(tile, k // SUB)
                coef_ref[plan.own_tiles + k + 1] = limited(other, (k + 1) // SUB)
            elif index < plan.coef_tiles + 4:
                extra.append(tile)
    y, halo, squares, rhs = extra
    s = norm_of(plan, squares)
    v = rhs / s
    v_ref[...] = v
    s_ref[...] = s
    w_ref[...] = finish_far(plan, y, halo, s, [v], coef_ref, zs_ref, out_ref)


def near_kernel(plan, j, in_ref, coef_ref, field_ref, *rest):
    us, ss = rest[: j - 1], rest[j - 1 : 2 * j - 1]
    out_ref, u_ref, h_ref, zr_ref, zs_ref = rest[2 * j - 1 :]
    *w, dots = receive(plan, in_ref, zr_ref)
    pos = lane() % plan.piece
    h = jnp.sum(jnp.where(pos == 0, dots, 0.0), axis=1, keepdims=True) / plan.count
    h = jnp.broadcast_to(h, dots.shape)
    h_ref[...] = h
    fields = [field_ref, *us]
    for t in range(3):
        acc = None
        for i in range(j):
            term = spread(h, i) * (fields[i][t] / ss[i][...])
            acc = term if acc is None else acc + term
        w[t] = w[t] - acc
        u_ref[t] = w[t]
    y = near_levels(plan, w, lambda t, side, k, b: coef_ref[t, side, k, b])
    send(plan, [y, halo_of(plan, y), square_tile(w[1])], zs_ref, out_ref)


def enter_far(plan, in_ref, h_ref, w_in_ref, vs, z_ref):
    y, halo, squares, _ = receive(plan, in_ref, z_ref)
    s = norm_of(plan, squares)
    h = h_ref[...]
    acc = None
    for i, v in enumerate(vs):
        term = spread(h, i) * v
        acc = term if acc is None else acc + term
    return y, halo, s, (w_in_ref[...] - acc) / s


def far_kernel(plan, j, in_ref, coef_ref, h_ref, w_in_ref, *rest):
    vs = [v[...] for v in rest[:j]]
    out_ref, w_ref, v_ref, s_ref, zr_ref, zs_ref = rest[j:]
    y, halo, s, v = enter_far(plan, in_ref, h_ref, w_in_ref, vs, zr_ref)
    v_ref[...] = v
    s_ref[...] = s
    w_ref[...] = finish_far(plan, y, halo, s, vs + [v], coef_ref, zs_ref, out_ref)


def output_kernel(plan, in_ref, field_ref, *rest):
    us = rest[: ITERS - 1]
    ss = [s[...] for s in rest[ITERS - 1 : 2 * ITERS - 1]]
    hs = [h[...] for h in rest[2 * ITERS - 1 : 3 * ITERS - 2]]
    basis_ref, hess_ref, z_ref = rest[3 * ITERS - 2 :]
    w, hi, lo, last = receive(plan, in_ref, z_ref)
    shifts = [plan.piece * 2**i for i in range(plan.devices.bit_length() - 1)]
    one = folded((hi, lo), shifts, 1)
    two = folded((last, pltpu.roll(last, SUB // 2, 0)), shifts, 1)
    sums = [tuple(x[i : i + 1] for x in one) for i in range(SUB)]
    sums += [tuple(x[i : i + 1] for x in two) for i in range(SUB // 2)]
    names = products()
    got = dict(zip(names, sums))
    h = [got[i, None][0] / plan.count for i in range(ITERS)]
    zero = jnp.zeros_like(h[0])
    squares = got[None, None]
    for i in range(ITERS):
        left = tuple(2.0 * x for x in got[i, None])
        for j in range(ITERS):
            left = pair_add(left, pair_mul((-h[j], zero), got[min(i, j), max(i, j)]))
        squares = pair_add(squares, pair_mul((-h[i], zero), left))
    squares = jnp.maximum(squares[0], 0.0)
    wide = lambda x: jnp.broadcast_to(x, (SUB, plan.rows))
    ss.append(wide(jnp.sqrt(squares / plan.count + EPS)))
    fields = [field_ref[1]] + [u[1] for u in us]
    vs = [f / s for f, s in zip(fields, ss)]
    acc = None
    for i in range(ITERS):
        term = wide(h[i]) * vs[i]
        acc = term if acc is None else acc + term
    vs.append((w - acc) / ss[-1])
    for j in range(ITERS + 1):
        basis_ref[j] = vs[j]
    top = jnp.zeros_like(w)
    for i in range(ITERS):
        top = jnp.where(sub() == i, wide(h[i]), top)
    hs.append(top)
    hess = jnp.zeros_like(w)
    for j in range(ITERS):
        col = jnp.where(sub() <= j, hs[j], jnp.where(sub() == j + 1, ss[j + 1], 0.0))
        hess = jnp.where(lane() == j, col, hess)
    hess_ref[...] = hess[: ITERS + 1, :ITERS]


def transposed(
    plan, right_side, diag_block, below_block, above_block, lower_level, upper_level, final_block
):
    r, d = plan.rows, plan.devices
    flat = lambda x: x.reshape(-1, r)
    lo, up, fin = flat(lower_level), flat(upper_level), flat(final_block)
    dia, bel, abo = flat(diag_block), flat(below_block), flat(above_block)
    shape = lambda *s: jax.ShapeDtypeStruct(s, jnp.float32)
    tile = shape(SUB, r)
    scratch = lambda *s: pltpu.VMEM(s, jnp.float32)

    def call(kernel, outs, scratches, *args, space=pltpu.VMEM, flops=1_000_000, **more):
        return pl.pallas_call(
            kernel,
            out_shape=outs,
            in_specs=[pl.BlockSpec(memory_space=space)] * len(args),
            out_specs=jax.tree.map(lambda _: pl.BlockSpec(memory_space=pltpu.VMEM), outs),
            scratch_shapes=scratches,
            compiler_params=pltpu.CompilerParams(vmem_limit_bytes=24 * 2**20),
            cost_estimate=pl.CostEstimate(flops=flops, bytes_accessed=1_000_000, transcendentals=0),
            **more,
        )(*args)

    def exchange(x):
        y = lax.all_to_all(x.reshape(d, -1, r), AXIS, 0, 0)
        return y.reshape(-1, r)

    part = functools.partial
    edge = call(
        part(edge_kernel, plan),
        shape(64 * 2 * plan.sent + SUB, r),
        [pltpu.SemaphoreType.DMA((3,))],
        lo, up, right_side,
        space=pl.ANY,
    )
    other = lax.ppermute(edge, AXIS, [(i, i + 1 if i % 2 else i - 1) for i in range(1, d - 1)])
    pair = lax.ppermute(edge, AXIS, [(i, i ^ 1) for i in range(d)])
    left = plan.coef_tiles - plan.whole_groups * plan.per_group
    chunk, rest = call(
        part(pack_kernel, plan),
        (shape(d * plan.chunk, r), shape(max(left, 1), SUB, r)),
        [scratch(plan.whole_groups, r, r)],
        lo, up, fin, dia, bel, abo,
        flops=20_000_000,
    )
    chunk, near, fields = call(
        part(first_kernel, plan),
        (shape(d * plan.chunk, r), shape(3, 2, len(plan.near), SUB, SUB, r), shape(3, SUB, r)),
        [scratch(plan.groups - plan.whole_groups, r, r)],
        lo, up, right_side, pair, other, rest, chunk,
        input_output_aliases={6: 0},
    )
    small = shape(d, r)
    two = [scratch(r, r), scratch(r, r)]
    out, coef, w, v, s = call(
        part(start_far_kernel, plan),
        (small, shape(plan.own_tiles + plan.halo_tiles, SUB, r), tile, tile, tile),
        [scratch(plan.groups, r, r), scratch(r, r)],
        exchange(chunk),
    )
    us, ss, vs, hs = [], [s], [v], []
    for j in range(1, ITERS):
        out, u, h = call(
            part(near_kernel, plan, j),
            (small, shape(3, SUB, r), tile),
            two,
            exchange(out), near, fields, *us, *ss,
        )
        us.append(u)
        hs.append(h)
        if j < ITERS - 1:
            out, w, v, s = call(
                part(far_kernel, plan, j), (small, tile, tile, tile), two, exchange(out), coef, h, w, *vs
            )
            vs.append(v)
        else:
            out, s = call(part(last_far_kernel, plan), (small, tile), two, exchange(out), coef, h, w, *vs)
        ss.append(s)
    return call(
        part(output_kernel, plan),
        (shape(ITERS + 1, SUB, r), shape(ITERS + 1, ITERS)),
        [scratch(r, r)],
        exchange(out), fields, *us, *ss, *hs,
    )


def on_device(*args):
    right_side, lower_level = args[0], args[4]
    devices, rows = lax.axis_size(AXIS), right_side.shape[1]
    if not fits(devices, rows, right_side.shape[0]):
        return general(*args)
    return tuple(transposed(Plan(devices, rows, lower_level.shape[0]), *args))


def solution(mesh):
    return jax.shard_map(
        on_device,
        mesh=mesh,
        in_specs=(
            P(None, "chain"),
            P(None, None, "chain"),
            P(None, None, "chain"),
            P(None, None, "chain"),
            P(None, None, None, "chain"),
            P(None, None, None, "chain"),
            P(None, None, "chain"),
        ),
        out_specs=(P(None, None, "chain"), P()),
        check_vma=False,
    )
```

```python
import functools

import jax
import jax.numpy as jnp
from jax import lax
from jax.experimental import pallas as pl
from jax.experimental.pallas import tpu as pltpu
from jax.sharding import PartitionSpec as P


ITERS = 3


EPS = 1e-06
AXIS = "chain"
SUB = 8
EARLY = 6


def padded_2(x, sides, width):
    for axis, dim in sides:
        peers, length = (lax.axis_size(axis), x.shape[dim])
        up = [(i, (i + 1) % peers) for i in range(peers - 1)]
        down = [(j, i) for i, j in up]
        last = lax.slice_in_dim(x, length - width, length, axis=dim)
        initial = lax.slice_in_dim(x, 0, width, axis=dim)
        before = lax.ppermute(last, axis, up)
        after = lax.ppermute(initial, axis, down)
        x = jnp.concatenate([before, x, after], axis=dim)
    return x


def from_behind(x, axis, by):
    peers = lax.axis_size(axis)
    pairs = [(i, i + by) for i in range(peers) if 0 <= i + by < peers]
    return lax.ppermute(x, axis, pairs)


def blockmul(blocks, field):
    return jnp.einsum("abi,bi->ai", blocks, field, precision=lax.Precision.HIGHEST)


def general(
    right_side, diag_block, below_block, above_block, lower_level, upper_level, final_block
):
    rows_here = right_side.shape[1]
    devices = lax.axis_size("chain")
    whole = rows_here * devices
    count = right_side.shape[0] * whole
    depth = lower_level.shape[0]
    near = [level for level in range(depth) if 2**level < rows_here]
    far = [level for level in range(depth) if 2**level >= rows_here and 2**level < whole]
    reach = sum((2**level for level in near))
    stacked_coef = jnp.concatenate([lower_level[: len(near)], upper_level[: len(near)]], 0)
    wide_coef = padded_2(stacked_coef, (("chain", 3),), reach)
    start_sum = lax.psum(jnp.sum(right_side * right_side), "chain")
    basis = [right_side / jnp.sqrt(start_sum / count + EPS)]
    hess = jnp.zeros((ITERS + 1, ITERS), jnp.float32)
    for column in range(ITERS):
        precondition_field = basis[column]
        current = padded_2(precondition_field, (("chain", 1),), reach)
        offset = 0
        for position in range(len(near)):
            stride = 2 ** near[position]
            length = current.shape[1]
            first_col = offset + stride
            last_col = offset + length - stride
            low_coef = wide_coef[position][:, :, first_col:last_col]
            high_coef = wide_coef[len(near) + position][:, :, first_col:last_col]
            current = (
                current[:, stride : length - stride]
                + blockmul(low_coef, current[:, : length - 2 * stride])
                + blockmul(high_coef, current[:, 2 * stride :])
            )
            offset = first_col
        precondition_field = current
        for precondition_level in far:
            hops = 2**precondition_level // rows_here
            below_rows = from_behind(precondition_field, "chain", hops)
            above_rows = from_behind(precondition_field, "chain", -hops)
            precondition_field = (
                precondition_field
                + blockmul(lower_level[precondition_level], below_rows)
                + blockmul(upper_level[precondition_level], above_rows)
            )
        field = precondition_field + blockmul(final_block, precondition_field)
        padded = padded_2(field, (("chain", 1),), 1)
        result = 2.0 * field + blockmul(diag_block, field)
        result = result + blockmul(below_block, padded[:, :rows_here])
        vector = result + blockmul(above_block, padded[:, 2:])
        stacked = jnp.stack(basis)
        local_dots = jnp.einsum("kai,ai->k", stacked, vector, precision=lax.Precision.HIGHEST)
        dots = lax.psum(local_dots, "chain") / count
        vector = vector - jnp.einsum("k,kai->ai", dots, stacked, precision=lax.Precision.HIGHEST)
        squares = lax.psum(jnp.sum(vector * vector), "chain") / count
        length = jnp.sqrt(squares + EPS)
        basis.append(vector / length)
        hess = hess.at[: column + 1, column].set(dots).at[column + 1, column].set(length)
    return (jnp.stack(basis), hess)


class Plan:
    def __init__(self, devices, rows, depth):
        self.devices, self.rows, self.depth = devices, rows, depth
        self.piece = rows // devices
        self.near = [k for k in range(depth) if 2**k < rows]
        self.far = [k for k in range(depth) if rows <= 2**k < rows * devices]
        self.sent = len(self.near) - 1
        self.count = SUB * rows * devices
        n = len(self.far)
        self.own_mats = 2 * n + 4
        self.halo_mats = 2 * n + 1
        self.own_tiles = self.own_mats * SUB
        self.halo_tiles = self.halo_mats * SUB
        self.halo_packed = self.halo_tiles // 2
        self.coef_tiles = self.own_tiles + self.halo_packed
        self.per_group = rows // SUB
        tiles = self.coef_tiles + 4
        groups = -(-tiles // self.per_group)
        step = max(1, SUB // self.piece)
        self.groups = -(-groups // step) * step
        self.whole_groups = self.coef_tiles // self.per_group
        self.early = self.whole_groups * EARLY // 8 // step * step
        self.width = rows // self.piece


def fits(devices, rows, block, lanes=128):
    piece = rows // devices
    return block == SUB and rows == lanes and piece >= 1 and piece * devices == rows and rows // piece >= 4 * SUB


def lane(shape=(SUB, 128)):
    return lax.broadcasted_iota(jnp.int32, shape, 1)


def sub(shape=(SUB, 128)):
    return lax.broadcasted_iota(jnp.int32, shape, 0)


def spread(v, b):
    return jnp.broadcast_to(v[b : b + 1, :], v.shape)


def total(x):
    return jnp.sum(jnp.sum(x, axis=0, keepdims=True), axis=1, keepdims=True)


def send(plan, tiles, z_ref, out_ref):
    r = plan.rows
    stacked = jnp.concatenate(tiles + [jnp.zeros((r - SUB * len(tiles), r), jnp.float32)], 0)
    z_ref[...] = stacked.T
    out = z_ref[pl.ds(0, plan.devices, stride=plan.piece), :]
    for i in range(1, plan.piece):
        part = z_ref[pl.ds(i, plan.devices, stride=plan.piece), :]
        out = out + pltpu.roll(part, i * plan.width, 1)
    out_ref[...] = out


def receive(plan, in_ref, z_ref):
    got = in_ref[...]
    for i in range(plan.piece):
        part = got if i == 0 else pltpu.roll(got, plan.rows - i * plan.width, 1)
        z_ref[pl.ds(i, plan.devices, stride=plan.piece), :] = part
    t = z_ref[...].T
    return [t[SUB * k : SUB * k + SUB] for k in range(4)]


def halo_of(plan, y):
    pos = lane() % plan.piece
    before, after = pltpu.roll(y, 1, 1), pltpu.roll(y, plan.rows - 1, 1)
    return jnp.where(pos == 0, before, jnp.where(pos == plan.piece - 1, after, 0.0))


def wrapped(plan, x):
    q, r = plan.piece, plan.rows
    me = lax.axis_index(AXIS)
    at = lane()
    pos = at % q
    later = jnp.where(at == 0, 0.0, pltpu.roll(x, q, 1))
    sooner = jnp.where(at == r - 1, 0.0, pltpu.roll(x, r - q, 1))
    first = jnp.where(me == 0, later, x)
    last = jnp.where(me == plan.devices - 1, sooner, x)
    return jnp.where(pos == 0, first, jnp.where(pos == q - 1, last, 0.0))


def near_levels(plan, v, coef):
    r = plan.rows
    at = lane()
    for k in plan.near:
        s = 2**k
        turned = [pltpu.roll(x, s, 1) for x in v]
        back = [pltpu.roll(x, r - s, 1) for x in v]
        lower = [turned[0]] + [jnp.where(at < s, turned[t - 1], turned[t]) for t in (1, 2)]
        upper = [jnp.where(at >= r - s, back[t + 1], back[t]) for t in (0, 1)] + [back[2]]
        fresh = list(v)
        for t in (0, 1, 2) if k < plan.sent else (1,):
            low_sum = high_sum = None
            for b in range(SUB):
                low = coef(t, 0, k, b) * spread(lower[t], b)
                high = coef(t, 1, k, b) * spread(upper[t], b)
                low_sum = low if low_sum is None else low_sum + low
                high_sum = high if high_sum is None else high_sum + high
            fresh[t] = v[t] + low_sum + high_sum
        v = fresh
    return v[1]


def square_tile(u):
    return jnp.where(sub() == 0, jnp.broadcast_to(total(u * u), u.shape), 0.0)


def load_kernel(plan, *refs):
    count = (len(refs) - 2) // 2
    ins, outs, edge_ref, sems = refs[:count], refs[count:-2], refs[-2], refs[-1]
    rhs_ref, lo_ref, up_ref = ins[:3]
    n = 64 * plan.sent
    pairs = [
        (lo_ref.at[pl.ds(0, n)], edge_ref.at[pl.ds(0, n)]),
        (up_ref.at[pl.ds(0, n)], edge_ref.at[pl.ds(n, n)]),
        (rhs_ref, edge_ref.at[pl.ds(2 * n, SUB)]),
    ]
    pairs += list(zip(ins, outs))
    copies = [pltpu.make_async_copy(x, y, sems.at[i]) for i, (x, y) in enumerate(pairs)]
    for c in copies:
        c.start()
    for c in copies:
        c.wait()


def pack_tile(plan, raw, index):
    if index < plan.own_tiles:
        return raw(index)
    j = 2 * (index - plan.own_tiles)
    a, b = halo_of(plan, raw(j)), halo_of(plan, raw(j + 1))
    pos = lane() % plan.piece
    moved = jnp.where(pos == 1, pltpu.roll(b, 1, 1), pltpu.roll(b, plan.rows - 1, 1))
    return jnp.where((pos == 0) | (pos == plan.piece - 1), a, moved)


def pack_group(plan, at, rows, tiles, z_ref, slot, out_ref):
    z_ref[slot] = jnp.concatenate(tiles, 0).T
    for i in range(plan.piece):
        out_ref[pl.ds(at * plan.piece + i, plan.devices, stride=rows), :] = z_ref[
            slot, pl.ds(i, plan.devices, stride=plan.piece), :
        ]


def pack_kernel(plan, first, last, lo_ref, up_ref, fin_ref, dia_ref, bel_ref, abo_ref, out_ref, *rest):
    z_ref = rest[-1]
    mats = [(lo_ref, 64 * k) for k in plan.far] + [(up_ref, 64 * k) for k in plan.far]
    mats += [(fin_ref, 0), (dia_ref, 0), (bel_ref, 0), (abo_ref, 0)]

    def raw(index):
        ref, base = mats[index // SUB]
        return ref[pl.ds(base + index % SUB, SUB, stride=SUB), :]

    t = plan.per_group
    rows = out_ref.shape[0] // plan.devices
    for g in range(first, last):
        pack_group(plan, g - first, rows, [pack_tile(plan, raw, g * t + i) for i in range(t)], z_ref, g - first, out_ref)
    if len(rest) > 1:
        for i in range(last * t, plan.coef_tiles):
            rest[0][i - last * t] = pack_tile(plan, raw, i)


def first_kernel(
    plan, lo_ref, up_ref, rhs_ref, pair_ref, other_ref, rest_in_ref, chunk_ref, out_ref, coef_ref, field_ref, z_ref
):
    n = 64 * 2 * plan.sent
    odd = lax.rem(lax.axis_index(AXIS), 2) == 1
    rhs = rhs_ref[...]

    def halo(t, start, stride):
        a, b = pair_ref[pl.ds(start, SUB, stride=stride), :], other_ref[pl.ds(start, SUB, stride=stride), :]
        return jnp.where(odd, a, b) if t == 0 else jnp.where(odd, b, a)

    def coef(t, side, k, b):
        if t == 1:
            ref = up_ref if side else lo_ref
            x = ref[pl.ds(64 * k + b, SUB, stride=SUB), :]
        else:
            x = halo(t, 64 * (plan.sent * side + k) + b, SUB)
        coef_ref[t, side, k, b] = x
        return x

    fields = [halo(0, n, 1), rhs, halo(2, n, 1)]
    for t in range(3):
        field_ref[t] = fields[t]
    y = near_levels(plan, fields, coef)
    t = plan.per_group
    first = plan.whole_groups * t
    tiles = [rest_in_ref[i] for i in range(plan.coef_tiles - first)]
    tiles += [y, halo_of(plan, y), square_tile(rhs), rhs]
    tiles += [jnp.zeros_like(rhs)] * (plan.groups * t - first - len(tiles))
    rows = out_ref.shape[0] // plan.devices
    for g in range(plan.whole_groups, plan.groups):
        at, slot = g * t - first, g - plan.whole_groups
        pack_group(plan, g - plan.early, rows, tiles[at : at + t], z_ref, slot, out_ref)


def far_stage(plan, own, halo, coef_ref):
    q, r, n = plan.piece, plan.rows, len(plan.far)
    base = plan.own_tiles

    def apply(mat, x, start):
        out = coef_ref[start + mat * SUB] * spread(x, 0)
        for b in range(1, SUB):
            out = out + coef_ref[start + mat * SUB + b] * spread(x, b)
        return out

    for k in range(n):
        by = q * 2**k
        fresh = []
        for x, start in ((own, 0), (halo, base)):
            low = apply(k, pltpu.roll(x, by, 1), start)
            high = apply(n + k, pltpu.roll(x, r - by, 1), start)
            fresh.append(x + low + high)
        own, halo = fresh
    own = own + apply(2 * n, own, 0)
    halo = wrapped(plan, halo + apply(2 * n, halo, base))
    pos = lane() % q
    before = jnp.where(pos == 0, halo, pltpu.roll(own, 1, 1))
    after = jnp.where(pos == q - 1, halo, pltpu.roll(own, r - 1, 1))
    w = 2.0 * own + apply(2 * n + 1, own, 0)
    return w + apply(2 * n + 2, before, 0) + apply(2 * n + 3, after, 0)


def norm_of(plan, squares):
    pos = lane() % plan.piece
    one = jnp.where((pos == 0) & (sub() == 0), squares, 0.0)
    return jnp.sqrt(jnp.broadcast_to(total(one), one.shape) / plan.count + EPS)


def finish_far(plan, y, halo, s, vs, coef_ref, z_ref, out_ref):
    w = far_stage(plan, y / s, halo / s, coef_ref)
    q, r = plan.piece, plan.rows
    at = lane()
    before = jnp.where(at < q, 0.0, pltpu.roll(w, q, 1))
    after = jnp.where(at >= r - q, 0.0, pltpu.roll(w, r - q, 1))
    dots = jnp.zeros_like(w)
    for i, v in enumerate(vs):
        dots = jnp.where(sub() == i, jnp.broadcast_to(total(v * w), w.shape), dots)
    send(plan, [before, w, after, dots], z_ref, out_ref)
    return w


def two_sum(a, b):
    s = a + b
    t = s - a
    return s, (a - (s - t)) + (b - t)


def halves(a):
    c = 4097.0 * a
    hi = c - (c - a)
    return hi, a - hi


def two_prod(a, b):
    p = a * b
    ah, al = halves(a)
    bh, bl = halves(b)
    return p, ((ah * bh - p) + ah * bl + al * bh) + al * bl


def pair_add(x, y):
    s, e = two_sum(x[0], y[0])
    e = e + (x[1] + y[1])
    hi = s + e
    return hi, e - (hi - s)


def pair_mul(x, y):
    p, e = two_prod(x[0], y[0])
    e = e + (x[0] * y[1] + x[1] * y[0])
    hi = p + e
    return hi, e - (hi - p)


def folded(x, shifts, axis):
    for s in shifts:
        x = pair_add(x, tuple(pltpu.roll(a, s, axis) for a in x))
    return x


def products():
    out = [(i, None) for i in range(ITERS)] + [(None, None)]
    return out + [(i, j) for i in range(ITERS) for j in range(i, ITERS)]


def last_far_kernel(plan, in_ref, coef_ref, h_ref, w_in_ref, *rest):
    j = ITERS - 1
    vs = [v[...] for v in rest[:j]]
    out_ref, s_ref, zr_ref, zs_ref = rest[j:]
    y, halo, s, v = enter_far(plan, in_ref, h_ref, w_in_ref, vs, zr_ref)
    s_ref[...] = s
    vs = vs + [v]
    w = far_stage(plan, y / s, halo / s, coef_ref)
    sums = []
    for a, b in products():
        pair = two_prod(w if a is None else vs[a], w if b is None else vs[b])
        sums.append(folded(pair, (4, 2, 1), 0))
    at = sub()
    packed = []
    for start in range(0, len(sums), SUB):
        tile = [jnp.zeros_like(w), jnp.zeros_like(w)]
        for i, pair in enumerate(sums[start : start + SUB]):
            tile = [jnp.where(at == i, x, old) for x, old in zip(pair, tile)]
        packed.append(folded(tile, [2**i for i in range(plan.rows.bit_length() - 1)], 1))
    (hi, lo), (hi2, lo2) = packed
    last = jnp.where(at < SUB // 2, hi2, pltpu.roll(lo2, SUB // 2, 0))
    send(plan, [w, hi, lo, last], zs_ref, out_ref)


def start_far_kernel(plan, early_ref, late_ref, out_ref, coef_ref, w_ref, v_ref, s_ref, z_ref, zs_ref):
    q, r = plan.piece, plan.rows
    at = lane()
    pos = at % q
    n = len(plan.far)
    g_tiles = plan.per_group
    extra = []
    for g in range(plan.groups):
        in_ref, at_group = (early_ref, g) if g < plan.early else (late_ref, g - plan.early)
        rows = in_ref.shape[0] // plan.devices
        for i in range(q):
            z_ref[g, pl.ds(i, plan.devices, stride=q), :] = in_ref[
                pl.ds(at_group * q + i, plan.devices, stride=rows), :
            ]
        t = z_ref[g].T
        for j in range(g_tiles):
            index = g * g_tiles + j
            tile = t[SUB * j : SUB * j + SUB]

            def limited(x, mat):
                if mat < n:
                    return jnp.where(at < q * 2**mat, 0.0, x)
                if mat < 2 * n:
                    return jnp.where(at >= r - q * 2 ** (mat - n), 0.0, x)
                return x

            if index < plan.own_tiles:
                coef_ref[index] = limited(tile, index // SUB)
            elif index < plan.coef_tiles:
                k = 2 * (index - plan.own_tiles)
                other = jnp.where(pos == 0, pltpu.roll(tile, r - 1, 1), pltpu.roll(tile, 1, 1))
                coef_ref[plan.own_tiles + k] = limited(tile, k // SUB)
                coef_ref[plan.own_tiles + k + 1] = limited(other, (k + 1) // SUB)
            elif index < plan.coef_tiles + 4:
                extra.append(tile)
    y, halo, squares, rhs = extra
    s = norm_of(plan, squares)
    v = rhs / s
    v_ref[...] = v
    s_ref[...] = s
    w_ref[...] = finish_far(plan, y, halo, s, [v], coef_ref, zs_ref, out_ref)


def near_kernel(plan, j, in_ref, coef_ref, field_ref, *rest):
    us, ss = rest[: j - 1], rest[j - 1 : 2 * j - 1]
    out_ref, u_ref, h_ref, zr_ref, zs_ref = rest[2 * j - 1 :]
    *w, dots = receive(plan, in_ref, zr_ref)
    pos = lane() % plan.piece
    h = jnp.sum(jnp.where(pos == 0, dots, 0.0), axis=1, keepdims=True) / plan.count
    h = jnp.broadcast_to(h, dots.shape)
    h_ref[...] = h
    fields = [field_ref, *us]
    for t in range(3):
        acc = None
        for i in range(j):
            term = spread(h, i) * (fields[i][t] / ss[i][...])
            acc = term if acc is None else acc + term
        w[t] = w[t] - acc
        u_ref[t] = w[t]
    y = near_levels(plan, w, lambda t, side, k, b: coef_ref[t, side, k, b])
    send(plan, [y, halo_of(plan, y), square_tile(w[1])], zs_ref, out_ref)


def enter_far(plan, in_ref, h_ref, w_in_ref, vs, z_ref):
    y, halo, squares, _ = receive(plan, in_ref, z_ref)
    s = norm_of(plan, squares)
    h = h_ref[...]
    acc = None
    for i, v in enumerate(vs):
        term = spread(h, i) * v
        acc = term if acc is None else acc + term
    return y, halo, s, (w_in_ref[...] - acc) / s


def far_kernel(plan, j, in_ref, coef_ref, h_ref, w_in_ref, *rest):
    vs = [v[...] for v in rest[:j]]
    out_ref, w_ref, v_ref, s_ref, zr_ref, zs_ref = rest[j:]
    y, halo, s, v = enter_far(plan, in_ref, h_ref, w_in_ref, vs, zr_ref)
    v_ref[...] = v
    s_ref[...] = s
    w_ref[...] = finish_far(plan, y, halo, s, vs + [v], coef_ref, zs_ref, out_ref)


def output_kernel(plan, in_ref, field_ref, *rest):
    us = rest[: ITERS - 1]
    ss = [s[...] for s in rest[ITERS - 1 : 2 * ITERS - 1]]
    hs = [h[...] for h in rest[2 * ITERS - 1 : 3 * ITERS - 2]]
    basis_ref, hess_ref, z_ref = rest[3 * ITERS - 2 :]
    w, hi, lo, last = receive(plan, in_ref, z_ref)
    shifts = [plan.piece * 2**i for i in range(plan.devices.bit_length() - 1)]
    one = folded((hi, lo), shifts, 1)
    two = folded((last, pltpu.roll(last, SUB // 2, 0)), shifts, 1)
    sums = [tuple(x[i : i + 1] for x in one) for i in range(SUB)]
    sums += [tuple(x[i : i + 1] for x in two) for i in range(SUB // 2)]
    names = products()
    got = dict(zip(names, sums))
    h = [got[i, None][0] / plan.count for i in range(ITERS)]
    zero = jnp.zeros_like(h[0])
    squares = got[None, None]
    for i in range(ITERS):
        left = tuple(2.0 * x for x in got[i, None])
        for j in range(ITERS):
            left = pair_add(left, pair_mul((-h[j], zero), got[min(i, j), max(i, j)]))
        squares = pair_add(squares, pair_mul((-h[i], zero), left))
    squares = jnp.maximum(squares[0], 0.0)
    wide = lambda x: jnp.broadcast_to(x, (SUB, plan.rows))
    ss.append(wide(jnp.sqrt(squares / plan.count + EPS)))
    fields = [field_ref[1]] + [u[1] for u in us]
    vs = [f / s for f, s in zip(fields, ss)]
    acc = None
    for i in range(ITERS):
        term = wide(h[i]) * vs[i]
        acc = term if acc is None else acc + term
    vs.append((w - acc) / ss[-1])
    for j in range(ITERS + 1):
        basis_ref[j] = vs[j]
    top = jnp.zeros_like(w)
    for i in range(ITERS):
        top = jnp.where(sub() == i, wide(h[i]), top)
    hs.append(top)
    hess = jnp.zeros_like(w)
    for j in range(ITERS):
        col = jnp.where(sub() <= j, hs[j], jnp.where(sub() == j + 1, ss[j + 1], 0.0))
        hess = jnp.where(lane() == j, col, hess)
    hess_ref[...] = hess[: ITERS + 1, :ITERS]


def transposed(
    plan, right_side, diag_block, below_block, above_block, lower_level, upper_level, final_block
):
    r, d = plan.rows, plan.devices
    flat = lambda x: x.reshape(-1, r)
    lo, up, fin = flat(lower_level), flat(upper_level), flat(final_block)
    dia, bel, abo = flat(diag_block), flat(below_block), flat(above_block)
    shape = lambda *s: jax.ShapeDtypeStruct(s, jnp.float32)
    tile = shape(SUB, r)
    scratch = lambda *s: pltpu.VMEM(s, jnp.float32)

    def call(kernel, outs, scratches, *args, space=pltpu.VMEM, flops=1_000_000, **more):
        return pl.pallas_call(
            kernel,
            out_shape=outs,
            in_specs=[pl.BlockSpec(memory_space=space)] * len(args),
            out_specs=jax.tree.map(lambda _: pl.BlockSpec(memory_space=pltpu.VMEM), outs),
            scratch_shapes=scratches,
            compiler_params=pltpu.CompilerParams(vmem_limit_bytes=24 * 2**20),
            cost_estimate=pl.CostEstimate(flops=flops, bytes_accessed=1_000_000, transcendentals=0),
            **more,
        )(*args)

    def exchange(x):
        y = lax.all_to_all(x.reshape(d, -1, r), AXIS, 0, 0)
        return y.reshape(-1, r)

    part = functools.partial
    raw = tuple(pltpu.with_memory_space_constraint(x, pltpu.HBM) for x in (right_side, lo, up, fin, dia, bel, abo))
    *loaded, edge = call(
        part(load_kernel, plan),
        (*(shape(*x.shape) for x in raw), shape(64 * 2 * plan.sent + SUB, r)),
        [pltpu.SemaphoreType.DMA((len(raw) + 3,))],
        *raw,
        space=pltpu.HBM,
    )
    rhs, lo, up = loaded[:3]
    mats = loaded[1:]
    other = lax.ppermute(edge, AXIS, [(i, i + 1 if i % 2 else i - 1) for i in range(1, d - 1)])
    pair = lax.ppermute(edge, AXIS, [(i, i ^ 1) for i in range(d)])
    rows_of = lambda groups: d * groups * plan.piece
    early = call(
        part(pack_kernel, plan, 0, plan.early),
        shape(rows_of(plan.early), r),
        [scratch(plan.early, r, r)],
        *mats,
        flops=10_000_000,
    )
    early = exchange(early)
    left = plan.coef_tiles - plan.whole_groups * plan.per_group
    late_shape = shape(rows_of(plan.groups - plan.early), r)
    late, rest = call(
        part(pack_kernel, plan, plan.early, plan.whole_groups),
        (late_shape, shape(max(left, 1), SUB, r)),
        [scratch(plan.whole_groups - plan.early, r, r)],
        *mats,
        flops=10_000_000,
    )
    late, near, fields = call(
        part(first_kernel, plan),
        (late_shape, shape(3, 2, len(plan.near), SUB, SUB, r), shape(3, SUB, r)),
        [scratch(plan.groups - plan.whole_groups, r, r)],
        lo, up, rhs, pair, other, rest, late,
        input_output_aliases={6: 0},
    )
    small = shape(d, r)
    two = [scratch(r, r), scratch(r, r)]
    out, coef, w, v, s = call(
        part(start_far_kernel, plan),
        (small, shape(plan.own_tiles + plan.halo_tiles, SUB, r), tile, tile, tile),
        [scratch(plan.groups, r, r), scratch(r, r)],
        early, exchange(late),
    )
    us, ss, vs, hs = [], [s], [v], []
    for j in range(1, ITERS):
        out, u, h = call(
            part(near_kernel, plan, j),
            (small, shape(3, SUB, r), tile),
            two,
            exchange(out), near, fields, *us, *ss,
        )
        us.append(u)
        hs.append(h)
        if j < ITERS - 1:
            out, w, v, s = call(
                part(far_kernel, plan, j), (small, tile, tile, tile), two, exchange(out), coef, h, w, *vs
            )
            vs.append(v)
        else:
            out, s = call(part(last_far_kernel, plan), (small, tile), two, exchange(out), coef, h, w, *vs)
        ss.append(s)
    return call(
        part(output_kernel, plan),
        (shape(ITERS + 1, SUB, r), shape(ITERS + 1, ITERS)),
        [scratch(r, r)],
        exchange(out), fields, *us, *ss, *hs,
    )


def on_device(*args):
    right_side, lower_level = args[0], args[4]
    devices, rows = lax.axis_size(AXIS), right_side.shape[1]
    if not fits(devices, rows, right_side.shape[0]):
        return general(*args)
    return tuple(transposed(Plan(devices, rows, lower_level.shape[0]), *args))


def solution(mesh):
    return jax.shard_map(
        on_device,
        mesh=mesh,
        in_specs=(
            P(None, "chain"),
            P(None, None, "chain"),
            P(None, None, "chain"),
            P(None, None, "chain"),
            P(None, None, None, "chain"),
            P(None, None, None, "chain"),
            P(None, None, "chain"),
        ),
        out_specs=(P(None, None, "chain"), P()),
        check_vma=False,
    )
```

```python
import functools

import jax
import jax.numpy as jnp
from jax import lax
from jax.experimental import pallas as pl
from jax.experimental.pallas import tpu as pltpu
from jax.sharding import PartitionSpec as P


ITERS = 3


EPS = 1e-06
AXIS = "chain"
SUB = 8
EARLY = 5


def padded_2(x, sides, width):
    for axis, dim in sides:
        peers, length = (lax.axis_size(axis), x.shape[dim])
        up = [(i, (i + 1) % peers) for i in range(peers - 1)]
        down = [(j, i) for i, j in up]
        last = lax.slice_in_dim(x, length - width, length, axis=dim)
        initial = lax.slice_in_dim(x, 0, width, axis=dim)
        before = lax.ppermute(last, axis, up)
        after = lax.ppermute(initial, axis, down)
        x = jnp.concatenate([before, x, after], axis=dim)
    return x


def from_behind(x, axis, by):
    peers = lax.axis_size(axis)
    pairs = [(i, i + by) for i in range(peers) if 0 <= i + by < peers]
    return lax.ppermute(x, axis, pairs)


def blockmul(blocks, field):
    return jnp.einsum("abi,bi->ai", blocks, field, precision=lax.Precision.HIGHEST)


def general(
    right_side, diag_block, below_block, above_block, lower_level, upper_level, final_block
):
    rows_here = right_side.shape[1]
    devices = lax.axis_size("chain")
    whole = rows_here * devices
    count = right_side.shape[0] * whole
    depth = lower_level.shape[0]
    near = [level for level in range(depth) if 2**level < rows_here]
    far = [level for level in range(depth) if 2**level >= rows_here and 2**level < whole]
    reach = sum((2**level for level in near))
    stacked_coef = jnp.concatenate([lower_level[: len(near)], upper_level[: len(near)]], 0)
    wide_coef = padded_2(stacked_coef, (("chain", 3),), reach)
    start_sum = lax.psum(jnp.sum(right_side * right_side), "chain")
    basis = [right_side / jnp.sqrt(start_sum / count + EPS)]
    hess = jnp.zeros((ITERS + 1, ITERS), jnp.float32)
    for column in range(ITERS):
        precondition_field = basis[column]
        current = padded_2(precondition_field, (("chain", 1),), reach)
        offset = 0
        for position in range(len(near)):
            stride = 2 ** near[position]
            length = current.shape[1]
            first_col = offset + stride
            last_col = offset + length - stride
            low_coef = wide_coef[position][:, :, first_col:last_col]
            high_coef = wide_coef[len(near) + position][:, :, first_col:last_col]
            current = (
                current[:, stride : length - stride]
                + blockmul(low_coef, current[:, : length - 2 * stride])
                + blockmul(high_coef, current[:, 2 * stride :])
            )
            offset = first_col
        precondition_field = current
        for precondition_level in far:
            hops = 2**precondition_level // rows_here
            below_rows = from_behind(precondition_field, "chain", hops)
            above_rows = from_behind(precondition_field, "chain", -hops)
            precondition_field = (
                precondition_field
                + blockmul(lower_level[precondition_level], below_rows)
                + blockmul(upper_level[precondition_level], above_rows)
            )
        field = precondition_field + blockmul(final_block, precondition_field)
        padded = padded_2(field, (("chain", 1),), 1)
        result = 2.0 * field + blockmul(diag_block, field)
        result = result + blockmul(below_block, padded[:, :rows_here])
        vector = result + blockmul(above_block, padded[:, 2:])
        stacked = jnp.stack(basis)
        local_dots = jnp.einsum("kai,ai->k", stacked, vector, precision=lax.Precision.HIGHEST)
        dots = lax.psum(local_dots, "chain") / count
        vector = vector - jnp.einsum("k,kai->ai", dots, stacked, precision=lax.Precision.HIGHEST)
        squares = lax.psum(jnp.sum(vector * vector), "chain") / count
        length = jnp.sqrt(squares + EPS)
        basis.append(vector / length)
        hess = hess.at[: column + 1, column].set(dots).at[column + 1, column].set(length)
    return (jnp.stack(basis), hess)


class Plan:
    def __init__(self, devices, rows, depth):
        self.devices, self.rows, self.depth = devices, rows, depth
        self.piece = rows // devices
        self.near = [k for k in range(depth) if 2**k < rows]
        self.far = [k for k in range(depth) if rows <= 2**k < rows * devices]
        self.sent = len(self.near) - 1
        self.count = SUB * rows * devices
        n = len(self.far) - 1
        self.halo_mats = 2 * n + 2
        self.own_mats = self.halo_mats + 3
        self.own_tiles = self.own_mats * SUB
        self.halo_tiles = self.halo_mats * SUB
        self.coef_tiles = self.own_tiles + self.halo_tiles // 2
        self.per_group = rows // SUB
        self.groups = -(-self.coef_tiles // self.per_group)
        self.early = self.groups * EARLY // 9
        self.early_rows = self.early * self.piece
        self.late_rows = (self.groups - self.early) * self.piece + 1
        self.width = rows // self.piece


def fits(devices, rows, block, lanes=128):
    piece = rows // devices
    return block == SUB and rows == lanes and piece >= 1 and piece * devices == rows and rows // piece >= 4 * SUB


def lane(shape=(SUB, 128)):
    return lax.broadcasted_iota(jnp.int32, shape, 1)


def sub(shape=(SUB, 128)):
    return lax.broadcasted_iota(jnp.int32, shape, 0)


def spread(v, b):
    return jnp.broadcast_to(v[b : b + 1, :], v.shape)


def total(x):
    return jnp.sum(jnp.sum(x, axis=0, keepdims=True), axis=1, keepdims=True)


def send(plan, tiles, z_ref, row=None):
    n = plan.width - SUB * len(tiles)
    filler = [jnp.zeros((n, plan.rows), jnp.float32)] if n else []
    z_ref[...] = jnp.concatenate((tiles + filler) * plan.piece, 0).T
    group = lane((plan.devices, plan.rows)) // plan.width
    out = z_ref[pl.ds(0, plan.devices, stride=plan.piece), :]
    for i in range(1, plan.piece):
        part = z_ref[pl.ds(i, plan.devices, stride=plan.piece), :]
        out = jnp.where(group == i, part, out)
    return out if row is None else out + row


def receive(plan, got, z_ref):
    for i in range(plan.piece):
        z_ref[pl.ds(i, plan.devices, stride=plan.piece), :] = got
    t = z_ref[...].T
    pos = lane() % plan.piece
    tiles = []
    for k in range(4):
        at = SUB * k
        tile = t[at : at + SUB]
        for i in range(1, plan.piece):
            tile = jnp.where(pos == i, t[i * plan.width + at : i * plan.width + at + SUB], tile)
        tiles.append(tile)
    return tiles


def halo_of(plan, y):
    pos = lane() % plan.piece
    before, after = pltpu.roll(y, 1, 1), pltpu.roll(y, plan.rows - 1, 1)
    return jnp.where(pos == 0, before, jnp.where(pos == plan.piece - 1, after, 0.0))


def wrapped(plan, x):
    q, r = plan.piece, plan.rows
    me = lax.axis_index(AXIS)
    at = lane()
    pos = at % q
    later = jnp.where(at == 0, 0.0, pltpu.roll(x, q, 1))
    sooner = jnp.where(at == r - 1, 0.0, pltpu.roll(x, r - q, 1))
    first = jnp.where(me == 0, later, x)
    last = jnp.where(me == plan.devices - 1, sooner, x)
    return jnp.where(pos == 0, first, jnp.where(pos == q - 1, last, 0.0))


def near_levels(plan, v, coef):
    r = plan.rows
    at = lane()
    for k in plan.near:
        s = 2**k
        turned = [pltpu.roll(x, s, 1) for x in v]
        back = [pltpu.roll(x, r - s, 1) for x in v]
        lower = [turned[0]] + [jnp.where(at < s, turned[t - 1], turned[t]) for t in (1, 2)]
        upper = [jnp.where(at >= r - s, back[t + 1], back[t]) for t in (0, 1)] + [back[2]]
        fresh = list(v)
        for t in (0, 1, 2) if k < plan.sent else (1,):
            low_sum = high_sum = None
            for b in range(SUB):
                low = coef(t, 0, k, b) * spread(lower[t], b)
                high = coef(t, 1, k, b) * spread(upper[t], b)
                low_sum = low if low_sum is None else low_sum + low
                high_sum = high if high_sum is None else high_sum + high
            fresh[t] = v[t] + low_sum + high_sum
        v = fresh
    return v[1]


def square_tile(u):
    return jnp.where(sub() == 0, jnp.broadcast_to(total(u * u), u.shape), 0.0)


def load_kernel(plan, *refs):
    count = (len(refs) - 3) // 2
    ins, outs, edge_refs, sems = refs[:count], refs[count:-3], refs[-3:-1], refs[-1]
    rhs_ref, lo_ref, up_ref = ins[:3]
    n = 64 * plan.sent
    pairs = []
    for edge_ref in edge_refs:
        pairs += [
            (lo_ref.at[pl.ds(0, n)], edge_ref.at[pl.ds(0, n)]),
            (up_ref.at[pl.ds(0, n)], edge_ref.at[pl.ds(n, n)]),
            (rhs_ref, edge_ref.at[pl.ds(2 * n, SUB)]),
        ]
    pairs += list(zip(ins, outs))
    copies = [pltpu.make_async_copy(x, y, sems.at[i]) for i, (x, y) in enumerate(pairs)]
    for c in copies:
        c.start()
    for c in copies:
        c.wait()


def take_kernel(in_ref, out_ref):
    out_ref[...] = in_ref[...]


def pack_kernel(plan, first, last, lo_ref, up_ref, fin_ref, dia_ref, bel_ref, abo_ref, out_ref, z_ref):
    half = lax.axis_index(AXIS) >= plan.devices // 2
    *most, top = plan.far
    mats = [(lo_ref, 64 * k) for k in most] + [(up_ref, 64 * k) for k in most] + [None]
    mats += [(fin_ref, 0), (dia_ref, 0), (bel_ref, 0), (abo_ref, 0)]

    def raw(index):
        mat, b = divmod(index, SUB)
        if mats[mat] is None:
            low, high = (ref[pl.ds(64 * top + b, SUB, stride=SUB), :] for ref in (lo_ref, up_ref))
            return jnp.where(half, low, high)
        ref, base = mats[mat]
        return ref[pl.ds(base + b, SUB, stride=SUB), :]

    def tile(index):
        if index < plan.own_tiles:
            return raw(index)
        if index >= plan.coef_tiles:
            return jnp.zeros((SUB, plan.rows), jnp.float32)
        j = 2 * (index - plan.own_tiles)
        a, b = halo_of(plan, raw(j)), halo_of(plan, raw(j + 1))
        pos = lane() % plan.piece
        moved = jnp.where(pos == 1, pltpu.roll(b, 1, 1), pltpu.roll(b, plan.rows - 1, 1))
        return jnp.where((pos == 0) | (pos == plan.piece - 1), a, moved)

    t = plan.per_group
    rows = out_ref.shape[0] // plan.devices
    for slot, g in enumerate(range(first, last)):
        z_ref[slot] = jnp.concatenate([tile(g * t + i) for i in range(t)], 0).T
        for i in range(plan.piece):
            out_ref[pl.ds(slot * plan.piece + i, plan.devices, stride=rows), :] = z_ref[
                slot, pl.ds(i, plan.devices, stride=plan.piece), :
            ]


def first_kernel(
    plan, lo_ref, up_ref, rhs_ref, pair_ref, other_ref, late_ref, out_ref, coef_ref, field_ref, z_ref
):
    n = 64 * 2 * plan.sent
    odd = lax.rem(lax.axis_index(AXIS), 2) == 1
    rhs = rhs_ref[...]

    def halo(t, start, stride):
        a, b = pair_ref[pl.ds(start, SUB, stride=stride), :], other_ref[pl.ds(start, SUB, stride=stride), :]
        return jnp.where(odd, a, b) if t == 0 else jnp.where(odd, b, a)

    def coef(t, side, k, b):
        if t == 1:
            ref = up_ref if side else lo_ref
            x = ref[pl.ds(64 * k + b, SUB, stride=SUB), :]
        else:
            x = halo(t, 64 * (plan.sent * side + k) + b, SUB)
        coef_ref[t, side, k, b] = x
        return x

    fields = [halo(0, n, 1), rhs, halo(2, n, 1)]
    for t in range(3):
        field_ref[t] = fields[t]
    y = near_levels(plan, fields, coef)
    out_ref[pl.ds(plan.late_rows - 1, plan.devices, stride=plan.late_rows), :] = send(
        plan, [y, halo_of(plan, y), square_tile(rhs), rhs], z_ref
    )


def far_stage(plan, own, halo, coef_ref):
    q, r, n = plan.piece, plan.rows, len(plan.far) - 1
    base = plan.own_tiles

    def apply(mat, x, start):
        out = coef_ref[start + mat * SUB] * spread(x, 0)
        for b in range(1, SUB):
            out = out + coef_ref[start + mat * SUB + b] * spread(x, b)
        return out

    for k in range(n):
        by = q * 2**k
        fresh = []
        for x, start in ((own, 0), (halo, base)):
            low = apply(k, pltpu.roll(x, by, 1), start)
            high = apply(n + k, pltpu.roll(x, r - by, 1), start)
            fresh.append(x + low + high)
        own, halo = fresh
    own, halo = (x + apply(2 * n, pltpu.roll(x, r // 2, 1), start) for x, start in ((own, 0), (halo, base)))
    own = own + apply(2 * n + 1, own, 0)
    halo = wrapped(plan, halo + apply(2 * n + 1, halo, base))
    pos = lane() % q
    before = jnp.where(pos == 0, halo, pltpu.roll(own, 1, 1))
    after = jnp.where(pos == q - 1, halo, pltpu.roll(own, r - 1, 1))
    w = 2.0 * own + apply(2 * n + 2, own, 0)
    return w + apply(2 * n + 3, before, 0) + apply(2 * n + 4, after, 0)


def norm_of(plan, squares):
    pos = lane() % plan.piece
    one = jnp.where((pos == 0) & (sub() == 0), squares, 0.0)
    return jnp.sqrt(jnp.broadcast_to(total(one), one.shape) / plan.count + EPS)


def finish_far(plan, y, halo, s, vs, coef_ref, z_ref, out_ref):
    w = far_stage(plan, y, halo, coef_ref) / s
    q, r = plan.piece, plan.rows
    at = lane()
    before = jnp.where(at < q, 0.0, pltpu.roll(w, q, 1))
    after = jnp.where(at >= r - q, 0.0, pltpu.roll(w, r - q, 1))
    dots = jnp.zeros_like(w)
    for i, v in enumerate(vs):
        dots = jnp.where(sub() == i, jnp.broadcast_to(total(v * w), w.shape), dots)
    out_ref[...] = send(plan, [before, w, after, dots], z_ref)
    return w


def two_sum(a, b):
    s = a + b
    t = s - a
    return s, (a - (s - t)) + (b - t)


def halves(a):
    c = 4097.0 * a
    hi = c - (c - a)
    return hi, a - hi


def two_prod(a, b):
    p = a * b
    ah, al = halves(a)
    bh, bl = halves(b)
    return p, ((ah * bh - p) + ah * bl + al * bh) + al * bl


def pair_add(x, y):
    s, e = two_sum(x[0], y[0])
    e = e + (x[1] + y[1])
    hi = s + e
    return hi, e - (hi - s)


def pair_mul(x, y):
    p, e = two_prod(x[0], y[0])
    e = e + (x[0] * y[1] + x[1] * y[0])
    hi = p + e
    return hi, e - (hi - p)


def folded(x, shifts, axis):
    for s in shifts:
        x = pair_add(x, tuple(pltpu.roll(a, s, axis) for a in x))
    return x


def products():
    out = [(i, None) for i in range(ITERS)] + [(None, None)]
    return out + [(i, j) for i in range(ITERS) for j in range(i, ITERS)]


def rows_sum(pair):
    parts = [tuple(x[SUB * i : SUB * i + SUB] for x in pair) for i in range(pair[0].shape[0] // SUB)]
    while len(parts) > 1:
        half = len(parts) // 2
        parts = [pair_add(a, b) for a, b in zip(parts[:half], parts[half:])]
    one = folded(parts[0], (4, 2, 1), 0)
    return tuple(x[0:1] for x in one)


def last_far_kernel(plan, in_ref, coef_ref, h_ref, w_in_ref, *rest):
    j = ITERS - 1
    vs = [v[...] for v in rest[:j]]
    out_ref, s_ref, zr_ref, zs_ref = rest[j:]
    y, halo, s, v = enter_far(plan, in_ref, h_ref, w_in_ref, vs, zr_ref)
    s_ref[...] = s
    vs = vs + [v]
    w = far_stage(plan, y, halo, coef_ref) / s
    at = sub((2 * SUB, plan.rows))
    packed = [jnp.zeros((2 * SUB, plan.rows), jnp.float32)] * 2
    for i, (a, b) in enumerate(products()):
        pair = two_prod(w if a is None else vs[a], w if b is None else vs[b])
        pair = folded(pair, (4, 2, 1), 0)
        packed = [jnp.where(at == i, jnp.concatenate([x, x], 0), old) for x, old in zip(pair, packed)]
    filler = jnp.zeros((plan.rows - 2 * SUB, plan.rows), jnp.float32)
    hi, lo = rows_sum(tuple(jnp.concatenate([x, filler], 0).T for x in packed))
    hi, lo = (jnp.concatenate([x] * SUB, 0) for x in (hi, lo))
    row = pltpu.roll(hi, SUB, 1) + pltpu.roll(lo, SUB + len(products()), 1)
    out_ref[...] = send(plan, [w], zs_ref, row[0:1])


def start_far_kernel(plan, early_ref, late_ref, out_ref, coef_ref, w_ref, v_ref, s_ref, z_ref, zr_ref, zs_ref):
    q, r = plan.piece, plan.rows
    at = lane()
    pos = at % q
    n = len(plan.far) - 1

    def limited(x, mat):
        if mat < n:
            return jnp.where(at < q * 2**mat, 0.0, x)
        if mat < 2 * n:
            return jnp.where(at >= r - q * 2 ** (mat - n), 0.0, x)
        return x

    for g in range(plan.groups):
        in_ref, slot, rows = (early_ref, g, plan.early_rows)
        if g >= plan.early:
            in_ref, slot, rows = (late_ref, g - plan.early, plan.late_rows)
        for i in range(q):
            z_ref[g, pl.ds(i, plan.devices, stride=q), :] = in_ref[
                pl.ds(slot * q + i, plan.devices, stride=rows), :
            ]
        t = z_ref[g].T
        for j in range(plan.per_group):
            index = g * plan.per_group + j
            tile = t[SUB * j : SUB * j + SUB]
            if index < plan.own_tiles:
                coef_ref[index] = limited(tile, index // SUB)
            elif index < plan.coef_tiles:
                k = 2 * (index - plan.own_tiles)
                other = jnp.where(pos == 0, pltpu.roll(tile, r - 1, 1), pltpu.roll(tile, 1, 1))
                coef_ref[plan.own_tiles + k] = limited(tile, k // SUB)
                coef_ref[plan.own_tiles + k + 1] = limited(other, (k + 1) // SUB)
    got = late_ref[pl.ds(plan.late_rows - 1, plan.devices, stride=plan.late_rows), :]
    y, halo, squares, rhs = receive(plan, got, zr_ref)
    s = norm_of(plan, squares)
    v = rhs / s
    v_ref[...] = v
    s_ref[...] = s
    w_ref[...] = finish_far(plan, y, halo, s, [v], coef_ref, zs_ref, out_ref)


def near_kernel(plan, j, in_ref, coef_ref, field_ref, *rest):
    us, ss = rest[: j - 1], rest[j - 1 : 2 * j - 1]
    out_ref, u_ref, h_ref, zr_ref, zs_ref = rest[2 * j - 1 :]
    *w, dots = receive(plan, in_ref[...], zr_ref)
    pos = lane() % plan.piece
    h = jnp.sum(jnp.where(pos == 0, dots, 0.0), axis=1, keepdims=True) / plan.count
    h = jnp.broadcast_to(h, dots.shape)
    h_ref[...] = h
    fields = [field_ref, *us]
    for t in range(3):
        acc = None
        for i in range(j):
            term = spread(h, i) * (fields[i][t] / ss[i][...])
            acc = term if acc is None else acc + term
        w[t] = w[t] - acc
        u_ref[t] = w[t]
    y = near_levels(plan, w, lambda t, side, k, b: coef_ref[t, side, k, b])
    out_ref[...] = send(plan, [y, halo_of(plan, y), square_tile(w[1])], zs_ref)


def enter_far(plan, in_ref, h_ref, w_in_ref, vs, z_ref):
    y, halo, squares, _ = receive(plan, in_ref[...], z_ref)
    s = norm_of(plan, squares)
    h = h_ref[...]
    acc = None
    for i, v in enumerate(vs):
        term = spread(h, i) * v
        acc = term if acc is None else acc + term
    return y, halo, s, (w_in_ref[...] - acc) / s


def far_kernel(plan, j, in_ref, coef_ref, h_ref, w_in_ref, *rest):
    vs = [v[...] for v in rest[:j]]
    out_ref, w_ref, v_ref, s_ref, zr_ref, zs_ref = rest[j:]
    y, halo, s, v = enter_far(plan, in_ref, h_ref, w_in_ref, vs, zr_ref)
    v_ref[...] = v
    s_ref[...] = s
    w_ref[...] = finish_far(plan, y, halo, s, vs + [v], coef_ref, zs_ref, out_ref)


def output_kernel(plan, in_ref, field_ref, *rest):
    us = rest[: ITERS - 1]
    ss = [s[...] for s in rest[ITERS - 1 : 2 * ITERS - 1]]
    hs = [h[...] for h in rest[2 * ITERS - 1 : 3 * ITERS - 2]]
    basis_ref, hess_ref, z_ref = rest[3 * ITERS - 2 :]
    raw = in_ref[...]
    low = pltpu.roll(raw, plan.rows - len(products()), 1)
    row = rows_sum((raw, low))
    w = receive(plan, in_ref[...], z_ref)[0]
    wide = lambda x: jnp.broadcast_to(x, (SUB, plan.rows))
    sums = [tuple(wide(x[:, SUB + i : SUB + i + 1]) for x in row) for i in range(len(products()))]
    names = products()
    got = dict(zip(names, sums))
    h = [got[i, None][0] / plan.count for i in range(ITERS)]
    zero = jnp.zeros_like(h[0])
    squares = got[None, None]
    for i in range(ITERS):
        left = tuple(2.0 * x for x in got[i, None])
        for j in range(ITERS):
            left = pair_add(left, pair_mul((-h[j], zero), got[min(i, j), max(i, j)]))
        squares = pair_add(squares, pair_mul((-h[i], zero), left))
    squares = jnp.maximum(squares[0], 0.0)
    ss.append(jnp.sqrt(squares / plan.count + EPS))
    fields = [field_ref[1]] + [u[1] for u in us]
    vs = [f / s for f, s in zip(fields, ss)]
    acc = None
    for i in range(ITERS):
        term = h[i] * vs[i]
        acc = term if acc is None else acc + term
    vs.append((w - acc) / ss[-1])
    for j in range(ITERS + 1):
        basis_ref[j] = vs[j]
    top = jnp.zeros_like(w)
    for i in range(ITERS):
        top = jnp.where(sub() == i, h[i], top)
    hs.append(top)
    hess = jnp.zeros_like(w)
    for j in range(ITERS):
        col = jnp.where(sub() <= j, hs[j], jnp.where(sub() == j + 1, ss[j + 1], 0.0))
        hess = jnp.where(lane() == j, col, hess)
    hess_ref[...] = hess[: ITERS + 1, :ITERS]


def transposed(
    plan, right_side, diag_block, below_block, above_block, lower_level, upper_level, final_block
):
    r, d = plan.rows, plan.devices
    flat = lambda x: x.reshape(-1, r)
    lo, up, fin = flat(lower_level), flat(upper_level), flat(final_block)
    dia, bel, abo = flat(diag_block), flat(below_block), flat(above_block)
    shape = lambda *s: jax.ShapeDtypeStruct(s, jnp.float32)
    tile = shape(SUB, r)
    scratch = lambda *s: pltpu.VMEM(s, jnp.float32)

    def call(kernel, outs, scratches, *args, space=pltpu.VMEM, flops=1_000_000, **more):
        return pl.pallas_call(
            kernel,
            out_shape=outs,
            in_specs=[pl.BlockSpec(memory_space=space)] * len(args),
            out_specs=jax.tree.map(lambda _: pl.BlockSpec(memory_space=pltpu.VMEM), outs),
            scratch_shapes=scratches,
            compiler_params=pltpu.CompilerParams(vmem_limit_bytes=24 * 2**20),
            cost_estimate=pl.CostEstimate(flops=flops, bytes_accessed=1_000_000, transcendentals=0),
            **more,
        )(*args)

    def exchange(x):
        y = lax.all_to_all(x.reshape(-1, 1, r), AXIS, 0, 0, tiled=True)
        return y.reshape(-1, r)

    part = functools.partial
    raw = tuple(pltpu.with_memory_space_constraint(x, pltpu.HBM) for x in (right_side, lo, up, fin, dia, bel, abo))
    edge = shape(64 * 2 * plan.sent + SUB, r)
    *loaded, edge_across, edge_pair = call(
        part(load_kernel, plan),
        (*(shape(*x.shape) for x in raw), edge, edge),
        [pltpu.SemaphoreType.DMA((len(raw) + 6,))],
        *raw,
        space=pltpu.HBM,
    )
    rhs, lo, up = loaded[:3]
    mats = loaded[1:]
    other = lax.ppermute(edge_across, AXIS, [(i, i + 1 if i % 2 else i - 1) for i in range(1, d - 1)])
    pair = lax.ppermute(edge_pair, AXIS, [(i, i ^ 1) for i in range(d)])
    pair = call(take_kernel, edge, [], pair)
    early = call(
        part(pack_kernel, plan, 0, plan.early),
        shape(d * plan.early_rows, r),
        [scratch(plan.early, r, r)],
        *mats,
        flops=10_000_000,
    )
    early = exchange(early)
    late_shape = shape(d * plan.late_rows, r)
    late = call(
        part(pack_kernel, plan, plan.early, plan.groups),
        late_shape,
        [scratch(plan.groups - plan.early, r, r)],
        *mats,
        flops=10_000_000,
    )
    late, near, fields = call(
        part(first_kernel, plan),
        (late_shape, shape(3, 2, len(plan.near), SUB, SUB, r), shape(3, SUB, r)),
        [scratch(r, r)],
        lo, up, rhs, pair, other, late,
        input_output_aliases={5: 0},
    )
    small = shape(d, r)
    two = [scratch(r, r), scratch(r, r)]
    out, coef, w, v, s = call(
        part(start_far_kernel, plan),
        (small, shape(plan.own_tiles + plan.halo_tiles, SUB, r), tile, tile, tile),
        [scratch(plan.groups, r, r), *two],
        early, exchange(late),
    )
    us, ss, vs, hs = [], [s], [v], []
    for j in range(1, ITERS):
        out, u, h = call(
            part(near_kernel, plan, j),
            (small, shape(3, SUB, r), tile),
            two,
            exchange(out), near, fields, *us, *ss,
        )
        us.append(u)
        hs.append(h)
        if j < ITERS - 1:
            out, w, v, s = call(
                part(far_kernel, plan, j), (small, tile, tile, tile), two, exchange(out), coef, h, w, *vs
            )
            vs.append(v)
        else:
            out, s = call(part(last_far_kernel, plan), (small, tile), two, exchange(out), coef, h, w, *vs)
        ss.append(s)
    return call(
        part(output_kernel, plan),
        (shape(ITERS + 1, SUB, r), shape(ITERS + 1, ITERS)),
        [scratch(r, r)],
        exchange(out), fields, *us, *ss, *hs,
    )


def on_device(*args):
    right_side, lower_level = args[0], args[4]
    devices, rows = lax.axis_size(AXIS), right_side.shape[1]
    if not fits(devices, rows, right_side.shape[0]):
        return general(*args)
    return tuple(transposed(Plan(devices, rows, lower_level.shape[0]), *args))


def solution(mesh):
    return jax.shard_map(
        on_device,
        mesh=mesh,
        in_specs=(
            P(None, "chain"),
            P(None, None, "chain"),
            P(None, None, "chain"),
            P(None, None, "chain"),
            P(None, None, None, "chain"),
            P(None, None, None, "chain"),
            P(None, None, "chain"),
        ),
        out_specs=(P(None, None, "chain"), P()),
        check_vma=False,
    )
```

```python
import functools

import jax
import jax.numpy as jnp
from jax import lax
from jax.experimental import pallas as pl
from jax.experimental.pallas import tpu as pltpu
from jax.sharding import PartitionSpec as P


ITERS = 3


EPS = 1e-06
AXIS = "chain"
SUB = 8
EARLY = 5


def padded_2(x, sides, width):
    for axis, dim in sides:
        peers, length = (lax.axis_size(axis), x.shape[dim])
        up = [(i, (i + 1) % peers) for i in range(peers - 1)]
        down = [(j, i) for i, j in up]
        last = lax.slice_in_dim(x, length - width, length, axis=dim)
        initial = lax.slice_in_dim(x, 0, width, axis=dim)
        before = lax.ppermute(last, axis, up)
        after = lax.ppermute(initial, axis, down)
        x = jnp.concatenate([before, x, after], axis=dim)
    return x


def from_behind(x, axis, by):
    peers = lax.axis_size(axis)
    pairs = [(i, i + by) for i in range(peers) if 0 <= i + by < peers]
    return lax.ppermute(x, axis, pairs)


def blockmul(blocks, field):
    return jnp.einsum("abi,bi->ai", blocks, field, precision=lax.Precision.HIGHEST)


def general(
    right_side, diag_block, below_block, above_block, lower_level, upper_level, final_block
):
    rows_here = right_side.shape[1]
    devices = lax.axis_size("chain")
    whole = rows_here * devices
    count = right_side.shape[0] * whole
    depth = lower_level.shape[0]
    near = [level for level in range(depth) if 2**level < rows_here]
    far = [level for level in range(depth) if 2**level >= rows_here and 2**level < whole]
    reach = sum((2**level for level in near))
    stacked_coef = jnp.concatenate([lower_level[: len(near)], upper_level[: len(near)]], 0)
    wide_coef = padded_2(stacked_coef, (("chain", 3),), reach)
    start_sum = lax.psum(jnp.sum(right_side * right_side), "chain")
    basis = [right_side / jnp.sqrt(start_sum / count + EPS)]
    hess = jnp.zeros((ITERS + 1, ITERS), jnp.float32)
    for column in range(ITERS):
        precondition_field = basis[column]
        current = padded_2(precondition_field, (("chain", 1),), reach)
        offset = 0
        for position in range(len(near)):
            stride = 2 ** near[position]
            length = current.shape[1]
            first_col = offset + stride
            last_col = offset + length - stride
            low_coef = wide_coef[position][:, :, first_col:last_col]
            high_coef = wide_coef[len(near) + position][:, :, first_col:last_col]
            current = (
                current[:, stride : length - stride]
                + blockmul(low_coef, current[:, : length - 2 * stride])
                + blockmul(high_coef, current[:, 2 * stride :])
            )
            offset = first_col
        precondition_field = current
        for precondition_level in far:
            hops = 2**precondition_level // rows_here
            below_rows = from_behind(precondition_field, "chain", hops)
            above_rows = from_behind(precondition_field, "chain", -hops)
            precondition_field = (
                precondition_field
                + blockmul(lower_level[precondition_level], below_rows)
                + blockmul(upper_level[precondition_level], above_rows)
            )
        field = precondition_field + blockmul(final_block, precondition_field)
        padded = padded_2(field, (("chain", 1),), 1)
        result = 2.0 * field + blockmul(diag_block, field)
        result = result + blockmul(below_block, padded[:, :rows_here])
        vector = result + blockmul(above_block, padded[:, 2:])
        stacked = jnp.stack(basis)
        local_dots = jnp.einsum("kai,ai->k", stacked, vector, precision=lax.Precision.HIGHEST)
        dots = lax.psum(local_dots, "chain") / count
        vector = vector - jnp.einsum("k,kai->ai", dots, stacked, precision=lax.Precision.HIGHEST)
        squares = lax.psum(jnp.sum(vector * vector), "chain") / count
        length = jnp.sqrt(squares + EPS)
        basis.append(vector / length)
        hess = hess.at[: column + 1, column].set(dots).at[column + 1, column].set(length)
    return (jnp.stack(basis), hess)


class Plan:
    def __init__(self, devices, rows, depth):
        self.devices, self.rows, self.depth = devices, rows, depth
        self.piece = rows // devices
        self.near = [k for k in range(depth) if 2**k < rows]
        self.far = [k for k in range(depth) if rows <= 2**k < rows * devices]
        self.sent = len(self.near) - 1
        self.count = SUB * rows * devices
        n = len(self.far) - 1
        self.halo_mats = 2 * n + 2
        self.own_mats = self.halo_mats + 3
        self.own_tiles = self.own_mats * SUB
        self.halo_tiles = self.halo_mats * SUB
        self.coef_tiles = self.own_tiles + self.halo_tiles // 2
        self.per_group = rows // SUB
        self.groups = -(-self.coef_tiles // self.per_group)
        self.early = self.groups * EARLY // 9
        self.early_rows = self.early * self.piece
        self.late_rows = (self.groups - self.early) * self.piece + 1
        self.width = rows // self.piece


def fits(devices, rows, block, lanes=128):
    piece = rows // devices
    return block == SUB and rows == lanes and piece >= 1 and piece * devices == rows and rows // piece >= 4 * SUB


def lane(shape=(SUB, 128)):
    return lax.broadcasted_iota(jnp.int32, shape, 1)


def sub(shape=(SUB, 128)):
    return lax.broadcasted_iota(jnp.int32, shape, 0)


def spread(v, b):
    return jnp.broadcast_to(v[b : b + 1, :], v.shape)


def total(x):
    return jnp.sum(jnp.sum(x, axis=0, keepdims=True), axis=1, keepdims=True)


def send(plan, tiles, z_ref, wrap=False, row=None, sums=None):
    q, r = plan.piece, plan.rows
    n = plan.width - SUB * len(tiles)
    filler = [jnp.zeros((n, r), jnp.float32)] if n else []
    z = jnp.concatenate(([t for t, _ in tiles] + filler) * q, 0).T
    pad = jnp.zeros((SUB, r), jnp.float32)
    z_ref[pl.ds(0, SUB), :] = z[r - SUB :] if wrap else pad
    z_ref[pl.ds(SUB, r), :] = z
    z_ref[pl.ds(SUB + r, SUB), :] = z[:SUB] if wrap else pad
    place = lane((plan.devices, r)) // SUB
    out = jnp.zeros((plan.devices, r), jnp.float32)
    for i in range(q):
        loads = {}
        for k, (_, offsets) in enumerate(tiles):
            if offsets is None or offsets[i] is None:
                continue
            if offsets[i] not in loads:
                loads[offsets[i]] = z_ref[pl.ds(SUB + i + offsets[i], plan.devices, stride=q), :]
            out = jnp.where(place == i * (plan.width // SUB) + k, loads[offsets[i]], out)
    if sums is not None:
        parts = [z[SUB * i : SUB * i + SUB] for i in range(r // SUB)]
        while len(parts) > 1:
            parts = [x + y for x, y in zip(parts[::2], parts[1::2])]
        whole = jnp.broadcast_to(jnp.sum(parts[0], axis=0, keepdims=True), out.shape)
        out = jnp.where(place == sums, whole, out)
    return out if row is None else out + row


def sent_field(plan, y):
    q = plan.piece
    return [(y, (0,) * q), (y, (-1,) + (None,) * (q - 2) + (1,))]


def receive(plan, got, z_ref):
    for i in range(plan.piece):
        z_ref[pl.ds(i, plan.devices, stride=plan.piece), :] = got
    t = z_ref[...].T
    pos = lane() % plan.piece
    tiles = []
    for k in range(4):
        at = SUB * k
        tile = t[at : at + SUB]
        for i in range(1, plan.piece):
            tile = jnp.where(pos == i, t[i * plan.width + at : i * plan.width + at + SUB], tile)
        tiles.append(tile)
    return tiles


def halo_of(plan, y):
    pos = lane() % plan.piece
    before, after = pltpu.roll(y, 1, 1), pltpu.roll(y, plan.rows - 1, 1)
    return jnp.where(pos == 0, before, jnp.where(pos == plan.piece - 1, after, 0.0))


def wrapped(plan, x):
    q, r = plan.piece, plan.rows
    me = lax.axis_index(AXIS)
    at = lane()
    pos = at % q
    later = jnp.where(at == 0, 0.0, pltpu.roll(x, q, 1))
    sooner = jnp.where(at == r - 1, 0.0, pltpu.roll(x, r - q, 1))
    first = jnp.where(me == 0, later, x)
    last = jnp.where(me == plan.devices - 1, sooner, x)
    return jnp.where(pos == 0, first, jnp.where(pos == q - 1, last, 0.0))


def near_levels(plan, v, coef):
    r = plan.rows
    at = lane()
    for k in plan.near:
        s = 2**k
        turned = [pltpu.roll(x, s, 1) for x in v]
        back = [pltpu.roll(x, r - s, 1) for x in v]
        lower = [turned[0]] + [jnp.where(at < s, turned[t - 1], turned[t]) for t in (1, 2)]
        upper = [jnp.where(at >= r - s, back[t + 1], back[t]) for t in (0, 1)] + [back[2]]
        fresh = list(v)
        for t in (0, 1, 2) if k < plan.sent else (1,):
            low_sum = high_sum = None
            for b in range(SUB):
                low = coef(t, 0, k, b) * spread(lower[t], b)
                high = coef(t, 1, k, b) * spread(upper[t], b)
                low_sum = low if low_sum is None else low_sum + low
                high_sum = high if high_sum is None else high_sum + high
            fresh[t] = v[t] + low_sum + high_sum
        v = fresh
    return v[1]


def square_tile(u):
    return jnp.where(sub() == 0, jnp.broadcast_to(total(u * u), u.shape), 0.0)


def load_kernel(plan, *refs):
    count = (len(refs) - 3) // 2
    ins, outs, edge_refs, sems = refs[:count], refs[count:-3], refs[-3:-1], refs[-1]
    copies = [pltpu.make_async_copy(x, y, sems.at[i]) for i, (x, y) in enumerate(zip(ins, outs))]
    for c in copies:
        c.start()
    for c in copies:
        c.wait()
    rhs_ref, lo_ref, up_ref = outs[:3]
    n = 64 * (plan.sent - 1)
    odd = lax.rem(lax.axis_index(AXIS), 2) == 1
    first = lane((64, plan.rows)) < plan.rows // 2
    low = lo_ref[pl.ds(n, 64), :]
    high = pltpu.roll(up_ref[pl.ds(n, 64), :], plan.rows // 2, 1)
    as_prev, as_next = jnp.where(first, high, low), jnp.where(first, low, high)
    across_ref, pair_ref = edge_refs
    across_ref[pl.ds(2 * n, 64), :] = jnp.where(odd, as_prev, as_next)
    pair_ref[pl.ds(2 * n, 64), :] = jnp.where(odd, as_next, as_prev)
    for ref in edge_refs:
        ref[pl.ds(0, n), :] = lo_ref[pl.ds(0, n), :]
        ref[pl.ds(n, n), :] = up_ref[pl.ds(0, n), :]
        ref[pl.ds(2 * n + 64, SUB), :] = rhs_ref[...]


def take_kernel(in_ref, out_ref):
    out_ref[...] = in_ref[...]


def pack_kernel(plan, first, last, lo_ref, up_ref, fin_ref, dia_ref, bel_ref, abo_ref, out_ref, z_ref):
    half = lax.axis_index(AXIS) >= plan.devices // 2
    *most, top = plan.far
    mats = [(lo_ref, 64 * k) for k in most] + [(up_ref, 64 * k) for k in most] + [None]
    mats += [(fin_ref, 0), (dia_ref, 0), (bel_ref, 0), (abo_ref, 0)]

    def raw(index):
        mat, b = divmod(index, SUB)
        if mats[mat] is None:
            low, high = (ref[pl.ds(64 * top + b, SUB, stride=SUB), :] for ref in (lo_ref, up_ref))
            return jnp.where(half, low, high)
        ref, base = mats[mat]
        return ref[pl.ds(base + b, SUB, stride=SUB), :]

    def tile(index):
        if index < plan.own_tiles:
            return raw(index)
        if index >= plan.coef_tiles:
            return jnp.zeros((SUB, plan.rows), jnp.float32)
        j = 2 * (index - plan.own_tiles)
        a, b = halo_of(plan, raw(j)), halo_of(plan, raw(j + 1))
        pos = lane() % plan.piece
        moved = jnp.where(pos == 1, pltpu.roll(b, 1, 1), pltpu.roll(b, plan.rows - 1, 1))
        return jnp.where((pos == 0) | (pos == plan.piece - 1), a, moved)

    t = plan.per_group
    rows = out_ref.shape[0] // plan.devices
    for slot, g in enumerate(range(first, last)):
        z_ref[slot] = jnp.concatenate([tile(g * t + i) for i in range(t)], 0).T
        for i in range(plan.piece):
            out_ref[pl.ds(slot * plan.piece + i, plan.devices, stride=rows), :] = z_ref[
                slot, pl.ds(i, plan.devices, stride=plan.piece), :
            ]


def first_kernel(
    plan, lo_ref, up_ref, rhs_ref, pair_ref, other_ref, late_ref, out_ref, coef_ref, field_ref, z_ref
):
    last = plan.sent - 1
    n = 64 * (2 * last + 1)
    odd = lax.rem(lax.axis_index(AXIS), 2) == 1
    rhs = rhs_ref[...]

    def halo(t, start, stride):
        a, b = pair_ref[pl.ds(start, SUB, stride=stride), :], other_ref[pl.ds(start, SUB, stride=stride), :]
        return jnp.where(odd, a, b) if t == 0 else jnp.where(odd, b, a)

    def coef(t, side, k, b):
        if t == 1:
            ref = up_ref if side else lo_ref
            x = ref[pl.ds(64 * k + b, SUB, stride=SUB), :]
        elif k < last:
            x = halo(t, 64 * (last * side + k) + b, SUB)
        else:
            x = halo(t, 64 * 2 * last + b, SUB)
            x = pltpu.roll(x, plan.rows // 2, 1) if side else x
        coef_ref[t, side, k, b] = x
        return x

    fields = [halo(0, n, 1), rhs, halo(2, n, 1)]
    for t in range(3):
        field_ref[t] = fields[t]
    y = near_levels(plan, fields, coef)
    plain = (0,) * plan.piece
    out_ref[pl.ds(plan.late_rows - 1, plan.devices, stride=plan.late_rows), :] = send(
        plan, [*sent_field(plan, y), (square_tile(rhs), plain), (rhs, plain)], z_ref, wrap=True
    )


def far_stage(plan, own, halo, coef_ref):
    q, r, n = plan.piece, plan.rows, len(plan.far) - 1
    base = plan.own_tiles

    def apply(mat, x, start):
        out = coef_ref[start + mat * SUB] * spread(x, 0)
        for b in range(1, SUB):
            out = out + coef_ref[start + mat * SUB + b] * spread(x, b)
        return out

    for k in range(n):
        by = q * 2**k
        fresh = []
        for x, start in ((own, 0), (halo, base)):
            low = apply(k, pltpu.roll(x, by, 1), start)
            high = apply(n + k, pltpu.roll(x, r - by, 1), start)
            fresh.append(x + low + high)
        own, halo = fresh
    own, halo = (x + apply(2 * n, pltpu.roll(x, r // 2, 1), start) for x, start in ((own, 0), (halo, base)))
    own = own + apply(2 * n + 1, own, 0)
    halo = wrapped(plan, halo + apply(2 * n + 1, halo, base))
    pos = lane() % q
    before = jnp.where(pos == 0, halo, pltpu.roll(own, 1, 1))
    after = jnp.where(pos == q - 1, halo, pltpu.roll(own, r - 1, 1))
    w = 2.0 * own + apply(2 * n + 2, own, 0)
    return w + apply(2 * n + 3, before, 0) + apply(2 * n + 4, after, 0)


def norm_of(plan, squares):
    pos = lane() % plan.piece
    one = jnp.where((pos == 0) & (sub() == 0), squares, 0.0)
    return jnp.sqrt(jnp.broadcast_to(total(one), one.shape) / plan.count + EPS)


def finish_far(plan, y, halo, s, vs, coef_ref, z_ref, out_ref):
    w = far_stage(plan, y, halo, coef_ref) / s
    q = plan.piece
    dots = jnp.zeros_like(w)
    for i, v in enumerate(vs):
        dots = jnp.where(sub() == i, jnp.sum(v * w, axis=0, keepdims=True), dots)
    tiles = [(w, (by,) * q) for by in (-q, 0, q)] + [(dots, None)]
    out_ref[...] = send(plan, tiles, z_ref, sums=3)
    return w


def two_sum(a, b):
    s = a + b
    t = s - a
    return s, (a - (s - t)) + (b - t)


def halves(a):
    c = 4097.0 * a
    hi = c - (c - a)
    return hi, a - hi


def two_prod(a, b):
    p = a * b
    ah, al = halves(a)
    bh, bl = halves(b)
    return p, ((ah * bh - p) + ah * bl + al * bh) + al * bl


def pair_add(x, y):
    s, e = two_sum(x[0], y[0])
    e = e + (x[1] + y[1])
    hi = s + e
    return hi, e - (hi - s)


def pair_mul(x, y):
    p, e = two_prod(x[0], y[0])
    e = e + (x[0] * y[1] + x[1] * y[0])
    hi = p + e
    return hi, e - (hi - p)


def folded(x, shifts, axis):
    for s in shifts:
        x = pair_add(x, tuple(pltpu.roll(a, s, axis) for a in x))
    return x


def products():
    out = [(i, None) for i in range(ITERS)] + [(None, None)]
    return out + [(i, j) for i in range(ITERS) for j in range(i, ITERS)]


def rows_sum(pair):
    parts = [tuple(x[SUB * i : SUB * i + SUB] for x in pair) for i in range(pair[0].shape[0] // SUB)]
    while len(parts) > 1:
        half = len(parts) // 2
        parts = [pair_add(a, b) for a, b in zip(parts[:half], parts[half:])]
    one = folded(parts[0], (4, 2, 1), 0)
    return tuple(x[0:1] for x in one)


def last_far_kernel(plan, in_ref, coef_ref, h_ref, w_in_ref, *rest):
    j = ITERS - 1
    vs = [v[...] for v in rest[:j]]
    out_ref, s_ref, zr_ref, zs_ref = rest[j:]
    y, halo, s, v = enter_far(plan, in_ref, h_ref, w_in_ref, vs, zr_ref)
    s_ref[...] = s
    vs = vs + [v]
    w = far_stage(plan, y, halo, coef_ref) / s
    at = sub((2 * SUB, plan.rows))
    packed = [jnp.zeros((2 * SUB, plan.rows), jnp.float32)] * 2
    for i, (a, b) in enumerate(products()):
        pair = two_prod(w if a is None else vs[a], w if b is None else vs[b])
        pair = folded(pair, (4, 2, 1), 0)
        packed = [jnp.where(at == i, jnp.concatenate([x, x], 0), old) for x, old in zip(pair, packed)]
    filler = jnp.zeros((plan.rows - 2 * SUB, plan.rows), jnp.float32)
    hi, lo = rows_sum(tuple(jnp.concatenate([x, filler], 0).T for x in packed))
    hi, lo = (jnp.concatenate([x] * SUB, 0) for x in (hi, lo))
    row = pltpu.roll(hi, SUB, 1) + pltpu.roll(lo, SUB + len(products()), 1)
    out_ref[...] = send(plan, [(w, (0,) * plan.piece)], zs_ref, row=row[0:1])


def start_far_kernel(plan, early_ref, late_ref, out_ref, coef_ref, w_ref, v_ref, s_ref, z_ref, zr_ref, zs_ref):
    q, r = plan.piece, plan.rows
    at = lane()
    pos = at % q
    n = len(plan.far) - 1

    def limited(x, mat):
        if mat < n:
            return jnp.where(at < q * 2**mat, 0.0, x)
        if mat < 2 * n:
            return jnp.where(at >= r - q * 2 ** (mat - n), 0.0, x)
        return x

    for g in range(plan.groups):
        in_ref, slot, rows = (early_ref, g, plan.early_rows)
        if g >= plan.early:
            in_ref, slot, rows = (late_ref, g - plan.early, plan.late_rows)
        for i in range(q):
            z_ref[g, pl.ds(i, plan.devices, stride=q), :] = in_ref[
                pl.ds(slot * q + i, plan.devices, stride=rows), :
            ]
        t = z_ref[g].T
        for j in range(plan.per_group):
            index = g * plan.per_group + j
            tile = t[SUB * j : SUB * j + SUB]
            if index < plan.own_tiles:
                coef_ref[index] = limited(tile, index // SUB)
            elif index < plan.coef_tiles:
                k = 2 * (index - plan.own_tiles)
                other = jnp.where(pos == 0, pltpu.roll(tile, r - 1, 1), pltpu.roll(tile, 1, 1))
                coef_ref[plan.own_tiles + k] = limited(tile, k // SUB)
                coef_ref[plan.own_tiles + k + 1] = limited(other, (k + 1) // SUB)
    got = late_ref[pl.ds(plan.late_rows - 1, plan.devices, stride=plan.late_rows), :]
    y, halo, squares, rhs = receive(plan, got, zr_ref)
    s = norm_of(plan, squares)
    v = rhs / s
    v_ref[...] = v
    s_ref[...] = s
    w_ref[...] = finish_far(plan, y, halo, s, [v], coef_ref, zs_ref, out_ref)


def near_kernel(plan, j, in_ref, coef_ref, field_ref, *rest):
    us, ss = rest[: j - 1], rest[j - 1 : 2 * j - 1]
    out_ref, u_ref, h_ref, zr_ref, zs_ref = rest[2 * j - 1 :]
    got = in_ref[...]
    dots = jnp.sum(got, axis=0, keepdims=True) / plan.count
    h = [jnp.broadcast_to(dots[:, 3 * SUB + i : 3 * SUB + i + 1], (SUB, plan.rows)) for i in range(j)]
    w = receive(plan, got, zr_ref)[:3]
    tall = jnp.zeros_like(h[0])
    for i in range(j):
        tall = jnp.where(sub() == i, h[i], tall)
    h_ref[...] = tall
    fields = [field_ref, *us]
    for t in range(3):
        acc = None
        for i in range(j):
            term = h[i] * (fields[i][t] / ss[i][...])
            acc = term if acc is None else acc + term
        w[t] = w[t] - acc
        u_ref[t] = w[t]
    y = near_levels(plan, w, lambda t, side, k, b: coef_ref[t, side, k, b])
    out_ref[...] = send(plan, [*sent_field(plan, y), (square_tile(w[1]), (0,) * plan.piece)], zs_ref, wrap=True)


def enter_far(plan, in_ref, h_ref, w_in_ref, vs, z_ref):
    y, halo, squares, _ = receive(plan, in_ref[...], z_ref)
    s = norm_of(plan, squares)
    h = h_ref[...]
    acc = None
    for i, v in enumerate(vs):
        term = spread(h, i) * v
        acc = term if acc is None else acc + term
    return y, halo, s, (w_in_ref[...] - acc) / s


def far_kernel(plan, j, in_ref, coef_ref, h_ref, w_in_ref, *rest):
    vs = [v[...] for v in rest[:j]]
    out_ref, w_ref, v_ref, s_ref, zr_ref, zs_ref = rest[j:]
    y, halo, s, v = enter_far(plan, in_ref, h_ref, w_in_ref, vs, zr_ref)
    v_ref[...] = v
    s_ref[...] = s
    w_ref[...] = finish_far(plan, y, halo, s, vs + [v], coef_ref, zs_ref, out_ref)


def output_kernel(plan, in_ref, field_ref, *rest):
    us = rest[: ITERS - 1]
    ss = [s[...] for s in rest[ITERS - 1 : 2 * ITERS - 1]]
    hs = [h[...] for h in rest[2 * ITERS - 1 : 3 * ITERS - 2]]
    basis_ref, hess_ref, z_ref = rest[3 * ITERS - 2 :]
    raw = in_ref[...]
    low = pltpu.roll(raw, plan.rows - len(products()), 1)
    row = rows_sum((raw, low))
    w = receive(plan, in_ref[...], z_ref)[0]
    wide = lambda x: jnp.broadcast_to(x, (SUB, plan.rows))
    sums = [tuple(wide(x[:, SUB + i : SUB + i + 1]) for x in row) for i in range(len(products()))]
    names = products()
    got = dict(zip(names, sums))
    h = [got[i, None][0] / plan.count for i in range(ITERS)]
    zero = jnp.zeros_like(h[0])
    squares = got[None, None]
    for i in range(ITERS):
        left = tuple(2.0 * x for x in got[i, None])
        for j in range(ITERS):
            left = pair_add(left, pair_mul((-h[j], zero), got[min(i, j), max(i, j)]))
        squares = pair_add(squares, pair_mul((-h[i], zero), left))
    squares = jnp.maximum(squares[0], 0.0)
    ss.append(jnp.sqrt(squares / plan.count + EPS))
    fields = [field_ref[1]] + [u[1] for u in us]
    vs = [f / s for f, s in zip(fields, ss)]
    acc = None
    for i in range(ITERS):
        term = h[i] * vs[i]
        acc = term if acc is None else acc + term
    vs.append((w - acc) / ss[-1])
    for j in range(ITERS + 1):
        basis_ref[j] = vs[j]
    top = jnp.zeros_like(w)
    for i in range(ITERS):
        top = jnp.where(sub() == i, h[i], top)
    hs.append(top)
    hess = jnp.zeros_like(w)
    for j in range(ITERS):
        col = jnp.where(sub() <= j, hs[j], jnp.where(sub() == j + 1, ss[j + 1], 0.0))
        hess = jnp.where(lane() == j, col, hess)
    hess_ref[...] = hess[: ITERS + 1, :ITERS]


def transposed(
    plan, right_side, diag_block, below_block, above_block, lower_level, upper_level, final_block
):
    r, d = plan.rows, plan.devices
    flat = lambda x: x.reshape(-1, r)
    lo, up, fin = flat(lower_level), flat(upper_level), flat(final_block)
    dia, bel, abo = flat(diag_block), flat(below_block), flat(above_block)
    shape = lambda *s: jax.ShapeDtypeStruct(s, jnp.float32)
    tile = shape(SUB, r)
    scratch = lambda *s: pltpu.VMEM(s, jnp.float32)

    def call(kernel, outs, scratches, *args, space=pltpu.VMEM, flops=1_000_000, **more):
        return pl.pallas_call(
            kernel,
            out_shape=outs,
            in_specs=[pl.BlockSpec(memory_space=space)] * len(args),
            out_specs=jax.tree.map(lambda _: pl.BlockSpec(memory_space=pltpu.VMEM), outs),
            scratch_shapes=scratches,
            compiler_params=pltpu.CompilerParams(vmem_limit_bytes=24 * 2**20),
            cost_estimate=pl.CostEstimate(flops=flops, bytes_accessed=1_000_000, transcendentals=0),
            **more,
        )(*args)

    def exchange(x):
        y = lax.all_to_all(x.reshape(-1, 1, r), AXIS, 0, 0, tiled=True)
        return y.reshape(-1, r)

    part = functools.partial
    raw = tuple(pltpu.with_memory_space_constraint(x, pltpu.HBM) for x in (right_side, lo, up, fin, dia, bel, abo))
    edge = shape(64 * (2 * plan.sent - 1) + SUB, r)
    *loaded, edge_across, edge_pair = call(
        part(load_kernel, plan),
        (*(shape(*x.shape) for x in raw), edge, edge),
        [pltpu.SemaphoreType.DMA((len(raw),))],
        *raw,
        space=pltpu.HBM,
    )
    rhs, lo, up = loaded[:3]
    mats = loaded[1:]
    other = lax.ppermute(edge_across, AXIS, [(i, i + 1 if i % 2 else i - 1) for i in range(1, d - 1)])
    pair = lax.ppermute(edge_pair, AXIS, [(i, i ^ 1) for i in range(d)])
    pair = call(take_kernel, edge, [], pair)
    early = call(
        part(pack_kernel, plan, 0, plan.early),
        shape(d * plan.early_rows, r),
        [scratch(plan.early, r, r)],
        *mats,
        flops=10_000_000,
    )
    early = exchange(early)
    late_shape = shape(d * plan.late_rows, r)
    late = call(
        part(pack_kernel, plan, plan.early, plan.groups),
        late_shape,
        [scratch(plan.groups - plan.early, r, r)],
        *mats,
        flops=10_000_000,
    )
    late, near, fields = call(
        part(first_kernel, plan),
        (late_shape, shape(3, 2, len(plan.near), SUB, SUB, r), shape(3, SUB, r)),
        [scratch(r + 2 * SUB, r)],
        lo, up, rhs, pair, other, late,
        input_output_aliases={5: 0},
    )
    small = shape(d, r)
    padded = scratch(r + 2 * SUB, r)
    two = [scratch(r, r), padded]
    out, coef, w, v, s = call(
        part(start_far_kernel, plan),
        (small, shape(plan.own_tiles + plan.halo_tiles, SUB, r), tile, tile, tile),
        [scratch(plan.groups, r, r), *two],
        early, exchange(late),
    )
    us, ss, vs, hs = [], [s], [v], []
    for j in range(1, ITERS):
        out, u, h = call(
            part(near_kernel, plan, j),
            (small, shape(3, SUB, r), tile),
            two,
            exchange(out), near, fields, *us, *ss,
        )
        us.append(u)
        hs.append(h)
        if j < ITERS - 1:
            out, w, v, s = call(
                part(far_kernel, plan, j), (small, tile, tile, tile), two, exchange(out), coef, h, w, *vs
            )
            vs.append(v)
        else:
            out, s = call(part(last_far_kernel, plan), (small, tile), two, exchange(out), coef, h, w, *vs)
        ss.append(s)
    return call(
        part(output_kernel, plan),
        (shape(ITERS + 1, SUB, r), shape(ITERS + 1, ITERS)),
        [scratch(r, r)],
        exchange(out), fields, *us, *ss, *hs,
    )


def on_device(*args):
    right_side, lower_level = args[0], args[4]
    devices, rows = lax.axis_size(AXIS), right_side.shape[1]
    if not fits(devices, rows, right_side.shape[0]):
        return general(*args)
    return tuple(transposed(Plan(devices, rows, lower_level.shape[0]), *args))


def solution(mesh):
    return jax.shard_map(
        on_device,
        mesh=mesh,
        in_specs=(
            P(None, "chain"),
            P(None, None, "chain"),
            P(None, None, "chain"),
            P(None, None, "chain"),
            P(None, None, None, "chain"),
            P(None, None, None, "chain"),
            P(None, None, "chain"),
        ),
        out_specs=(P(None, None, "chain"), P()),
        check_vma=False,
    )
```

```python
import functools

import jax
import jax.numpy as jnp
from jax import lax
from jax.experimental import pallas as pl
from jax.experimental.pallas import tpu as pltpu
from jax.sharding import PartitionSpec as P


ITERS = 3


EPS = 1e-06
AXIS = "chain"
SUB = 8


def padded_2(x, sides, width):
    for axis, dim in sides:
        peers, length = (lax.axis_size(axis), x.shape[dim])
        up = [(i, (i + 1) % peers) for i in range(peers - 1)]
        down = [(j, i) for i, j in up]
        last = lax.slice_in_dim(x, length - width, length, axis=dim)
        initial = lax.slice_in_dim(x, 0, width, axis=dim)
        before = lax.ppermute(last, axis, up)
        after = lax.ppermute(initial, axis, down)
        x = jnp.concatenate([before, x, after], axis=dim)
    return x


def from_behind(x, axis, by):
    peers = lax.axis_size(axis)
    pairs = [(i, i + by) for i in range(peers) if 0 <= i + by < peers]
    return lax.ppermute(x, axis, pairs)


def blockmul(blocks, field):
    return jnp.einsum("abi,bi->ai", blocks, field, precision=lax.Precision.HIGHEST)


def general(
    right_side, diag_block, below_block, above_block, lower_level, upper_level, final_block
):
    rows_here = right_side.shape[1]
    devices = lax.axis_size("chain")
    whole = rows_here * devices
    count = right_side.shape[0] * whole
    depth = lower_level.shape[0]
    near = [level for level in range(depth) if 2**level < rows_here]
    far = [level for level in range(depth) if 2**level >= rows_here and 2**level < whole]
    reach = sum((2**level for level in near))
    stacked_coef = jnp.concatenate([lower_level[: len(near)], upper_level[: len(near)]], 0)
    wide_coef = padded_2(stacked_coef, (("chain", 3),), reach)
    start_sum = lax.psum(jnp.sum(right_side * right_side), "chain")
    basis = [right_side / jnp.sqrt(start_sum / count + EPS)]
    hess = jnp.zeros((ITERS + 1, ITERS), jnp.float32)
    for column in range(ITERS):
        precondition_field = basis[column]
        current = padded_2(precondition_field, (("chain", 1),), reach)
        offset = 0
        for position in range(len(near)):
            stride = 2 ** near[position]
            length = current.shape[1]
            first_col = offset + stride
            last_col = offset + length - stride
            low_coef = wide_coef[position][:, :, first_col:last_col]
            high_coef = wide_coef[len(near) + position][:, :, first_col:last_col]
            current = (
                current[:, stride : length - stride]
                + blockmul(low_coef, current[:, : length - 2 * stride])
                + blockmul(high_coef, current[:, 2 * stride :])
            )
            offset = first_col
        precondition_field = current
        for precondition_level in far:
            hops = 2**precondition_level // rows_here
            below_rows = from_behind(precondition_field, "chain", hops)
            above_rows = from_behind(precondition_field, "chain", -hops)
            precondition_field = (
                precondition_field
                + blockmul(lower_level[precondition_level], below_rows)
                + blockmul(upper_level[precondition_level], above_rows)
            )
        field = precondition_field + blockmul(final_block, precondition_field)
        padded = padded_2(field, (("chain", 1),), 1)
        result = 2.0 * field + blockmul(diag_block, field)
        result = result + blockmul(below_block, padded[:, :rows_here])
        vector = result + blockmul(above_block, padded[:, 2:])
        stacked = jnp.stack(basis)
        local_dots = jnp.einsum("kai,ai->k", stacked, vector, precision=lax.Precision.HIGHEST)
        dots = lax.psum(local_dots, "chain") / count
        vector = vector - jnp.einsum("k,kai->ai", dots, stacked, precision=lax.Precision.HIGHEST)
        squares = lax.psum(jnp.sum(vector * vector), "chain") / count
        length = jnp.sqrt(squares + EPS)
        basis.append(vector / length)
        hess = hess.at[: column + 1, column].set(dots).at[column + 1, column].set(length)
    return (jnp.stack(basis), hess)


class Plan:
    def __init__(self, devices, rows, depth):
        self.devices, self.rows, self.depth = devices, rows, depth
        self.piece = rows // devices
        self.near = [k for k in range(depth) if 2**k < rows]
        self.far = [k for k in range(depth) if rows <= 2**k < rows * devices]
        self.sent = len(self.near) - 1
        self.count = SUB * rows * devices
        n = len(self.far) - 1
        self.halo_mats = 2 * n + 2
        self.own_mats = self.halo_mats + 3
        self.own_tiles = self.own_mats * SUB
        self.halo_tiles = self.halo_mats * SUB
        self.coef_tiles = self.own_tiles + self.halo_tiles // self.piece
        self.per_group = rows // SUB
        self.groups = -(-self.coef_tiles // self.per_group)
        self.early = -(-self.halo_tiles // self.per_group)
        self.early_rows = self.early * self.piece
        self.late_rows = (self.groups - self.early) * self.piece + 1
        self.width = rows // self.piece


def fits(devices, rows, block, lanes=128):
    piece = rows // devices
    return block == SUB and rows == lanes and piece >= 1 and piece * devices == rows and rows // piece >= 4 * SUB


def lane(shape=(SUB, 128)):
    return lax.broadcasted_iota(jnp.int32, shape, 1)


def sub(shape=(SUB, 128)):
    return lax.broadcasted_iota(jnp.int32, shape, 0)


def spread(v, b):
    return jnp.broadcast_to(v[b : b + 1, :], v.shape)


def added(terms):
    while len(terms) > 1:
        terms = [x + y for x, y in zip(terms[::2], terms[1::2])]
    return terms[0]


def total(x):
    return jnp.sum(jnp.sum(x, axis=0, keepdims=True), axis=1, keepdims=True)


def send(plan, tiles, z_ref, wrap=False, row=None, sums=None):
    q, r = plan.piece, plan.rows
    n = plan.width - SUB * len(tiles)
    filler = [jnp.zeros((n, r), jnp.float32)] if n else []
    z = jnp.concatenate(([t for t, _ in tiles] + filler) * q, 0).T
    pad = jnp.zeros((SUB, r), jnp.float32)
    z_ref[pl.ds(0, SUB), :] = z[r - SUB :] if wrap else pad
    z_ref[pl.ds(SUB, r), :] = z
    z_ref[pl.ds(SUB + r, SUB), :] = z[:SUB] if wrap else pad
    place = lane((plan.devices, r)) // SUB
    out = jnp.zeros((plan.devices, r), jnp.float32)
    for i in range(q):
        loads = {}
        for k, (_, offsets) in enumerate(tiles):
            if offsets is None or offsets[i] is None:
                continue
            if offsets[i] not in loads:
                loads[offsets[i]] = z_ref[pl.ds(SUB + i + offsets[i], plan.devices, stride=q), :]
            out = jnp.where(place == i * (plan.width // SUB) + k, loads[offsets[i]], out)
    if sums is not None:
        parts = [z[SUB * i : SUB * i + SUB] for i in range(r // SUB)]
        while len(parts) > 1:
            parts = [x + y for x, y in zip(parts[::2], parts[1::2])]
        whole = jnp.broadcast_to(jnp.sum(parts[0], axis=0, keepdims=True), out.shape)
        out = jnp.where(place == sums, whole, out)
    return out if row is None else out + row


def sent_field(plan, y):
    q = plan.piece
    return [(y, (0,) * q), (y, (-1,) + (None,) * (q - 2) + (1,))]


def receive(plan, got, z_ref):
    for i in range(plan.piece):
        z_ref[pl.ds(i, plan.devices, stride=plan.piece), :] = got
    t = z_ref[...].T
    pos = lane() % plan.piece
    tiles = []
    for k in range(4):
        at = SUB * k
        tile = t[at : at + SUB]
        for i in range(1, plan.piece):
            tile = jnp.where(pos == i, t[i * plan.width + at : i * plan.width + at + SUB], tile)
        tiles.append(tile)
    return tiles


def wrapped(plan, x):
    q, r = plan.piece, plan.rows
    me = lax.axis_index(AXIS)
    at = lane()
    pos = at % q
    later = jnp.where(at == 0, 0.0, pltpu.roll(x, q, 1))
    sooner = jnp.where(at == r - 1, 0.0, pltpu.roll(x, r - q, 1))
    first = jnp.where(me == 0, later, x)
    last = jnp.where(me == plan.devices - 1, sooner, x)
    return jnp.where(pos == 0, first, jnp.where(pos == q - 1, last, 0.0))


def near_levels(plan, v, coef):
    r = plan.rows
    at = lane()
    for k in plan.near:
        s = 2**k
        turned = [pltpu.roll(x, s, 1) for x in v]
        back = [pltpu.roll(x, r - s, 1) for x in v]
        lower = [turned[0]] + [jnp.where(at < s, turned[t - 1], turned[t]) for t in (1, 2)]
        upper = [jnp.where(at >= r - s, back[t + 1], back[t]) for t in (0, 1)] + [back[2]]
        fresh = list(v)
        for t in (0, 1, 2) if k < plan.sent else (1,):
            sums = [None] * 4
            for b in range(SUB):
                for side, x in enumerate((lower[t], upper[t])):
                    term = coef(t, side, k, b) * spread(x, b)
                    at_sum = 2 * side + b % 2
                    sums[at_sum] = term if sums[at_sum] is None else sums[at_sum] + term
            fresh[t] = v[t] + (sums[0] + sums[1]) + (sums[2] + sums[3])
        v = fresh
    return v[1]


def square_tile(u):
    return jnp.where(sub() == 0, jnp.broadcast_to(total(u * u), u.shape), 0.0)


def load_kernel(plan, *refs):
    count = (len(refs) - 3) // 2
    ins, outs, edge_refs, sems = refs[:count], refs[count:-3], refs[-3:-1], refs[-1]
    copies = [pltpu.make_async_copy(x, y, sems.at[i]) for i, (x, y) in enumerate(zip(ins, outs))]
    for c in copies:
        c.start()
    for c in copies:
        c.wait()
    rhs_ref, lo_ref, up_ref = outs[:3]
    n = 64 * (plan.sent - 1)
    odd = lax.rem(lax.axis_index(AXIS), 2) == 1
    first = lane((64, plan.rows)) < plan.rows // 2
    low = lo_ref[pl.ds(n, 64), :]
    high = pltpu.roll(up_ref[pl.ds(n, 64), :], plan.rows // 2, 1)
    as_prev, as_next = jnp.where(first, high, low), jnp.where(first, low, high)
    across_ref, pair_ref = edge_refs
    across_ref[pl.ds(2 * n, 64), :] = jnp.where(odd, as_prev, as_next)
    pair_ref[pl.ds(2 * n, 64), :] = jnp.where(odd, as_next, as_prev)
    for ref in edge_refs:
        ref[pl.ds(0, n), :] = lo_ref[pl.ds(0, n), :]
        ref[pl.ds(n, n), :] = up_ref[pl.ds(0, n), :]
        ref[pl.ds(2 * n + 64, SUB), :] = rhs_ref[...]


def take_kernel(in_ref, out_ref):
    out_ref[...] = in_ref[...]


def pack_kernel(plan, first, last, lo_ref, up_ref, fin_ref, dia_ref, bel_ref, abo_ref, out_ref, z_ref):
    half = lax.axis_index(AXIS) >= plan.devices // 2
    *most, top = plan.far
    mats = [(lo_ref, 64 * k) for k in most] + [(up_ref, 64 * k) for k in most] + [None]
    mats += [(fin_ref, 0), (dia_ref, 0), (bel_ref, 0), (abo_ref, 0)]

    def raw(index):
        mat, b = divmod(index, SUB)
        if mats[mat] is None:
            low, high = (ref[pl.ds(64 * top + b, SUB, stride=SUB), :] for ref in (lo_ref, up_ref))
            return jnp.where(half, low, high)
        ref, base = mats[mat]
        return ref[pl.ds(base + b, SUB, stride=SUB), :]

    def tile(index):
        if index < plan.own_tiles:
            return raw(index)
        if index >= plan.coef_tiles:
            return jnp.zeros((SUB, plan.rows), jnp.float32)
        q, r = plan.piece, plan.rows
        even = lane() // q % 2 == 0
        out = None
        for m in range(q):
            x = raw(q * (index - plan.own_tiles) + m)
            x = jnp.where(even, pltpu.roll(x, m + 1, 1), pltpu.roll(x, r - q + m, 1))
            out = x if out is None else jnp.where(lane() % q == m, x, out)
        return out

    t = plan.per_group
    rows = out_ref.shape[0] // plan.devices
    for slot, g in enumerate(range(first, last)):
        z_ref[slot] = jnp.concatenate([tile(g * t + i) for i in range(t)], 0).T
        for i in range(plan.piece):
            out_ref[pl.ds(slot * plan.piece + i, plan.devices, stride=rows), :] = z_ref[
                slot, pl.ds(i, plan.devices, stride=plan.piece), :
            ]


def first_kernel(
    plan, lo_ref, up_ref, rhs_ref, pair_ref, other_ref, late_ref, out_ref, coef_ref, field_ref, z_ref, row_ref, sem
):
    last = plan.sent - 1
    n = 64 * (2 * last + 1)
    odd = lax.rem(lax.axis_index(AXIS), 2) == 1
    rhs = rhs_ref[...]

    def halo(t, start, stride):
        a, b = pair_ref[pl.ds(start, SUB, stride=stride), :], other_ref[pl.ds(start, SUB, stride=stride), :]
        return jnp.where(odd, a, b) if t == 0 else jnp.where(odd, b, a)

    def coef(t, side, k, b):
        if t == 1:
            ref = up_ref if side else lo_ref
            x = ref[pl.ds(64 * k + b, SUB, stride=SUB), :]
        elif k < last:
            x = halo(t, 64 * (last * side + k) + b, SUB)
        else:
            x = halo(t, 64 * 2 * last + b, SUB)
            x = pltpu.roll(x, plan.rows // 2, 1) if side else x
        coef_ref[t, side, k, b] = x
        return x

    fields = [halo(0, n, 1), rhs, halo(2, n, 1)]
    for t in range(3):
        field_ref[t] = fields[t]
    y = near_levels(plan, fields, coef)
    plain = (0,) * plan.piece
    row = send(plan, [*sent_field(plan, y), (square_tile(rhs), plain), (rhs, plain)], z_ref, wrap=True)
    for i in range(plan.devices):
        row_ref[i] = row[i : i + 1]
    copy = pltpu.make_async_copy(row_ref, out_ref.at[:, plan.late_rows - 1], sem)
    copy.start()
    copy.wait()


def far_stage(plan, own, halo, coef_ref):
    q, r, n = plan.piece, plan.rows, len(plan.far) - 1
    base = plan.own_tiles

    def apply(mat, x, start):
        return added([coef_ref[start + mat * SUB + b] * spread(x, b) for b in range(SUB)])

    for k in range(n):
        by = q * 2**k
        fresh = []
        for x, start in ((own, 0), (halo, base)):
            low = apply(k, pltpu.roll(x, by, 1), start)
            high = apply(n + k, pltpu.roll(x, r - by, 1), start)
            fresh.append(x + low + high)
        own, halo = fresh
    own, halo = (x + apply(2 * n, pltpu.roll(x, r // 2, 1), start) for x, start in ((own, 0), (halo, base)))
    own = own + apply(2 * n + 1, own, 0)
    halo = wrapped(plan, halo + apply(2 * n + 1, halo, base))
    pos = lane() % q
    before = jnp.where(pos == 0, halo, pltpu.roll(own, 1, 1))
    after = jnp.where(pos == q - 1, halo, pltpu.roll(own, r - 1, 1))
    w = 2.0 * own + apply(2 * n + 2, own, 0)
    return w + apply(2 * n + 3, before, 0) + apply(2 * n + 4, after, 0)


def norm_of(plan, squares):
    pos = lane() % plan.piece
    one = jnp.where((pos == 0) & (sub() == 0), squares, 0.0)
    return jnp.sqrt(jnp.broadcast_to(total(one), one.shape) / plan.count + EPS)


def finish_far(plan, y, halo, s, vs, coef_ref, z_ref, out_ref):
    w = far_stage(plan, y, halo, coef_ref) / s
    q = plan.piece
    dots = jnp.zeros_like(w)
    for i, v in enumerate(vs):
        dots = jnp.where(sub() == i, jnp.sum(v * w, axis=0, keepdims=True), dots)
    tiles = [(w, (by,) * q) for by in (-q, 0, q)] + [(dots, None)]
    out_ref[...] = send(plan, tiles, z_ref, sums=3)
    return w


def two_sum(a, b):
    s = a + b
    t = s - a
    return s, (a - (s - t)) + (b - t)


def halves(a):
    c = 4097.0 * a
    hi = c - (c - a)
    return hi, a - hi


def two_prod(a, b):
    p = a * b
    ah, al = halves(a)
    bh, bl = halves(b)
    return p, ((ah * bh - p) + ah * bl + al * bh) + al * bl


def pair_add(x, y):
    s, e = two_sum(x[0], y[0])
    e = e + (x[1] + y[1])
    hi = s + e
    return hi, e - (hi - s)


def pair_mul(x, y):
    p, e = two_prod(x[0], y[0])
    e = e + (x[0] * y[1] + x[1] * y[0])
    hi = p + e
    return hi, e - (hi - p)


def folded(x, shifts, axis):
    for s in shifts:
        x = pair_add(x, tuple(pltpu.roll(a, s, axis) for a in x))
    return x


def products():
    out = [(i, None) for i in range(ITERS)] + [(None, None)]
    return out + [(i, j) for i in range(ITERS) for j in range(i, ITERS)]


def rows_sum(pair):
    parts = [tuple(x[SUB * i : SUB * i + SUB] for x in pair) for i in range(pair[0].shape[0] // SUB)]
    while len(parts) > 1:
        half = len(parts) // 2
        parts = [pair_add(a, b) for a, b in zip(parts[:half], parts[half:])]
    one = folded(parts[0], (4, 2, 1), 0)
    return tuple(x[0:1] for x in one)


def last_far_kernel(plan, in_ref, coef_ref, h_ref, w_in_ref, *rest):
    j = ITERS - 1
    vs = [v[...] for v in rest[:j]]
    out_ref, s_ref, zr_ref, zs_ref = rest[j:]
    y, halo, s, v = enter_far(plan, in_ref, h_ref, w_in_ref, vs, zr_ref)
    s_ref[...] = s
    vs = vs + [v]
    w = far_stage(plan, y, halo, coef_ref) / s
    at = sub((2 * SUB, plan.rows))
    packed = [jnp.zeros((2 * SUB, plan.rows), jnp.float32)] * 2
    for i, (a, b) in enumerate(products()):
        pair = two_prod(w if a is None else vs[a], w if b is None else vs[b])
        pair = folded(pair, (4, 2, 1), 0)
        packed = [jnp.where(at == i, jnp.concatenate([x, x], 0), old) for x, old in zip(pair, packed)]
    filler = jnp.zeros((plan.rows - 2 * SUB, plan.rows), jnp.float32)
    hi, lo = rows_sum(tuple(jnp.concatenate([x, filler], 0).T for x in packed))
    hi, lo = (jnp.concatenate([x] * SUB, 0) for x in (hi, lo))
    row = pltpu.roll(hi, SUB, 1) + pltpu.roll(lo, SUB + len(products()), 1)
    out_ref[...] = send(plan, [(w, (0,) * plan.piece)], zs_ref, row=row[0:1])


def unpack(plan, groups, in_ref, rows, coef_ref, z_ref, lent_ref=None):
    q, r = plan.piece, plan.rows
    at = lane()
    n = len(plan.far) - 1
    even = lax.rem(lax.axis_index(AXIS), 2) == 0
    outer = jnp.where(even, (at % q == 0).astype(jnp.int32), (at % q == q - 1).astype(jnp.int32)) == 1

    def limited(x, mat):
        if mat < n:
            return jnp.where(at < q * 2**mat, 0.0, x)
        if mat < 2 * n:
            return jnp.where(at >= r - q * 2 ** (mat - n), 0.0, x)
        return x

    def moved(x, by):
        return pltpu.roll(x, by % r, 1) if by % r else x

    for slot, g in enumerate(groups):
        for i in range(q):
            z_ref[slot, pl.ds(i, plan.devices, stride=q), :] = in_ref[
                pl.ds(slot * q + i, plan.devices, stride=rows), :
            ]
        t = z_ref[slot].T
        for j in range(plan.per_group):
            index = g * plan.per_group + j
            tile = t[SUB * j : SUB * j + SUB]
            if index < plan.own_tiles:
                coef_ref[index] = limited(tile, index // SUB)
            elif index < plan.coef_tiles:
                for m in range(q):
                    k = q * (index - plan.own_tiles) + m
                    x = jnp.where(even, moved(tile, -m), moved(tile, q - 1 - m))
                    coef_ref[plan.own_tiles + k] = jnp.where(outer, limited(x, k // SUB), lent_ref[k])


def unpack_kernel(plan, early_ref, coef_ref, lend_ref, z_ref):
    unpack(plan, range(plan.early), early_ref, plan.early_rows, coef_ref, z_ref)
    even = lax.rem(lax.axis_index(AXIS), 2) == 0
    by = plan.piece - 1
    for k in range(plan.halo_tiles):
        x = coef_ref[k]
        lend_ref[k] = jnp.where(even, pltpu.roll(x, plan.rows - by, 1), pltpu.roll(x, by, 1)) if by else x


def start_far_kernel(
    plan, late_ref, early_coef_ref, lent_ref, out_ref, coef_ref, w_ref, v_ref, s_ref, z_ref, zr_ref, zs_ref
):
    unpack(plan, range(plan.early, plan.groups), late_ref, plan.late_rows, coef_ref, z_ref, lent_ref)
    got = late_ref[pl.ds(plan.late_rows - 1, plan.devices, stride=plan.late_rows), :]
    y, halo, squares, rhs = receive(plan, got, zr_ref)
    s = norm_of(plan, squares)
    v = rhs / s
    v_ref[...] = v
    s_ref[...] = s
    w_ref[...] = finish_far(plan, y, halo, s, [v], coef_ref, zs_ref, out_ref)


def near_kernel(plan, j, in_ref, coef_ref, field_ref, *rest):
    us, ss = rest[: j - 1], rest[j - 1 : 2 * j - 1]
    out_ref, u_ref, h_ref, zr_ref, zs_ref = rest[2 * j - 1 :]
    got = in_ref[...]
    dots = jnp.sum(got, axis=0, keepdims=True) / plan.count
    h = [jnp.broadcast_to(dots[:, 3 * SUB + i : 3 * SUB + i + 1], (SUB, plan.rows)) for i in range(j)]
    w = receive(plan, got, zr_ref)[:3]
    tall = jnp.zeros_like(h[0])
    for i in range(j):
        tall = jnp.where(sub() == i, h[i], tall)
    h_ref[...] = tall
    fields = [field_ref, *us]
    for t in range(3):
        acc = None
        for i in range(j):
            term = h[i] * (fields[i][t] / ss[i][...])
            acc = term if acc is None else acc + term
        w[t] = w[t] - acc
        u_ref[t] = w[t]
    y = near_levels(plan, w, lambda t, side, k, b: coef_ref[t, side, k, b])
    out_ref[...] = send(plan, [*sent_field(plan, y), (square_tile(w[1]), (0,) * plan.piece)], zs_ref, wrap=True)


def enter_far(plan, in_ref, h_ref, w_in_ref, vs, z_ref):
    y, halo, squares, _ = receive(plan, in_ref[...], z_ref)
    s = norm_of(plan, squares)
    h = h_ref[...]
    acc = None
    for i, v in enumerate(vs):
        term = spread(h, i) * v
        acc = term if acc is None else acc + term
    return y, halo, s, (w_in_ref[...] - acc) / s


def far_kernel(plan, j, in_ref, coef_ref, h_ref, w_in_ref, *rest):
    vs = [v[...] for v in rest[:j]]
    out_ref, w_ref, v_ref, s_ref, zr_ref, zs_ref = rest[j:]
    y, halo, s, v = enter_far(plan, in_ref, h_ref, w_in_ref, vs, zr_ref)
    v_ref[...] = v
    s_ref[...] = s
    w_ref[...] = finish_far(plan, y, halo, s, vs + [v], coef_ref, zs_ref, out_ref)


def output_kernel(plan, in_ref, field_ref, *rest):
    us = rest[: ITERS - 1]
    ss = [s[...] for s in rest[ITERS - 1 : 2 * ITERS - 1]]
    hs = [h[...] for h in rest[2 * ITERS - 1 : 3 * ITERS - 2]]
    basis_ref, hess_ref, z_ref = rest[3 * ITERS - 2 :]
    raw = in_ref[...]
    low = pltpu.roll(raw, plan.rows - len(products()), 1)
    row = rows_sum((raw, low))
    w = receive(plan, in_ref[...], z_ref)[0]
    wide = lambda x: jnp.broadcast_to(x, (SUB, plan.rows))
    sums = [tuple(wide(x[:, SUB + i : SUB + i + 1]) for x in row) for i in range(len(products()))]
    names = products()
    got = dict(zip(names, sums))
    h = [got[i, None][0] / plan.count for i in range(ITERS)]
    zero = jnp.zeros_like(h[0])
    squares = got[None, None]
    for i in range(ITERS):
        left = tuple(2.0 * x for x in got[i, None])
        for j in range(ITERS):
            left = pair_add(left, pair_mul((-h[j], zero), got[min(i, j), max(i, j)]))
        squares = pair_add(squares, pair_mul((-h[i], zero), left))
    squares = jnp.maximum(squares[0], 0.0)
    ss.append(jnp.sqrt(squares / plan.count + EPS))
    fields = [field_ref[1]] + [u[1] for u in us]
    vs = [f / s for f, s in zip(fields, ss)]
    acc = None
    for i in range(ITERS):
        term = h[i] * vs[i]
        acc = term if acc is None else acc + term
    vs.append((w - acc) / ss[-1])
    for j in range(ITERS + 1):
        basis_ref[j] = vs[j]
    top = jnp.zeros_like(w)
    for i in range(ITERS):
        top = jnp.where(sub() == i, h[i], top)
    hs.append(top)
    hess = jnp.zeros_like(w)
    for j in range(ITERS):
        col = jnp.where(sub() <= j, hs[j], jnp.where(sub() == j + 1, ss[j + 1], 0.0))
        hess = jnp.where(lane() == j, col, hess)
    hess_ref[...] = hess[: ITERS + 1, :ITERS]


def transposed(
    plan, right_side, diag_block, below_block, above_block, lower_level, upper_level, final_block
):
    r, d = plan.rows, plan.devices
    flat = lambda x: x.reshape(-1, r)
    lo, up, fin = flat(lower_level), flat(upper_level), flat(final_block)
    dia, bel, abo = flat(diag_block), flat(below_block), flat(above_block)
    shape = lambda *s: jax.ShapeDtypeStruct(s, jnp.float32)
    tile = shape(SUB, r)
    scratch = lambda *s: pltpu.VMEM(s, jnp.float32)

    def call(kernel, outs, scratches, *args, space=pltpu.VMEM, flops=1_000_000, places=None, out_places=None, **more):
        return pl.pallas_call(
            kernel,
            out_shape=outs,
            in_specs=[pl.BlockSpec(memory_space=x) for x in places or [space] * len(args)],
            out_specs=jax.tree.map(lambda _: pl.BlockSpec(memory_space=pltpu.VMEM), outs)
            if out_places is None
            else [pl.BlockSpec(memory_space=x) for x in out_places],
            scratch_shapes=scratches,
            compiler_params=pltpu.CompilerParams(vmem_limit_bytes=24 * 2**20),
            cost_estimate=pl.CostEstimate(flops=flops, bytes_accessed=1_000_000, transcendentals=0),
            **more,
        )(*args)

    def exchange(x):
        y = lax.all_to_all(x.reshape(-1, 1, r), AXIS, 0, 0, tiled=True)
        return y.reshape(-1, r)

    part = functools.partial
    raw = tuple(pltpu.with_memory_space_constraint(x, pltpu.HBM) for x in (right_side, lo, up, fin, dia, bel, abo))
    edge = shape(64 * (2 * plan.sent - 1) + SUB, r)
    *loaded, edge_across, edge_pair = call(
        part(load_kernel, plan),
        (*(shape(*x.shape) for x in raw), edge, edge),
        [pltpu.SemaphoreType.DMA((len(raw),))],
        *raw,
        space=pltpu.HBM,
    )
    rhs, lo, up = loaded[:3]
    mats = loaded[1:]
    other = lax.ppermute(edge_across, AXIS, [(i, i + 1 if i % 2 else i - 1) for i in range(1, d - 1)])
    pair = lax.ppermute(edge_pair, AXIS, [(i, i ^ 1) for i in range(d)])
    pair = call(take_kernel, edge, [], pair)
    early = call(
        part(pack_kernel, plan, 0, plan.early),
        shape(d * plan.early_rows, r),
        [scratch(plan.early, r, r)],
        *mats,
        flops=10_000_000,
    )
    early = exchange(early)
    late_shape = shape(d * plan.late_rows, r)
    late = call(
        part(pack_kernel, plan, plan.early, plan.groups),
        late_shape,
        [scratch(plan.groups - plan.early, r, r)],
        *mats,
        flops=10_000_000,
    )
    late_shape = shape(d, plan.late_rows, 1, r)
    late, near, fields = call(
        part(first_kernel, plan),
        (late_shape, shape(3, 2, len(plan.near), SUB, SUB, r), shape(3, SUB, r)),
        [scratch(r + 2 * SUB, r), scratch(d, 1, r), pltpu.SemaphoreType.DMA],
        lo, up, rhs, pair, other, late.reshape(late_shape.shape),
        places=[pltpu.VMEM] * 5 + [pl.ANY],
        out_places=[pl.ANY] + [pltpu.VMEM] * 2,
        input_output_aliases={5: 0},
    )
    small = shape(d, r)
    padded = scratch(r + 2 * SUB, r)
    two = [scratch(r, r), padded]
    late = exchange(late)
    coef_shape = shape(plan.own_tiles + plan.halo_tiles, SUB, r)
    lend_shape = shape(plan.halo_tiles, SUB, r)
    coef, lent = call(
        part(unpack_kernel, plan), (coef_shape, lend_shape), [scratch(plan.early, r, r)], early, flops=5_000_000
    )
    lent = lax.ppermute(lent, AXIS, [(i, i ^ 1) for i in range(d)])
    out, coef, w, v, s = call(
        part(start_far_kernel, plan),
        (small, coef_shape, tile, tile, tile),
        [scratch(plan.groups - plan.early, r, r), *two],
        late, coef, lent,
        input_output_aliases={1: 1},
    )
    us, ss, vs, hs = [], [s], [v], []
    for j in range(1, ITERS):
        out, u, h = call(
            part(near_kernel, plan, j),
            (small, shape(3, SUB, r), tile),
            two,
            exchange(out), near, fields, *us, *ss,
        )
        us.append(u)
        hs.append(h)
        if j < ITERS - 1:
            out, w, v, s = call(
                part(far_kernel, plan, j), (small, tile, tile, tile), two, exchange(out), coef, h, w, *vs
            )
            vs.append(v)
        else:
            out, s = call(part(last_far_kernel, plan), (small, tile), two, exchange(out), coef, h, w, *vs)
        ss.append(s)
    return call(
        part(output_kernel, plan),
        (shape(ITERS + 1, SUB, r), shape(ITERS + 1, ITERS)),
        [scratch(r, r)],
        exchange(out), fields, *us, *ss, *hs,
    )


def on_device(*args):
    right_side, lower_level = args[0], args[4]
    devices, rows = lax.axis_size(AXIS), right_side.shape[1]
    if not fits(devices, rows, right_side.shape[0]):
        return general(*args)
    return tuple(transposed(Plan(devices, rows, lower_level.shape[0]), *args))


def solution(mesh):
    return jax.shard_map(
        on_device,
        mesh=mesh,
        in_specs=(
            P(None, "chain"),
            P(None, None, "chain"),
            P(None, None, "chain"),
            P(None, None, "chain"),
            P(None, None, None, "chain"),
            P(None, None, None, "chain"),
            P(None, None, "chain"),
        ),
        out_specs=(P(None, None, "chain"), P()),
        check_vma=False,
    )
```

```python
import functools

import jax
import jax.numpy as jnp
from jax import lax
from jax.experimental import pallas as pl
from jax.experimental.pallas import tpu as pltpu
from jax.sharding import PartitionSpec as P


ITERS = 3


EPS = 1e-06
AXIS = "chain"
SUB = 8


def padded_2(x, sides, width):
    for axis, dim in sides:
        peers, length = (lax.axis_size(axis), x.shape[dim])
        up = [(i, (i + 1) % peers) for i in range(peers - 1)]
        down = [(j, i) for i, j in up]
        last = lax.slice_in_dim(x, length - width, length, axis=dim)
        initial = lax.slice_in_dim(x, 0, width, axis=dim)
        before = lax.ppermute(last, axis, up)
        after = lax.ppermute(initial, axis, down)
        x = jnp.concatenate([before, x, after], axis=dim)
    return x


def from_behind(x, axis, by):
    peers = lax.axis_size(axis)
    pairs = [(i, i + by) for i in range(peers) if 0 <= i + by < peers]
    return lax.ppermute(x, axis, pairs)


def blockmul(blocks, field):
    return jnp.einsum("abi,bi->ai", blocks, field, precision=lax.Precision.HIGHEST)


def general(
    right_side, diag_block, below_block, above_block, lower_level, upper_level, final_block
):
    rows_here = right_side.shape[1]
    devices = lax.axis_size("chain")
    whole = rows_here * devices
    count = right_side.shape[0] * whole
    depth = lower_level.shape[0]
    near = [level for level in range(depth) if 2**level < rows_here]
    far = [level for level in range(depth) if 2**level >= rows_here and 2**level < whole]
    reach = sum((2**level for level in near))
    stacked_coef = jnp.concatenate([lower_level[: len(near)], upper_level[: len(near)]], 0)
    wide_coef = padded_2(stacked_coef, (("chain", 3),), reach)
    start_sum = lax.psum(jnp.sum(right_side * right_side), "chain")
    basis = [right_side / jnp.sqrt(start_sum / count + EPS)]
    hess = jnp.zeros((ITERS + 1, ITERS), jnp.float32)
    for column in range(ITERS):
        precondition_field = basis[column]
        current = padded_2(precondition_field, (("chain", 1),), reach)
        offset = 0
        for position in range(len(near)):
            stride = 2 ** near[position]
            length = current.shape[1]
            first_col = offset + stride
            last_col = offset + length - stride
            low_coef = wide_coef[position][:, :, first_col:last_col]
            high_coef = wide_coef[len(near) + position][:, :, first_col:last_col]
            current = (
                current[:, stride : length - stride]
                + blockmul(low_coef, current[:, : length - 2 * stride])
                + blockmul(high_coef, current[:, 2 * stride :])
            )
            offset = first_col
        precondition_field = current
        for precondition_level in far:
            hops = 2**precondition_level // rows_here
            below_rows = from_behind(precondition_field, "chain", hops)
            above_rows = from_behind(precondition_field, "chain", -hops)
            precondition_field = (
                precondition_field
                + blockmul(lower_level[precondition_level], below_rows)
                + blockmul(upper_level[precondition_level], above_rows)
            )
        field = precondition_field + blockmul(final_block, precondition_field)
        padded = padded_2(field, (("chain", 1),), 1)
        result = 2.0 * field + blockmul(diag_block, field)
        result = result + blockmul(below_block, padded[:, :rows_here])
        vector = result + blockmul(above_block, padded[:, 2:])
        stacked = jnp.stack(basis)
        local_dots = jnp.einsum("kai,ai->k", stacked, vector, precision=lax.Precision.HIGHEST)
        dots = lax.psum(local_dots, "chain") / count
        vector = vector - jnp.einsum("k,kai->ai", dots, stacked, precision=lax.Precision.HIGHEST)
        squares = lax.psum(jnp.sum(vector * vector), "chain") / count
        length = jnp.sqrt(squares + EPS)
        basis.append(vector / length)
        hess = hess.at[: column + 1, column].set(dots).at[column + 1, column].set(length)
    return (jnp.stack(basis), hess)


class Plan:
    def __init__(self, devices, rows, depth):
        self.devices, self.rows, self.depth = devices, rows, depth
        self.piece = rows // devices
        self.near = [k for k in range(depth) if 2**k < rows]
        self.far = [k for k in range(depth) if rows <= 2**k < rows * devices]
        self.sent = len(self.near) - 1
        self.count = SUB * rows * devices
        n = len(self.far) - 1
        self.halo_mats = 2 * n + 2
        self.own_mats = self.halo_mats + 3
        self.own_tiles = self.own_mats * SUB
        self.halo_tiles = self.halo_mats * SUB
        self.coef_tiles = self.own_tiles + self.halo_tiles // self.piece
        self.per_group = rows // SUB
        self.groups = -(-self.coef_tiles // self.per_group)
        self.early = -(-self.halo_tiles // self.per_group) + 1
        self.early_rows = self.early * self.piece
        self.late_rows = (self.groups - self.early) * self.piece + 1
        self.width = rows // self.piece


def fits(devices, rows, block, lanes=128):
    piece = rows // devices
    return block == SUB and rows == lanes and piece >= 1 and piece * devices == rows and rows // piece >= 4 * SUB


def lane(shape=(SUB, 128)):
    return lax.broadcasted_iota(jnp.int32, shape, 1)


def sub(shape=(SUB, 128)):
    return lax.broadcasted_iota(jnp.int32, shape, 0)


def spread(v, b):
    return jnp.broadcast_to(v[b : b + 1, :], v.shape)


def added(terms):
    while len(terms) > 1:
        terms = [x + y for x, y in zip(terms[::2], terms[1::2])]
    return terms[0]


def total(x):
    return jnp.sum(jnp.sum(x, axis=0, keepdims=True), axis=1, keepdims=True)


def send(plan, tiles, z_ref, wrap=False, row=None, sums=None):
    q, r = plan.piece, plan.rows
    n = plan.width - SUB * len(tiles)
    filler = [jnp.zeros((n, r), jnp.float32)] if n else []
    z = jnp.concatenate(([t for t, _ in tiles] + filler) * q, 0).T
    pad = jnp.zeros((SUB, r), jnp.float32)
    z_ref[pl.ds(0, SUB), :] = z[r - SUB :] if wrap else pad
    z_ref[pl.ds(SUB, r), :] = z
    z_ref[pl.ds(SUB + r, SUB), :] = z[:SUB] if wrap else pad
    place = lane((plan.devices, r)) // SUB
    out = jnp.zeros((plan.devices, r), jnp.float32)
    for i in range(q):
        loads = {}
        for k, (_, offsets) in enumerate(tiles):
            if offsets is None or offsets[i] is None:
                continue
            if offsets[i] not in loads:
                loads[offsets[i]] = z_ref[pl.ds(SUB + i + offsets[i], plan.devices, stride=q), :]
            out = jnp.where(place == i * (plan.width // SUB) + k, loads[offsets[i]], out)
    if sums is not None:
        parts = [z[SUB * i : SUB * i + SUB] for i in range(r // SUB)]
        while len(parts) > 1:
            parts = [x + y for x, y in zip(parts[::2], parts[1::2])]
        whole = jnp.broadcast_to(jnp.sum(parts[0], axis=0, keepdims=True), out.shape)
        out = jnp.where(place == sums, whole, out)
    return out if row is None else out + row


def sent_field(plan, y):
    q = plan.piece
    return [(y, (0,) * q), (y, (-1,) + (None,) * (q - 2) + (1,))]


def receive(plan, got, z_ref):
    for i in range(plan.piece):
        z_ref[pl.ds(i, plan.devices, stride=plan.piece), :] = got
    t = z_ref[...].T
    pos = lane() % plan.piece
    tiles = []
    for k in range(4):
        at = SUB * k
        tile = t[at : at + SUB]
        for i in range(1, plan.piece):
            tile = jnp.where(pos == i, t[i * plan.width + at : i * plan.width + at + SUB], tile)
        tiles.append(tile)
    return tiles


def wrapped(plan, x):
    q, r = plan.piece, plan.rows
    me = lax.axis_index(AXIS)
    at = lane()
    pos = at % q
    later = jnp.where(at == 0, 0.0, pltpu.roll(x, q, 1))
    sooner = jnp.where(at == r - 1, 0.0, pltpu.roll(x, r - q, 1))
    first = jnp.where(me == 0, later, x)
    last = jnp.where(me == plan.devices - 1, sooner, x)
    return jnp.where(pos == 0, first, jnp.where(pos == q - 1, last, 0.0))


def near_levels(plan, v, coef):
    r = plan.rows
    at = lane()
    for k in plan.near:
        s = 2**k
        turned = [pltpu.roll(x, s, 1) for x in v]
        back = [pltpu.roll(x, r - s, 1) for x in v]
        lower = [turned[0]] + [jnp.where(at < s, turned[t - 1], turned[t]) for t in (1, 2)]
        upper = [jnp.where(at >= r - s, back[t + 1], back[t]) for t in (0, 1)] + [back[2]]
        fresh = list(v)
        for t in (0, 1, 2) if k < plan.sent else (1,):
            low_sum = high_sum = None
            for b in range(SUB):
                low = coef(t, 0, k, b) * spread(lower[t], b)
                high = coef(t, 1, k, b) * spread(upper[t], b)
                low_sum = low if low_sum is None else low_sum + low
                high_sum = high if high_sum is None else high_sum + high
            fresh[t] = v[t] + low_sum + high_sum
        v = fresh
    return v[1]


def square_tile(u):
    return jnp.where(sub() == 0, jnp.broadcast_to(total(u * u), u.shape), 0.0)


def load_kernel(plan, *refs):
    count = (len(refs) - 3) // 2
    ins, outs, edge_refs, sems = refs[:count], refs[count:-3], refs[-3:-1], refs[-1]
    copies = [pltpu.make_async_copy(x, y, sems.at[i]) for i, (x, y) in enumerate(zip(ins, outs))]
    for c in copies:
        c.start()
    for c in copies:
        c.wait()
    rhs_ref, lo_ref, up_ref = outs[:3]
    n = 64 * (plan.sent - 1)
    odd = lax.rem(lax.axis_index(AXIS), 2) == 1
    first = lane((64, plan.rows)) < plan.rows // 2
    low = lo_ref[pl.ds(n, 64), :]
    high = pltpu.roll(up_ref[pl.ds(n, 64), :], plan.rows // 2, 1)
    as_prev, as_next = jnp.where(first, high, low), jnp.where(first, low, high)
    across_ref, pair_ref = edge_refs
    across_ref[pl.ds(2 * n, 64), :] = jnp.where(odd, as_prev, as_next)
    pair_ref[pl.ds(2 * n, 64), :] = jnp.where(odd, as_next, as_prev)
    for ref in edge_refs:
        ref[pl.ds(0, n), :] = lo_ref[pl.ds(0, n), :]
        ref[pl.ds(n, n), :] = up_ref[pl.ds(0, n), :]
        ref[pl.ds(2 * n + 64, SUB), :] = rhs_ref[...]


def take_kernel(in_ref, out_ref):
    out_ref[...] = in_ref[...]


def pack_kernel(plan, first, last, lo_ref, up_ref, fin_ref, dia_ref, bel_ref, abo_ref, out_ref, z_ref):
    half = lax.axis_index(AXIS) >= plan.devices // 2
    *most, top = plan.far
    mats = [(lo_ref, 64 * k) for k in most] + [(up_ref, 64 * k) for k in most] + [None]
    mats += [(fin_ref, 0), (dia_ref, 0), (bel_ref, 0), (abo_ref, 0)]

    def raw(index):
        mat, b = divmod(index, SUB)
        if mats[mat] is None:
            low, high = (ref[pl.ds(64 * top + b, SUB, stride=SUB), :] for ref in (lo_ref, up_ref))
            return jnp.where(half, low, high)
        ref, base = mats[mat]
        return ref[pl.ds(base + b, SUB, stride=SUB), :]

    def tile(index):
        if index < plan.own_tiles:
            return raw(index)
        if index >= plan.coef_tiles:
            return jnp.zeros((SUB, plan.rows), jnp.float32)
        q, r = plan.piece, plan.rows
        even = lane() // q % 2 == 0
        out = None
        for m in range(q):
            x = raw(q * (index - plan.own_tiles) + m)
            x = jnp.where(even, pltpu.roll(x, m + 1, 1), pltpu.roll(x, r - q + m, 1))
            out = x if out is None else jnp.where(lane() % q == m, x, out)
        return out

    t = plan.per_group
    rows = out_ref.shape[0] // plan.devices
    for slot, g in enumerate(range(first, last)):
        z_ref[slot] = jnp.concatenate([tile(g * t + i) for i in range(t)], 0).T
        for i in range(plan.piece):
            out_ref[pl.ds(slot * plan.piece + i, plan.devices, stride=rows), :] = z_ref[
                slot, pl.ds(i, plan.devices, stride=plan.piece), :
            ]


def first_kernel(
    plan, lo_ref, up_ref, rhs_ref, pair_ref, other_ref, late_ref, out_ref, coef_ref, field_ref, z_ref, row_ref, sem
):
    last = plan.sent - 1
    n = 64 * (2 * last + 1)
    odd = lax.rem(lax.axis_index(AXIS), 2) == 1
    rhs = rhs_ref[...]

    def halo(t, start, stride):
        a, b = pair_ref[pl.ds(start, SUB, stride=stride), :], other_ref[pl.ds(start, SUB, stride=stride), :]
        return jnp.where(odd, a, b) if t == 0 else jnp.where(odd, b, a)

    def coef(t, side, k, b):
        if t == 1:
            ref = up_ref if side else lo_ref
            x = ref[pl.ds(64 * k + b, SUB, stride=SUB), :]
        elif k < last:
            x = halo(t, 64 * (last * side + k) + b, SUB)
        else:
            x = halo(t, 64 * 2 * last + b, SUB)
            x = pltpu.roll(x, plan.rows // 2, 1) if side else x
        coef_ref[t, side, k, b] = x
        return x

    fields = [halo(0, n, 1), rhs, halo(2, n, 1)]
    for t in range(3):
        field_ref[t] = fields[t]
    y = near_levels(plan, fields, coef)
    plain = (0,) * plan.piece
    row = send(plan, [*sent_field(plan, y), (square_tile(rhs), plain), (rhs, plain)], z_ref, wrap=True)
    for i in range(plan.devices):
        row_ref[i] = row[i : i + 1]
    copy = pltpu.make_async_copy(row_ref, out_ref.at[:, plan.late_rows - 1], sem)
    copy.start()
    copy.wait()


def far_stage(plan, own, halo, coef_ref):
    q, r, n = plan.piece, plan.rows, len(plan.far) - 1
    base = plan.own_tiles

    def apply(mat, x, start):
        return added([coef_ref[start + mat * SUB + b] * spread(x, b) for b in range(SUB)])

    for k in range(n):
        by = q * 2**k
        fresh = []
        for x, start in ((own, 0), (halo, base)):
            low = apply(k, pltpu.roll(x, by, 1), start)
            high = apply(n + k, pltpu.roll(x, r - by, 1), start)
            fresh.append(x + low + high)
        own, halo = fresh
    own, halo = (x + apply(2 * n, pltpu.roll(x, r // 2, 1), start) for x, start in ((own, 0), (halo, base)))
    own = own + apply(2 * n + 1, own, 0)
    halo = wrapped(plan, halo + apply(2 * n + 1, halo, base))
    pos = lane() % q
    before = jnp.where(pos == 0, halo, pltpu.roll(own, 1, 1))
    after = jnp.where(pos == q - 1, halo, pltpu.roll(own, r - 1, 1))
    w = 2.0 * own + apply(2 * n + 2, own, 0)
    return w + apply(2 * n + 3, before, 0) + apply(2 * n + 4, after, 0)


def norm_of(plan, squares):
    pos = lane() % plan.piece
    one = jnp.where((pos == 0) & (sub() == 0), squares, 0.0)
    return jnp.sqrt(jnp.broadcast_to(total(one), one.shape) / plan.count + EPS)


def finish_far(plan, y, halo, s, vs, coef_ref, z_ref, out_ref):
    w = far_stage(plan, y, halo, coef_ref) / s
    q = plan.piece
    dots = jnp.zeros_like(w)
    for i, v in enumerate(vs):
        dots = jnp.where(sub() == i, jnp.sum(v * w, axis=0, keepdims=True), dots)
    tiles = [(w, (by,) * q) for by in (-q, 0, q)] + [(dots, None)]
    out_ref[...] = send(plan, tiles, z_ref, sums=3)
    return w


def two_sum(a, b):
    s = a + b
    t = s - a
    return s, (a - (s - t)) + (b - t)


def halves(a):
    c = 4097.0 * a
    hi = c - (c - a)
    return hi, a - hi


def two_prod(a, b):
    p = a * b
    ah, al = halves(a)
    bh, bl = halves(b)
    return p, ((ah * bh - p) + ah * bl + al * bh) + al * bl


def pair_add(x, y):
    s, e = two_sum(x[0], y[0])
    e = e + (x[1] + y[1])
    hi = s + e
    return hi, e - (hi - s)


def pair_mul(x, y):
    p, e = two_prod(x[0], y[0])
    e = e + (x[0] * y[1] + x[1] * y[0])
    hi = p + e
    return hi, e - (hi - p)


def folded(x, shifts, axis):
    for s in shifts:
        x = pair_add(x, tuple(pltpu.roll(a, s, axis) for a in x))
    return x


def products():
    out = [(i, None) for i in range(ITERS)] + [(None, None)]
    return out + [(i, j) for i in range(ITERS) for j in range(i, ITERS)]


def rows_sum(pair):
    parts = [tuple(x[SUB * i : SUB * i + SUB] for x in pair) for i in range(pair[0].shape[0] // SUB)]
    while len(parts) > 1:
        half = len(parts) // 2
        parts = [pair_add(a, b) for a, b in zip(parts[:half], parts[half:])]
    one = folded(parts[0], (4, 2, 1), 0)
    return tuple(x[0:1] for x in one)


def last_far_kernel(plan, in_ref, coef_ref, h_ref, w_in_ref, *rest):
    j = ITERS - 1
    vs = [v[...] for v in rest[:j]]
    out_ref, s_ref, zr_ref, zs_ref = rest[j:]
    y, halo, s, v = enter_far(plan, in_ref, h_ref, w_in_ref, vs, zr_ref)
    s_ref[...] = s
    vs = vs + [v]
    w = far_stage(plan, y, halo, coef_ref) / s
    at = sub((2 * SUB, plan.rows))
    packed = [jnp.zeros((2 * SUB, plan.rows), jnp.float32)] * 2
    for i, (a, b) in enumerate(products()):
        pair = two_prod(w if a is None else vs[a], w if b is None else vs[b])
        pair = folded(pair, (4, 2, 1), 0)
        packed = [jnp.where(at == i, jnp.concatenate([x, x], 0), old) for x, old in zip(pair, packed)]
    filler = jnp.zeros((plan.rows - 2 * SUB, plan.rows), jnp.float32)
    hi, lo = rows_sum(tuple(jnp.concatenate([x, filler], 0).T for x in packed))
    hi, lo = (jnp.concatenate([x] * SUB, 0) for x in (hi, lo))
    row = pltpu.roll(hi, SUB, 1) + pltpu.roll(lo, SUB + len(products()), 1)
    out_ref[...] = send(plan, [(w, (0,) * plan.piece)], zs_ref, row=row[0:1])


def unpack(plan, groups, in_ref, rows, coef_ref, z_ref, lent_ref=None):
    q, r = plan.piece, plan.rows
    at = lane()
    n = len(plan.far) - 1
    even = lax.rem(lax.axis_index(AXIS), 2) == 0
    outer = jnp.where(even, (at % q == 0).astype(jnp.int32), (at % q == q - 1).astype(jnp.int32)) == 1

    def limited(x, mat):
        if mat < n:
            return jnp.where(at < q * 2**mat, 0.0, x)
        if mat < 2 * n:
            return jnp.where(at >= r - q * 2 ** (mat - n), 0.0, x)
        return x

    def moved(x, by):
        return pltpu.roll(x, by % r, 1) if by % r else x

    for slot, g in enumerate(groups):
        for i in range(q):
            z_ref[slot, pl.ds(i, plan.devices, stride=q), :] = in_ref[
                pl.ds(slot * q + i, plan.devices, stride=rows), :
            ]
        t = z_ref[slot].T
        for j in range(plan.per_group):
            index = g * plan.per_group + j
            tile = t[SUB * j : SUB * j + SUB]
            if index < plan.own_tiles:
                coef_ref[index] = limited(tile, index // SUB)
            elif index < plan.coef_tiles:
                for m in range(q):
                    k = q * (index - plan.own_tiles) + m
                    x = jnp.where(even, moved(tile, -m), moved(tile, q - 1 - m))
                    coef_ref[plan.own_tiles + k] = jnp.where(outer, limited(x, k // SUB), lent_ref[k])


def unpack_kernel(plan, early_ref, coef_ref, lend_ref, z_ref):
    unpack(plan, range(plan.early), early_ref, plan.early_rows, coef_ref, z_ref)
    even = lax.rem(lax.axis_index(AXIS), 2) == 0
    by = plan.piece - 1
    for k in range(plan.halo_tiles):
        x = coef_ref[k]
        lend_ref[k] = jnp.where(even, pltpu.roll(x, plan.rows - by, 1), pltpu.roll(x, by, 1)) if by else x


def start_far_kernel(
    plan, late_ref, early_coef_ref, lent_ref, out_ref, coef_ref, w_ref, v_ref, s_ref, z_ref, zr_ref, zs_ref
):
    unpack(plan, range(plan.early, plan.groups), late_ref, plan.late_rows, coef_ref, z_ref, lent_ref)
    got = late_ref[pl.ds(plan.late_rows - 1, plan.devices, stride=plan.late_rows), :]
    y, halo, squares, rhs = receive(plan, got, zr_ref)
    s = norm_of(plan, squares)
    v = rhs / s
    v_ref[...] = v
    s_ref[...] = s
    w_ref[...] = finish_far(plan, y, halo, s, [v], coef_ref, zs_ref, out_ref)


def near_kernel(plan, j, in_ref, coef_ref, field_ref, *rest):
    us, ss = rest[: j - 1], rest[j - 1 : 2 * j - 1]
    out_ref, u_ref, h_ref, zr_ref, zs_ref = rest[2 * j - 1 :]
    got = in_ref[...]
    dots = jnp.sum(got, axis=0, keepdims=True) / plan.count
    h = [jnp.broadcast_to(dots[:, 3 * SUB + i : 3 * SUB + i + 1], (SUB, plan.rows)) for i in range(j)]
    w = receive(plan, got, zr_ref)[:3]
    tall = jnp.zeros_like(h[0])
    for i in range(j):
        tall = jnp.where(sub() == i, h[i], tall)
    h_ref[...] = tall
    fields = [field_ref, *us]
    for t in range(3):
        acc = None
        for i in range(j):
            term = h[i] * (fields[i][t] / ss[i][...])
            acc = term if acc is None else acc + term
        w[t] = w[t] - acc
        u_ref[t] = w[t]
    y = near_levels(plan, w, lambda t, side, k, b: coef_ref[t, side, k, b])
    out_ref[...] = send(plan, [*sent_field(plan, y), (square_tile(w[1]), (0,) * plan.piece)], zs_ref, wrap=True)


def enter_far(plan, in_ref, h_ref, w_in_ref, vs, z_ref):
    y, halo, squares, _ = receive(plan, in_ref[...], z_ref)
    s = norm_of(plan, squares)
    h = h_ref[...]
    acc = None
    for i, v in enumerate(vs):
        term = spread(h, i) * v
        acc = term if acc is None else acc + term
    return y, halo, s, (w_in_ref[...] - acc) / s


def far_kernel(plan, j, in_ref, coef_ref, h_ref, w_in_ref, *rest):
    vs = [v[...] for v in rest[:j]]
    out_ref, w_ref, v_ref, s_ref, zr_ref, zs_ref = rest[j:]
    y, halo, s, v = enter_far(plan, in_ref, h_ref, w_in_ref, vs, zr_ref)
    v_ref[...] = v
    s_ref[...] = s
    w_ref[...] = finish_far(plan, y, halo, s, vs + [v], coef_ref, zs_ref, out_ref)


def output_kernel(plan, in_ref, field_ref, *rest):
    us = rest[: ITERS - 1]
    ss = [s[...] for s in rest[ITERS - 1 : 2 * ITERS - 1]]
    hs = [h[...] for h in rest[2 * ITERS - 1 : 3 * ITERS - 2]]
    basis_ref, hess_ref, z_ref = rest[3 * ITERS - 2 :]
    raw = in_ref[...]
    low = pltpu.roll(raw, plan.rows - len(products()), 1)
    row = rows_sum((raw, low))
    w = receive(plan, in_ref[...], z_ref)[0]
    wide = lambda x: jnp.broadcast_to(x, (SUB, plan.rows))
    sums = [tuple(wide(x[:, SUB + i : SUB + i + 1]) for x in row) for i in range(len(products()))]
    names = products()
    got = dict(zip(names, sums))
    h = [got[i, None][0] / plan.count for i in range(ITERS)]
    zero = jnp.zeros_like(h[0])
    squares = got[None, None]
    for i in range(ITERS):
        left = tuple(2.0 * x for x in got[i, None])
        for j in range(ITERS):
            left = pair_add(left, pair_mul((-h[j], zero), got[min(i, j), max(i, j)]))
        squares = pair_add(squares, pair_mul((-h[i], zero), left))
    squares = jnp.maximum(squares[0], 0.0)
    ss.append(jnp.sqrt(squares / plan.count + EPS))
    fields = [field_ref[1]] + [u[1] for u in us]
    vs = [f / s for f, s in zip(fields, ss)]
    acc = None
    for i in range(ITERS):
        term = h[i] * vs[i]
        acc = term if acc is None else acc + term
    vs.append((w - acc) / ss[-1])
    for j in range(ITERS + 1):
        basis_ref[j] = vs[j]
    top = jnp.zeros_like(w)
    for i in range(ITERS):
        top = jnp.where(sub() == i, h[i], top)
    hs.append(top)
    hess = jnp.zeros_like(w)
    for j in range(ITERS):
        col = jnp.where(sub() <= j, hs[j], jnp.where(sub() == j + 1, ss[j + 1], 0.0))
        hess = jnp.where(lane() == j, col, hess)
    hess_ref[...] = hess[: ITERS + 1, :ITERS]


def transposed(
    plan, right_side, diag_block, below_block, above_block, lower_level, upper_level, final_block
):
    r, d = plan.rows, plan.devices
    flat = lambda x: x.reshape(-1, r)
    lo, up, fin = flat(lower_level), flat(upper_level), flat(final_block)
    dia, bel, abo = flat(diag_block), flat(below_block), flat(above_block)
    shape = lambda *s: jax.ShapeDtypeStruct(s, jnp.float32)
    tile = shape(SUB, r)
    scratch = lambda *s: pltpu.VMEM(s, jnp.float32)

    def call(kernel, outs, scratches, *args, space=pltpu.VMEM, flops=1_000_000, places=None, out_places=None, **more):
        return pl.pallas_call(
            kernel,
            out_shape=outs,
            in_specs=[pl.BlockSpec(memory_space=x) for x in places or [space] * len(args)],
            out_specs=jax.tree.map(lambda _: pl.BlockSpec(memory_space=pltpu.VMEM), outs)
            if out_places is None
            else [pl.BlockSpec(memory_space=x) for x in out_places],
            scratch_shapes=scratches,
            compiler_params=pltpu.CompilerParams(vmem_limit_bytes=24 * 2**20),
            cost_estimate=pl.CostEstimate(flops=flops, bytes_accessed=1_000_000, transcendentals=0),
            **more,
        )(*args)

    def exchange(x):
        y = lax.all_to_all(x.reshape(-1, 1, r), AXIS, 0, 0, tiled=True)
        return y.reshape(-1, r)

    part = functools.partial
    raw = tuple(pltpu.with_memory_space_constraint(x, pltpu.HBM) for x in (right_side, lo, up, fin, dia, bel, abo))
    edge = shape(64 * (2 * plan.sent - 1) + SUB, r)
    *loaded, edge_across, edge_pair = call(
        part(load_kernel, plan),
        (*(shape(*x.shape) for x in raw), edge, edge),
        [pltpu.SemaphoreType.DMA((len(raw),))],
        *raw,
        space=pltpu.HBM,
    )
    rhs, lo, up = loaded[:3]
    mats = loaded[1:]
    other = lax.ppermute(edge_across, AXIS, [(i, i + 1 if i % 2 else i - 1) for i in range(1, d - 1)])
    pair = lax.ppermute(edge_pair, AXIS, [(i, i ^ 1) for i in range(d)])
    pair = call(take_kernel, edge, [], pair)
    early = call(
        part(pack_kernel, plan, 0, plan.early),
        shape(d * plan.early_rows, r),
        [scratch(plan.early, r, r)],
        *mats,
        flops=10_000_000,
    )
    early = exchange(early)
    late_shape = shape(d * plan.late_rows, r)
    late = call(
        part(pack_kernel, plan, plan.early, plan.groups),
        late_shape,
        [scratch(plan.groups - plan.early, r, r)],
        *mats,
        flops=10_000_000,
    )
    late_shape = shape(d, plan.late_rows, 1, r)
    late, near, fields = call(
        part(first_kernel, plan),
        (late_shape, shape(3, 2, len(plan.near), SUB, SUB, r), shape(3, SUB, r)),
        [scratch(r + 2 * SUB, r), scratch(d, 1, r), pltpu.SemaphoreType.DMA],
        lo, up, rhs, pair, other, late.reshape(late_shape.shape),
        places=[pltpu.VMEM] * 5 + [pl.ANY],
        out_places=[pl.ANY] + [pltpu.VMEM] * 2,
        input_output_aliases={5: 0},
    )
    small = shape(d, r)
    padded = scratch(r + 2 * SUB, r)
    two = [scratch(r, r), padded]
    late = exchange(late)
    coef_shape = shape(plan.own_tiles + plan.halo_tiles, SUB, r)
    lend_shape = shape(plan.halo_tiles, SUB, r)
    coef, lent = call(
        part(unpack_kernel, plan), (coef_shape, lend_shape), [scratch(plan.early, r, r)], early, flops=5_000_000
    )
    lent = lax.ppermute(lent, AXIS, [(i, i ^ 1) for i in range(d)])
    out, coef, w, v, s = call(
        part(start_far_kernel, plan),
        (small, coef_shape, tile, tile, tile),
        [scratch(plan.groups - plan.early, r, r), *two],
        late, coef, lent,
        input_output_aliases={1: 1},
    )
    us, ss, vs, hs = [], [s], [v], []
    for j in range(1, ITERS):
        out, u, h = call(
            part(near_kernel, plan, j),
            (small, shape(3, SUB, r), tile),
            two,
            exchange(out), near, fields, *us, *ss,
        )
        us.append(u)
        hs.append(h)
        if j < ITERS - 1:
            out, w, v, s = call(
                part(far_kernel, plan, j), (small, tile, tile, tile), two, exchange(out), coef, h, w, *vs
            )
            vs.append(v)
        else:
            out, s = call(part(last_far_kernel, plan), (small, tile), two, exchange(out), coef, h, w, *vs)
        ss.append(s)
    return call(
        part(output_kernel, plan),
        (shape(ITERS + 1, SUB, r), shape(ITERS + 1, ITERS)),
        [scratch(r, r)],
        exchange(out), fields, *us, *ss, *hs,
    )


def on_device(*args):
    right_side, lower_level = args[0], args[4]
    devices, rows = lax.axis_size(AXIS), right_side.shape[1]
    if not fits(devices, rows, right_side.shape[0]):
        return general(*args)
    return tuple(transposed(Plan(devices, rows, lower_level.shape[0]), *args))


def solution(mesh):
    return jax.shard_map(
        on_device,
        mesh=mesh,
        in_specs=(
            P(None, "chain"),
            P(None, None, "chain"),
            P(None, None, "chain"),
            P(None, None, "chain"),
            P(None, None, None, "chain"),
            P(None, None, None, "chain"),
            P(None, None, "chain"),
        ),
        out_specs=(P(None, None, "chain"), P()),
        check_vma=False,
    )
```
